8 devices in a mesh: batch: 1 (over z), row: 2 (over y), col: 4 (over x, core).
Axes of the slice: x: 2, y: 2, z: 1, core: 2. Of those that a mesh axis runs over, the one named last changes fastest.
Arguments:
- left_op: bfloat16 [6144, 6144], P(('batch', 'row'), 'col')
- left_start: float32 [6144, 128], P(('batch', 'row', 'col'))
- right_op: bfloat16 [16384, 16384], P(('batch', 'row'), 'col')
- right_start: float32 [16384, 128], P(('batch', 'row', 'col'))
Outputs:
- output 1: float32 [6144, 128], P(('batch', 'row', 'col'))
- output 2: float32 [128, 128], P('batch')
- output 3: float32 [16384, 128], P(('batch', 'row', 'col'))
- output 4: float32 [128, 128], P('batch')
All inputs are finite; a program needn't handle non-finite values.
Results may differ from the reference program's by a relative error of at most 0.001.
Values are sent between devices in bfloat16 or wider.
A program may use at most 1 GiB of HBM per device.

```python
import jax
import jax.numpy as jnp
from jax import lax

N = 6144
N2 = 16384
S = 128
SWEEPS = 4


def build_operator(key, size):
    key_vec, key_val, key_noise = jax.random.split(key, 3)
    eig_basis = jax.random.normal(key_vec, (size, S), jnp.float32) * (size ** -0.5)
    levels = 1.5 * 4.0 ** jax.random.uniform(key_val, (S,), jnp.float32)
    noise_mat = jax.random.normal(key_noise, (size, size), jnp.float32) * (0.1 * size ** -0.5)
    full_mat = jnp.dot(eig_basis * levels, eig_basis.T) + noise_mat
    symmetric = 0.5 * (full_mat + full_mat.T) + 0.5 * jnp.eye(size, dtype=jnp.float32)
    return symmetric.astype(jnp.bfloat16)


def setup_inputs(seed: int = 0, part: int = 0) -> dict:
    base_key = jax.random.fold_in(jax.random.key(seed), part)
    key_left_op, key_left_start, key_right_op, key_right_start = jax.random.split(base_key, 4)
    return {
        "left_op": build_operator(key_left_op, N),
        "left_start": jax.random.normal(key_left_start, (N, S), jnp.float32),
        "right_op": build_operator(key_right_op, N2),
        "right_start": jax.random.normal(key_right_start, (N2, S), jnp.float32),
    }


def cholqr_step(y_mat, gram_mat):
    chol_low = jnp.linalg.cholesky(gram_mat)
    return lax.linalg.triangular_solve(chol_low, y_mat, left_side=False, lower=True, transpose_a=True)


def orthonormalize(y_mat):
    row_count = y_mat.shape[0]
    y_half = y_mat.astype(jnp.bfloat16)
    gram_one = jnp.dot(y_half.T, y_half, preferred_element_type=jnp.float32) / row_count
    y_one = cholqr_step(y_mat, gram_one)
    gram_two = jnp.dot(y_one.T, y_one, precision=lax.Precision.HIGHEST) / row_count
    return cholqr_step(y_one, gram_two)


def iterate(operator, start_block):
    def one_sweep(x_cur, unused):
        y_mat = jnp.dot(operator, x_cur.astype(jnp.bfloat16), preferred_element_type=jnp.float32)
        return orthonormalize(y_mat), None

    x_final, scan_rest = lax.scan(one_sweep, start_block, None, length=SWEEPS)
    z_mat = jnp.dot(operator, x_final.astype(jnp.bfloat16), preferred_element_type=jnp.float32)
    rayleigh = jnp.dot(x_final.T, z_mat, precision=lax.Precision.HIGHEST) / x_final.shape[0]
    return x_final, rayleigh


def reference(left_op, left_start, right_op, right_start):
    left_basis, left_rayleigh = iterate(left_op, left_start)
    right_basis, right_rayleigh = iterate(right_op, right_start)
    return (left_basis, left_rayleigh, right_basis, right_rayleigh)
```

```python
import functools

import jax
import jax.numpy as jnp
from jax import lax
from jax.experimental import pallas as pl
from jax.experimental.pallas import tpu as pltpu
from jax.sharding import PartitionSpec as P

SWEEPS = 4
S = 128
RING = 4
HIGH = lax.Precision.HIGHEST
MESH = pl.DeviceIdType.MESH
NT = (((1,), (1,)), ((), ()))


def high_dot(lhs, rhs):
    return jnp.dot(lhs, rhs, precision=HIGH, preferred_element_type=jnp.float32)


def high_dot_nt(lhs, rhs):
    return lax.dot_general(lhs, rhs, NT, precision=HIGH, preferred_element_type=jnp.float32)


def remote(src, dst, send_sem, recv_sem, row, col):
    return pltpu.make_async_remote_copy(
        src_ref=src, dst_ref=dst, send_sem=send_sem, recv_sem=recv_sem,
        device_id={"row": row, "col": col}, device_id_type=MESH,
    )


def inverse_factors(mats):
    lane = lax.broadcasted_iota(jnp.int32, (S, S), 1)
    row = lax.broadcasted_iota(jnp.int32, (S, S), 0)
    lane8 = lax.broadcasted_iota(jnp.int32, (8, S), 1)
    sub8 = lax.broadcasted_iota(jnp.int32, (8, S), 0)

    def panel(p, carry):
        k0 = pl.multiple_of(p * 8, 8)
        for ref in mats:
            full = ref[...]
            rows = ref[pl.ds(k0, 8), :]
            heads = [
                jnp.broadcast_to(jnp.sum(jnp.where(lane8 == k0 + j, rows, 0.0), axis=1, keepdims=True), (8, S))
                for j in range(8)
            ]
            below = jnp.where(row >= k0 + 8, full, 0.0)
            cols = [jnp.sum(jnp.where(lane == k0 + j, below, 0.0), axis=1, keepdims=True) for j in range(8)]
            in_panel8 = (lane8 >= k0) & (lane8 < k0 + 8)
            rows = jnp.where(in_panel8, jnp.where(lane8 - k0 == sub8, 1.0, 0.0), rows)
            done = rows
            for j in range(8):
                piv = heads[j][j : j + 1, :]
                inv = 1.0 / piv
                scaled = rows[j : j + 1, :] * inv
                done = jnp.where(sub8 == j, rows * lax.rsqrt(piv), done)
                mult = jnp.where(sub8 == j, 0.0, heads[j])
                for m in range(j + 1, 8):
                    head_row = heads[m][j : j + 1, :] * inv
                    heads[m] = jnp.where(sub8 == j, head_row, heads[m] - mult * head_row)
                rows = jnp.where(sub8 == j, scaled, rows - mult * scaled)
            rest = jnp.where((lane >= k0) & (lane < k0 + 8) & (row >= k0 + 8), 0.0, full)
            for j in range(8):
                rest = rest - cols[j] * rows[j : j + 1, :]
            ref[...] = rest
            ref[pl.ds(k0, 8), :] = done
        return carry

    lax.fori_loop(0, S // 8, panel, 0)
    for ref in mats:
        ref[...] = jnp.where(lane <= row, ref[...], 0.0)


class Op:
    def __init__(self, **refs):
        self.__dict__.update(refs)


def kernel(
    l_op, l_start, r_op, r_start,
    l_out, l_ray, r_out, r_ray,
    l_a, r_a,
    l_xs, l_xt, l_ps, l_pr, l_y, l_xf,
    r_xs, r_xt, r_ps, r_pr, r_y, r_xf,
    g_loc, g_one, g_sum, g_two, g_tot, l_m, r_m,
    l_asem, r_asem,
    gs_sem, gr_sem, fs_sem, fr_sem, ps_sem, pr_sem, xs_sem, xr_sem,
    a1s_sem, a1r_sem, a2s_sem, a2r_sem, a3s_sem, a3r_sem,
):
    y = lax.axis_index("row")
    col = lax.axis_index("col")
    x = col // 2
    k = col % 2
    mate = x * 2 + (1 - k)

    ops = [
        Op(i=0, n=l_op.shape[0] * 2, start=l_start, out=l_out, ray=l_ray, xs=l_xs, xt=l_xt, ps=l_ps, pr=l_pr, y=l_y, xf=l_xf, m=l_m),
        Op(i=1, n=r_op.shape[0] * 2, start=r_start, out=r_out, ray=r_ray, xs=r_xs, xt=r_xt, ps=r_ps, pr=r_pr, y=r_y, xf=r_xf, m=r_m),
    ]
    for o in ops:
        o.nb = o.n // 8
        o.tiles, o.tn = o.ps.shape[0], o.ps.shape[2]

    l_load = pltpu.make_async_copy(l_op, l_a, l_asem)
    l_load.start()

    def r_tile_col(t):
        half = jnp.where(t < 4, 1 - y, y)
        return pl.multiple_of(half * ops[1].nb + (t % 4) * ops[1].tn, ops[1].tn)

    def r_fetch(t):
        return pltpu.make_async_copy(
            r_op.at[:, pl.ds(r_tile_col(t), ops[1].tn)], r_a.at[t % RING], r_asem.at[t % RING]
        )

    for t in range(RING):
        r_fetch(t).start()

    def gather_start(o, dest_row, my_slot):
        for a in range(2):
            is_self = (dest_row == y) & (x == a)

            @pl.when(is_self)
            def _():
                o.xt[my_slot] = o.xs[...]

            @pl.when(jnp.logical_not(is_self))
            def _():
                remote(o.xs, o.xt.at[my_slot], gs_sem.at[o.i, a], gr_sem.at[o.i, o.src], dest_row, 2 * a + k).start()

    def gather(first):
        for o in ops:
            o.src = x if first else y
            my_slot = 2 * x + k if first else 2 * k + y
            gather_start(o, y if first else x, my_slot)
        for o in ops:
            for a in range(2):
                slot = 2 * a + k if first else 2 * k + a
                from_self = (x == a) if first else ((x == y) & (y == a))

                @pl.when(jnp.logical_not(from_self))
                def _():
                    remote(o.xs, o.xt.at[slot], gs_sem.at[o.i, 0], gr_sem.at[o.i, a], y, col).wait_recv()

                remote(o.xt.at[slot], o.xt.at[slot], fs_sem.at[o.i, a], fr_sem.at[o.i, a], y, mate).start()
        for o in ops:
            for a in range(2):
                slot = 2 * a + k if first else 2 * k + a
                other = 2 * a + (1 - k) if first else 2 * (1 - k) + a
                remote(o.xt.at[slot], o.xt.at[slot], fs_sem.at[o.i, a], fr_sem.at[o.i, a], y, mate).wait_send()
                remote(o.xt.at[other], o.xt.at[other], fs_sem.at[o.i, a], fr_sem.at[o.i, a], y, mate).wait_recv()
                dest_row = y if first else x
                is_self = (dest_row == y) & (x == a)

                @pl.when(jnp.logical_not(is_self))
                def _():
                    remote(o.xs, o.xt.at[slot], gs_sem.at[o.i, a], gr_sem.at[o.i, a], y, col).wait_send()

    def tile_send(o, t):
        return remote(o.ps.at[t], o.pr.at[t], ps_sem.at[o.i, t], pr_sem.at[o.i, t], 1 - y, col)

    def block_dot(o, a_rows):
        total = None
        for s in range(4):
            part = jnp.dot(o.xt[s], a_rows(s), preferred_element_type=jnp.float32)
            total = part if total is None else total + part
        return total

    def multiply_l():
        o = ops[0]
        nb = o.nb
        for t in range(o.tiles):
            start = pl.multiple_of((1 - y) * nb + t * o.tn, 128)
            o.ps[t] = block_dot(o, lambda s: l_a[pl.ds(s * nb, nb), pl.ds(start, o.tn)])
            tile_send(o, t).start()
        for t in range(o.tiles):
            start = pl.multiple_of(y * nb + t * o.tn, 128)
            o.y[:, pl.ds(t * o.tn, o.tn)] = block_dot(o, lambda s: l_a[pl.ds(s * nb, nb), pl.ds(start, o.tn)])

    def multiply_r(last):
        o = ops[1]

        def one(t, carry):
            r_fetch(t).wait()
            b = t % RING
            res = block_dot(o, lambda s: r_a[b, pl.ds(s * o.nb, o.nb), :])

            @pl.when(t < o.tiles)
            def _():
                o.ps[t] = res
                tile_send(o, t).start()

            @pl.when(t >= o.tiles)
            def _():
                o.y[:, pl.ds(pl.multiple_of((t - o.tiles) * o.tn, o.tn), o.tn)] = res

            ahead = t + RING
            if last:

                @pl.when(ahead < 2 * o.tiles)
                def _():
                    r_fetch(ahead).start()
            else:
                r_fetch(lax.rem(ahead, 2 * o.tiles)).start()
            return carry

        lax.fori_loop(0, 2 * o.tiles, one, 0)

    def reduce_finish(o):
        for t in range(o.tiles):
            copy = tile_send(o, t)
            copy.wait_recv()
            o.y[:, t * o.tn : (t + 1) * o.tn] = o.y[:, t * o.tn : (t + 1) * o.tn] + o.pr[t]
        for t in range(o.tiles):
            tile_send(o, t).wait_send()

    def all_reduce(par):
        half, other = pl.ds(pl.multiple_of(k * 64, 64), 64), pl.ds(pl.multiple_of((1 - k) * 64, 64), 64)
        one = remote(g_loc.at[:, other], g_one.at[par], a1s_sem.at[par], a1r_sem.at[par], y, mate)
        one.start()
        one.wait_recv()
        g_sum[...] = g_loc[:, half, :] + g_one[par]
        twos = []
        for q in range(3):
            yd = y + ((q + 1) // 2) * (1 - 2 * y)
            xd = x + ((q + 1) % 2) * (1 - 2 * x)
            two = remote(g_sum, g_two.at[par, q], a2s_sem.at[par, q], a2r_sem.at[par, q], yd, 2 * xd + k)
            two.start()
            twos.append(two)
        for two in twos:
            two.wait_recv()
        g_tot[:, half, :] = (g_sum[...] + g_two[par, 0]) + (g_two[par, 1] + g_two[par, 2])
        three = remote(g_tot.at[:, half], g_tot.at[:, half], a3s_sem.at[par], a3r_sem.at[par], y, mate)
        three.start()
        remote(g_tot.at[:, other], g_tot.at[:, other], a3s_sem.at[par], a3r_sem.at[par], y, mate).wait_recv()
        one.wait_send()
        for two in twos:
            two.wait_send()
        three.wait_send()

    def factor_and_apply():
        for o in ops:
            o.m[...] = g_tot[o.i] / float(o.n)
        inverse_factors([o.m for o in ops])
        for o in ops:
            o.y[...] = high_dot(o.m[...], o.y[...])

    def multiply(last):
        multiply_l()
        multiply_r(last)
        for o in ops:
            reduce_finish(o)

    for o in ops:
        for b in range(o.nb // S):
            o.xs[:, b * S : (b + 1) * S] = o.start[b * S : (b + 1) * S, :].T.astype(jnp.bfloat16)
    gather(True)
    l_load.wait()

    def sweep(i, carry):
        multiply(False)
        for o in ops:
            half = o.y[...].astype(jnp.bfloat16)
            g_loc[o.i] = lax.dot_general(half, half, NT, preferred_element_type=jnp.float32)
        all_reduce(0)
        factor_and_apply()
        for o in ops:
            g_loc[o.i] = high_dot_nt(o.y[...], o.y[...])
        all_reduce(1)
        factor_and_apply()
        for o in ops:
            o.xs[...] = o.y[...].astype(jnp.bfloat16)
        gather(False)
        return carry

    lax.fori_loop(0, SWEEPS, sweep, 0)

    stays = (x == y) & (col == 2 * k + y)
    for o in ops:

        @pl.when(stays)
        def _():
            o.xf[1] = o.y[...]

        @pl.when(jnp.logical_not(stays))
        def _():
            o.xf[0] = o.y[...]
            remote(o.xf.at[0], o.xf.at[1], xs_sem.at[o.i], xr_sem.at[o.i], x, 2 * k + y).start()

    multiply(True)
    for o in ops:
        @pl.when(stays)
        def _():
            g_loc[o.i] = high_dot_nt(o.xf[1], o.y[...])

        @pl.when(jnp.logical_not(stays))
        def _():
            g_loc[o.i] = high_dot_nt(o.xf[0], o.y[...])

    all_reduce(0)
    for o in ops:
        o.ray[...] = g_tot[o.i] / float(o.n)

        @pl.when(jnp.logical_not(stays))
        def _():
            copy = remote(o.xf.at[0], o.xf.at[1], xs_sem.at[o.i], xr_sem.at[o.i], x, 2 * k + y)
            copy.wait_recv()
            copy.wait_send()

        for b in range(o.nb // S):
            o.out[b * S : (b + 1) * S, :] = o.xf[1, :, b * S : (b + 1) * S].T


def solution(mesh):
    def local_program(left_op, left_start, right_op, right_start):
        def blocks(n, tiles):
            nb = n // 8
            f32, bf16 = jnp.float32, jnp.bfloat16
            return [
                pltpu.VMEM((S, nb), bf16),
                pltpu.VMEM((4, S, nb), bf16),
                pltpu.VMEM((tiles, S, nb // tiles), f32),
                pltpu.VMEM((tiles, S, nb // tiles), f32),
                pltpu.VMEM((S, nb), f32),
                pltpu.VMEM((2, S, nb), f32),
            ]

        l_n, r_n = left_op.shape[0] * 2, right_op.shape[0] * 2
        f32 = jnp.float32
        dma = pltpu.SemaphoreType.DMA
        vmem = pl.BlockSpec(memory_space=pltpu.VMEM)
        hbm = pl.BlockSpec(memory_space=pl.ANY)
        left_basis, left_ray, right_basis, right_ray = pl.pallas_call(
            kernel,
            out_shape=(
                jax.ShapeDtypeStruct((l_n // 8, S), f32),
                jax.ShapeDtypeStruct((S, S), f32),
                jax.ShapeDtypeStruct((r_n // 8, S), f32),
                jax.ShapeDtypeStruct((S, S), f32),
            ),
            in_specs=[hbm, vmem, hbm, vmem],
            out_specs=(vmem, vmem, vmem, vmem),
            scratch_shapes=[
                pltpu.VMEM(left_op.shape, jnp.bfloat16),
                pltpu.VMEM((RING, right_op.shape[0], r_n // 8 // 4), jnp.bfloat16),
                *blocks(l_n, 1),
                *blocks(r_n, 4),
                pltpu.VMEM((2, S, S), f32),
                pltpu.VMEM((2, 2, 64, S), f32),
                pltpu.VMEM((2, 64, S), f32),
                pltpu.VMEM((2, 3, 2, 64, S), f32),
                pltpu.VMEM((2, S, S), f32),
                pltpu.VMEM((S, S), f32),
                pltpu.VMEM((S, S), f32),
                dma,
                dma((RING,)),
                dma((2, 2)), dma((2, 2)), dma((2, 2)), dma((2, 2)),
                dma((2, 4)), dma((2, 4)), dma((2,)), dma((2,)),
                dma((2,)), dma((2,)), dma((2, 3)), dma((2, 3)), dma((2,)), dma((2,)),
            ],
            compiler_params=pltpu.CompilerParams(has_side_effects=True, vmem_limit_bytes=64 * 1024 * 1024 - 65536),
        )(left_op, left_start, right_op, right_start)
        return left_basis, left_ray, right_basis, right_ray

    op_spec = P(("batch", "row"), "col")
    vec_spec = P(("batch", "row", "col"), None)
    small_spec = P("batch", None)
    return jax.shard_map(
        local_program, mesh=mesh, in_specs=(op_spec, vec_spec, op_spec, vec_spec),
        out_specs=(vec_spec, small_spec, vec_spec, small_spec), check_vma=False,
    )
```

```python
import jax
import jax.numpy as jnp
from jax import lax
from jax.experimental import pallas as pl
from jax.experimental.pallas import tpu as pltpu
from jax.sharding import PartitionSpec as P

SWEEPS = 4
S = 128
RING = 4
TILES = 4
CHUNKS = 2
PANEL = 16
MESH = pl.DeviceIdType.MESH
F32, BF16 = jnp.float32, jnp.bfloat16
NT = (((1,), (1,)), ((), ()))
TN = (((0,), (0,)), ((), ()))


def dot(lhs, rhs):
    return jnp.dot(lhs, rhs, preferred_element_type=F32)


def dot_nt(lhs, rhs):
    return lax.dot_general(lhs, rhs, NT, preferred_element_type=F32)


def split(value):
    high = value.astype(BF16)
    rest = value - high.astype(F32)
    mid = rest.astype(BF16)
    low = (rest - mid.astype(F32)).astype(BF16)
    return high, mid, low


def remote(src, dst, send_sem, recv_sem, row, col):
    return pltpu.make_async_remote_copy(
        src_ref=src, dst_ref=dst, send_sem=send_sem, recv_sem=recv_sem,
        device_id={"row": row, "col": col}, device_id_type=MESH,
    )


def inverse_factors(mats):
    sub = lax.broadcasted_iota(jnp.int32, (PANEL, S), 0)
    lane = lax.broadcasted_iota(jnp.int32, (PANEL, S), 1)

    tall_row = lax.broadcasted_iota(jnp.int32, (S, S), 0)
    tall_lane = lax.broadcasted_iota(jnp.int32, (S, S), 1)

    def panel(p, carry):
        k0 = pl.multiple_of(p * PANEL, PANEL)
        inside = (tall_lane >= k0) & (tall_lane < k0 + PANEL) & (tall_row >= k0 + PANEL)
        at = lane - k0
        for ref in mats:
            rows = ref[pl.ds(k0, PANEL), :]
            heads = jnp.stack(
                [
                    jnp.broadcast_to(jnp.sum(jnp.where(at == j, rows, 0.0), axis=1, keepdims=True), (PANEL, S))
                    for j in range(PANEL)
                ]
            )
            high, mid, low = split(jnp.where(at >= PANEL, rows, 0.0))
            cols = jnp.concatenate([high, mid, high, mid, high, low], axis=0)
            rows = jnp.where((at >= 0) & (at < PANEL), jnp.where(at == sub, 1.0, 0.0), rows)
            done = rows
            piv = heads[0, 0:1, :]
            for j in range(PANEL):
                here = sub == j
                root = lax.rsqrt(piv)
                inv = root * root
                done = jnp.where(here, rows * root, done)
                mult = jnp.where(here, 0.0, heads[0])
                if j < PANEL - 1:
                    head_rows = heads[1:, j : j + 1, :] * inv
                    piv = heads[1, j + 1 : j + 2, :] - heads[0, j + 1 : j + 2, :] * head_rows[0]
                    heads = jnp.where(here[None], head_rows, heads[1:] - mult[None] * head_rows)
                scaled = rows[j : j + 1, :] * inv
                rows = jnp.where(here, scaled, rows - mult * scaled)
            high, mid, low = split(rows)
            rhs = jnp.concatenate([high, high, mid, mid, low, high], axis=0)
            change = lax.dot_general(cols, rhs, TN, preferred_element_type=F32)
            ref[...] = jnp.where(inside, 0.0, ref[...]) - change
            ref[pl.ds(k0, PANEL), :] = done
        return carry

    lax.fori_loop(0, S // PANEL, panel, 0)
    for ref in mats:
        ref[...] = jnp.where(tall_lane <= tall_row, ref[...], 0.0)


class Op:
    def __init__(self, **refs):
        self.__dict__.update(refs)


def kernel(
    l_op, l_start, r_op, r_start,
    l_out, r_out, ray_out,
    l_a, r_a,
    l_xs, l_xt, l_mate_s, l_mate_r, l_side_s, l_side_r, l_y, l_m, l_sp,
    r_xs, r_xt, r_ps, r_pr, r_y, r_m, r_sp, r_keep,
    g_loc, g_one, g_sum, g_two, g_tot,
    l_asem, r_asem,
    gs_sem, gr_sem, fs_sem, fr_sem, ps_sem, pr_sem, xs_sem, xr_sem,
    lgs_sem, lgr_sem, lms_sem, lmr_sem, lss_sem, lsr_sem,
    a1s_sem, a1r_sem, a2s_sem, a2r_sem, a3s_sem, a3r_sem,
):
    y = lax.axis_index("row")
    col = lax.axis_index("col")
    x = col // 2
    k = col % 2
    mate = x * 2 + (1 - k)
    l_n, r_n = l_op.shape[0] * 2, r_op.shape[0] * 2
    l_nb, r_nb = l_n // 8, r_n // 8
    tile = r_nb // TILES
    piece = r_nb // CHUNKS

    left = Op(i=0, n=l_n, nb=l_nb, y=l_y, m=l_m, sp=l_sp)
    right = Op(i=1, n=r_n, nb=r_nb, y=r_y, m=r_m, sp=r_sp)
    ops = [left, right]

    l_load = pltpu.make_async_copy(l_op, l_a, l_asem)
    l_load.start()

    def r_fetch(t):
        half = jnp.where(t < TILES, 1 - y, y)
        start = pl.multiple_of(half * r_nb + (t % TILES) * tile, tile)
        return pltpu.make_async_copy(r_op.at[:, pl.ds(start, tile)], r_a.at[t % RING], r_asem.at[t % RING])

    for t in range(RING):
        r_fetch(t).start()

    class Gather:
        def __init__(self, first):
            self.dest_row = y if first else x
            self.my_slot = 2 * x + k if first else 2 * k + y
            self.src = x if first else y
            self.slots = [2 * a + k if first else 2 * k + a for a in range(2)]
            self.other_slots = [2 * a + (1 - k) if first else 2 * (1 - k) + a for a in range(2)]
            self.sends_to_self = [(self.dest_row == y) & (x == a) for a in range(2)]
            self.gets_from_self = [(x == a) if first else ((x == y) & (y == a)) for a in range(2)]

        def copy(self, a, h, recv):
            return remote(
                r_xs.at[h], r_xt.at[self.my_slot, h], gs_sem.at[a, h], gr_sem.at[recv, h], self.dest_row, 2 * a + k
            )

        def forward(self, a, h, slots):
            ref = r_xt.at[slots[a], h]
            return remote(ref, ref, fs_sem.at[a, h], fr_sem.at[a, h], y, mate)

        def start(self, h):
            for a in range(2):

                @pl.when(self.sends_to_self[a])
                def _():
                    r_xt[self.my_slot, h] = r_xs[h]

                @pl.when(jnp.logical_not(self.sends_to_self[a]))
                def _():
                    self.copy(a, h, self.src).start()

        def finish(self):
            for h in range(CHUNKS):
                for a in range(2):

                    @pl.when(jnp.logical_not(self.gets_from_self[a]))
                    def _():
                        self.copy(0, h, a).wait_recv()

                    self.forward(a, h, self.slots).start()
            for h in range(CHUNKS):
                for a in range(2):
                    self.forward(a, h, self.other_slots).wait_recv()

        def drain(self):
            for h in range(CHUNKS):
                for a in range(2):
                    self.forward(a, h, self.slots).wait_send()

                    @pl.when(jnp.logical_not(self.sends_to_self[a]))
                    def _():
                        self.copy(a, h, self.src).wait_send()

    def left_copy(b, slot):
        return remote(l_xs, l_xt.at[slot], lgs_sem.at[b], lgr_sem.at[slot], b, 2 * y + x)

    def left_self(b):
        return (b == y) & (y == x) & (x == k)

    def left_start():
        for b in range(2):

            @pl.when(left_self(b))
            def _():
                l_xt[k] = l_xs[...]

            @pl.when(jnp.logical_not(left_self(b)))
            def _():
                left_copy(b, k).start()

    def left_finish():
        for slot in range(2):

            @pl.when(jnp.logical_not((y == x) & (x == k) & (k == slot)))
            def _():
                left_copy(0, slot).wait_recv()

    def left_drain():
        for b in range(2):

            @pl.when(jnp.logical_not(left_self(b)))
            def _():
                left_copy(b, k).wait_send()

    def left_block(index):
        rows = pl.ds(pl.multiple_of(index * l_nb, l_nb), l_nb)
        return dot_nt(l_xt[0], l_a[rows, :l_nb]) + dot_nt(l_xt[1], l_a[rows, l_nb:])

    def left_mate(a):
        return remote(l_mate_s.at[a], l_mate_r.at[a], lms_sem.at[a], lmr_sem.at[a], y, mate)

    def left_side():
        return remote(l_side_s, l_side_r, lss_sem, lsr_sem, y, 2 * (1 - x) + k)

    def left_multiply():
        for a in (1 - x, x):
            l_mate_s[a] = left_block(2 * a + (1 - k))
            left_mate(a).start()
        l_side_s[...] = left_block(2 * (1 - x) + k)
        l_y[...] = left_block(2 * x + k)

    def left_reduce_start():
        left_mate(1 - x).wait_recv()
        l_side_s[...] = l_side_s[...] + l_mate_r[1 - x]
        left_side().start()
        left_mate(x).wait_recv()
        l_y[...] = l_y[...] + l_mate_r[x]

    def left_reduce_finish():
        left_side().wait_recv()
        l_y[...] = l_y[...] + l_side_r[...]
        left_side().wait_send()
        for a in range(2):
            left_mate(a).wait_send()

    def right_send(t):
        return remote(r_ps.at[t], r_pr.at[t], ps_sem.at[t], pr_sem.at[t], 1 - y, col)

    def right_tile(t):
        r_fetch(t).wait()
        b = t % RING
        total = None
        for s in range(4):
            for h in range(CHUNKS):
                part = dot(r_xt[s, h], r_a[b, s * r_nb + h * piece : s * r_nb + (h + 1) * piece, :])
                total = part if total is None else total + part
        return total

    def right_multiply(own, last):
        def one(i, carry):
            t = i + TILES * own
            res = right_tile(t)
            if own:
                r_y[:, pl.ds(pl.multiple_of(i * tile, tile), tile)] = res
            else:
                r_ps[i] = res
                right_send(i).start()
            ahead = t + RING
            if not (last and own):
                r_fetch(lax.rem(ahead, 2 * TILES)).start()
            return carry

        lax.fori_loop(0, TILES, one, 0)

    def right_reduce_finish():
        for t in range(TILES):
            right_send(t).wait_recv()
            r_y[:, t * tile : (t + 1) * tile] = r_y[:, t * tile : (t + 1) * tile] + r_pr[t]
        for t in range(TILES):
            right_send(t).wait_send()

    def all_reduce(par):
        half, other = pl.ds(pl.multiple_of(k * 64, 64), 64), pl.ds(pl.multiple_of((1 - k) * 64, 64), 64)
        one = remote(g_loc.at[:, other], g_one.at[par], a1s_sem.at[par], a1r_sem.at[par], y, mate)
        one.start()
        one.wait_recv()
        g_sum[...] = g_loc[:, half, :] + g_one[par]
        twos = []
        for q in (2, 1, 0):
            yd = y + ((q + 1) // 2) * (1 - 2 * y)
            xd = x + ((q + 1) % 2) * (1 - 2 * x)
            two = remote(g_sum, g_two.at[par, q], a2s_sem.at[par, q], a2r_sem.at[par, q], yd, 2 * xd + k)
            two.start()
            twos.append(two)
        for two in twos:
            two.wait_recv()
        g_tot[:, half, :] = (g_sum[...] + g_two[par, 0]) + (g_two[par, 1] + g_two[par, 2])
        three = remote(g_tot.at[:, half], g_tot.at[:, half], a3s_sem.at[par], a3r_sem.at[par], y, mate)
        three.start()
        remote(g_tot.at[:, other], g_tot.at[:, other], a3s_sem.at[par], a3r_sem.at[par], y, mate).wait_recv()
        one.wait_send()
        for two in twos:
            two.wait_send()
        three.wait_send()

    def factor():
        for o in ops:
            o.m[...] = g_tot[o.i] / float(o.n)
        inverse_factors([o.m for o in ops])

    def apply_piece(o, lhs, start, width):
        high, mid, low = split(o.y[:, start : start + width])
        rhs = jnp.concatenate([high, high, mid, mid, low, high], axis=0)
        return dot(lhs, rhs)

    def apply_lhs(o):
        high, mid, low = split(o.m[...])
        return jnp.concatenate([high, mid, high, mid, high, low], axis=1)

    def second_gram(o):
        lhs = apply_lhs(o)
        for start in range(0, o.nb, 256):
            res = apply_piece(o, lhs, start, 256)
            o.y[:, start : start + 256] = res
            parts = split(res)
            for q in range(3):
                o.sp[q * S : (q + 1) * S, start : start + 256] = parts[q]
        both = dot_nt(o.sp[: 2 * S, :], o.sp[: 2 * S, :])
        cross = dot_nt(o.sp[:S, :], o.sp[2 * S :, :])
        g_loc[o.i] = both[:S, :S] + ((both[:S, S:] + both[S:, :S]) + (both[S:, S:] + (cross + cross.T)))

    def rayleigh(o, basis):
        g_loc[o.i] = lax.dot_general(basis, o.y[...], NT, precision=lax.Precision.HIGHEST, preferred_element_type=F32)

    def new_basis(gather):
        lhs = apply_lhs(right)
        for h in range(CHUNKS):
            for start in range(h * piece, (h + 1) * piece, 256):
                res = apply_piece(right, lhs, start, 256)
                r_y[:, start : start + 256] = res
                r_xs[h, :, start - h * piece : start - h * piece + 256] = res.astype(BF16)
            gather.start(h)
        lhs = apply_lhs(left)
        for start in range(0, l_nb, 256):
            res = apply_piece(left, lhs, start, 256)
            l_y[:, start : start + 256] = res
            l_xs[:, start : start + 256] = res.astype(BF16)
        left_start()

    def multiply(gather, last):
        gather.finish()
        right_multiply(0, last)
        left_finish()
        left_multiply()
        right_multiply(1, last)
        left_reduce_start()
        right_reduce_finish()
        left_reduce_finish()
        gather.drain()
        left_drain()

    first, later = Gather(True), Gather(False)
    for h in range(CHUNKS):
        for b in range(piece // S):
            r_xs[h, :, b * S : (b + 1) * S] = r_start[h * piece + b * S : h * piece + (b + 1) * S, :].T.astype(BF16)
        first.start(h)
    for b in range(l_nb // S):
        l_xs[:, b * S : (b + 1) * S] = l_start[b * S : (b + 1) * S, :].T.astype(BF16)
    left_start()
    first.finish()
    first.drain()
    l_load.wait()

    class Ready:
        def finish(self):
            pass

        def drain(self):
            pass

    def sweep(i, carry):
        multiply(Ready(), False)
        for o in ops:
            half = o.y[...].astype(BF16)
            g_loc[o.i] = dot_nt(half, half)
        all_reduce(0)
        factor()
        for o in ops:
            second_gram(o)
        all_reduce(1)
        factor()
        new_basis(later)
        later.finish()
        later.drain()
        return carry

    lax.fori_loop(0, SWEEPS, sweep, 0)

    stays = (x == y) & (col == 2 * k + y)
    home = remote(r_keep.at[0], r_keep.at[1], xs_sem, xr_sem, x, 2 * k + y)
    r_keep[0] = r_y[...]

    @pl.when(stays)
    def _():
        r_keep[1] = r_y[...]

    @pl.when(jnp.logical_not(stays))
    def _():
        home.start()

    l_out[...] = l_y[...]
    multiply(Ready(), True)
    rayleigh(left, l_out[...])
    rayleigh(right, r_keep[0])
    all_reduce(0)
    for o in ops:
        ray_out[o.i] = g_tot[o.i] / float(o.n)

    @pl.when(jnp.logical_not(stays))
    def _():
        home.wait_recv()
        home.wait_send()

    r_out[...] = r_keep[1]


def finish_kernel(l_in, r_in, ray_in, l_out, l_ray, r_out, r_ray):
    for src, dst in ((l_in, l_out), (r_in, r_out)):
        for b in range(dst.shape[0] // S):
            dst[b * S : (b + 1) * S, :] = src[:, b * S : (b + 1) * S].T
    l_ray[...] = ray_in[0]
    r_ray[...] = ray_in[1]


def solution(mesh):
    def local_program(left_op, left_start, right_op, right_start):
        l_nb, r_nb = left_op.shape[0] // 4, right_op.shape[0] // 4
        dma = pltpu.SemaphoreType.DMA
        vmem = pl.BlockSpec(memory_space=pltpu.VMEM)
        hbm = pl.BlockSpec(memory_space=pl.ANY)
        shape = jax.ShapeDtypeStruct
        left_t, right_t, rayleigh = pl.pallas_call(
            kernel,
            out_shape=(shape((S, l_nb), F32), shape((S, r_nb), F32), shape((2, S, S), F32)),
            in_specs=[hbm, vmem, hbm, vmem],
            out_specs=(vmem, vmem, vmem),
            scratch_shapes=[
                pltpu.VMEM(left_op.shape, BF16),
                pltpu.VMEM((RING, right_op.shape[0], r_nb // TILES), BF16),
                pltpu.VMEM((S, l_nb), BF16),
                pltpu.VMEM((2, S, l_nb), BF16),
                pltpu.VMEM((2, S, l_nb), F32),
                pltpu.VMEM((2, S, l_nb), F32),
                pltpu.VMEM((S, l_nb), F32),
                pltpu.VMEM((S, l_nb), F32),
                pltpu.VMEM((S, l_nb), F32),
                pltpu.VMEM((S, S), F32),
                pltpu.VMEM((3 * S, l_nb), BF16),
                pltpu.VMEM((CHUNKS, S, r_nb // CHUNKS), BF16),
                pltpu.VMEM((4, CHUNKS, S, r_nb // CHUNKS), BF16),
                pltpu.VMEM((TILES, S, r_nb // TILES), F32),
                pltpu.VMEM((TILES, S, r_nb // TILES), F32),
                pltpu.VMEM((S, r_nb), F32),
                pltpu.VMEM((S, S), F32),
                pltpu.VMEM((3 * S, r_nb), BF16),
                pltpu.VMEM((2, S, r_nb), F32),
                pltpu.VMEM((2, S, S), F32),
                pltpu.VMEM((2, 2, 64, S), F32),
                pltpu.VMEM((2, 64, S), F32),
                pltpu.VMEM((2, 3, 2, 64, S), F32),
                pltpu.VMEM((2, S, S), F32),
                dma, dma((RING,)),
                dma((2, CHUNKS)), dma((2, CHUNKS)), dma((2, CHUNKS)), dma((2, CHUNKS)),
                dma((TILES,)), dma((TILES,)), dma, dma,
                dma((2,)), dma((2,)), dma((2,)), dma((2,)), dma, dma,
                dma((2,)), dma((2,)), dma((2, 3)), dma((2, 3)), dma((2,)), dma((2,)),
            ],
            compiler_params=pltpu.CompilerParams(has_side_effects=True, vmem_limit_bytes=64 * 1024 * 1024 - 65536),
        )(left_op, left_start, right_op, right_start)
        left_basis, left_ray, right_basis, right_ray = pl.pallas_call(
            finish_kernel,
            out_shape=(shape((l_nb, S), F32), shape((S, S), F32), shape((r_nb, S), F32), shape((S, S), F32)),
            in_specs=[vmem] * 3,
            out_specs=(vmem,) * 4,
        )(left_t, right_t, rayleigh)
        return left_basis, left_ray, right_basis, right_ray

    op_spec = P(("batch", "row"), "col")
    vec_spec = P(("batch", "row", "col"), None)
    small_spec = P("batch", None)
    return jax.shard_map(
        local_program, mesh=mesh, in_specs=(op_spec, vec_spec, op_spec, vec_spec),
        out_specs=(vec_spec, small_spec, vec_spec, small_spec), check_vma=False,
    )
```

```python
import jax
import jax.numpy as jnp
from jax import lax
from jax.experimental import pallas as pl
from jax.experimental.pallas import tpu as pltpu
from jax.sharding import PartitionSpec as P

SWEEPS = 4
S = 128
RING = 4
TILES = 4
CHUNKS = 4
PANEL = 16
MESH = pl.DeviceIdType.MESH
F32, BF16 = jnp.float32, jnp.bfloat16
NT = (((1,), (1,)), ((), ()))
TN = (((0,), (0,)), ((), ()))


def dot(lhs, rhs):
    return jnp.dot(lhs, rhs, preferred_element_type=F32)


def dot_nt(lhs, rhs):
    return lax.dot_general(lhs, rhs, NT, preferred_element_type=F32)


def split(value):
    high = value.astype(BF16)
    rest = value - high.astype(F32)
    mid = rest.astype(BF16)
    low = (rest - mid.astype(F32)).astype(BF16)
    return high, mid, low


def remote(src, dst, send_sem, recv_sem, row, col):
    return pltpu.make_async_remote_copy(
        src_ref=src, dst_ref=dst, send_sem=send_sem, recv_sem=recv_sem,
        device_id={"row": row, "col": col}, device_id_type=MESH,
    )


def inverse_factors(mats):
    sub = lax.broadcasted_iota(jnp.int32, (PANEL, S), 0)
    lane = lax.broadcasted_iota(jnp.int32, (PANEL, S), 1)

    tall_row = lax.broadcasted_iota(jnp.int32, (S, S), 0)
    tall_lane = lax.broadcasted_iota(jnp.int32, (S, S), 1)

    def panel(p, carry):
        k0 = pl.multiple_of(p * PANEL, PANEL)
        inside = (tall_lane >= k0) & (tall_lane < k0 + PANEL) & (tall_row >= k0 + PANEL)
        at = lane - k0
        for ref in mats:
            rows = ref[pl.ds(k0, PANEL), :]
            heads = jnp.stack(
                [
                    jnp.broadcast_to(jnp.sum(jnp.where(at == j, rows, 0.0), axis=1, keepdims=True), (PANEL, S))
                    for j in range(PANEL)
                ]
            )
            high, mid, low = split(jnp.where(at >= PANEL, rows, 0.0))
            cols = jnp.concatenate([high, mid, high, mid, high, low], axis=0)
            rows = jnp.where((at >= 0) & (at < PANEL), jnp.where(at == sub, 1.0, 0.0), rows)
            done = rows
            piv = heads[0, 0:1, :]
            for j in range(PANEL):
                here = sub == j
                root = lax.rsqrt(piv)
                inv = root * root
                done = jnp.where(here, rows * root, done)
                mult = jnp.where(here, 0.0, heads[0])
                if j < PANEL - 1:
                    head_rows = heads[1:, j : j + 1, :] * inv
                    piv = heads[1, j + 1 : j + 2, :] - heads[0, j + 1 : j + 2, :] * head_rows[0]
                    heads = jnp.where(here[None], head_rows, heads[1:] - mult[None] * head_rows)
                scaled = rows[j : j + 1, :] * inv
                rows = jnp.where(here, scaled, rows - mult * scaled)
            high, mid, low = split(rows)
            rhs = jnp.concatenate([high, high, mid, mid, low, high], axis=0)
            change = lax.dot_general(cols, rhs, TN, preferred_element_type=F32)
            ref[...] = jnp.where(inside, 0.0, ref[...]) - change
            ref[pl.ds(k0, PANEL), :] = done
        return carry

    lax.fori_loop(0, S // PANEL, panel, 0)
    for ref in mats:
        ref[...] = jnp.where(tall_lane <= tall_row, ref[...], 0.0)


class Op:
    def __init__(self, **refs):
        self.__dict__.update(refs)


def kernel(
    l_op, l_start, r_op, r_start,
    l_out, r_out, ray_out,
    l_a, r_a,
    l_xs, l_xt, l_mate_s, l_mate_r, l_side_s, l_side_r, l_y, l_m, l_sp,
    r_xs, r_xt, r_hand, r_ps, r_pr, r_y, r_m, r_sp, r_keep,
    g_loc, g_one, g_sum, g_two, g_tot,
    l_asem, r_asem,
    gs_sem, gr_sem, fs_sem, fr_sem, hs_sem, hr_sem, ps_sem, pr_sem, xs_sem, xr_sem,
    lgs_sem, lgr_sem, lms_sem, lmr_sem, lss_sem, lsr_sem,
    a1s_sem, a1r_sem, a2s_sem, a2r_sem, a3s_sem, a3r_sem,
):
    y = lax.axis_index("row")
    col = lax.axis_index("col")
    x = col // 2
    k = col % 2
    mate = x * 2 + (1 - k)
    l_n, r_n = l_op.shape[0] * 2, r_op.shape[0] * 2
    l_nb, r_nb = l_n // 8, r_n // 8
    tile = r_nb // TILES
    piece = r_nb // CHUNKS

    left = Op(i=0, n=l_n, nb=l_nb, y=l_y, m=l_m, sp=l_sp)
    right = Op(i=1, n=r_n, nb=r_nb, y=r_y, m=r_m, sp=r_sp)
    ops = [left, right]

    l_load = pltpu.make_async_copy(l_op, l_a, l_asem)
    l_load.start()

    def r_fetch(t):
        half = jnp.where(t < TILES, 1 - y, y)
        start = pl.multiple_of(half * r_nb + (t % TILES) * tile, tile)
        return pltpu.make_async_copy(r_op.at[:, pl.ds(start, tile)], r_a.at[t % RING], r_asem.at[t % RING])

    for t in range(RING):
        r_fetch(t).start()

    class Gather:
        def __init__(self, first):
            self.dest_row = y if first else x
            self.my_slot = 2 * x + k if first else 2 * k + y
            self.src = x if first else y
            self.slots = [2 * a + k if first else 2 * k + a for a in range(2)]
            self.other_slots = [2 * a + (1 - k) if first else 2 * (1 - k) + a for a in range(2)]
            self.sends_to_self = [(self.dest_row == y) & (x == a) for a in range(2)]
            self.gets_from_self = [(x == a) if first else ((x == y) & (y == a)) for a in range(2)]
            self.relays = None if first else x == y
            self.sends_across = [False if first else (x != y) & (a == y) for a in range(2)]

        def copy(self, a, h, recv):
            return remote(
                r_xs.at[h], r_xt.at[self.my_slot, h], gs_sem.at[a, h], gr_sem.at[recv, h], self.dest_row, 2 * a + k
            )

        def across(self, a, h):
            return remote(r_xs.at[h], r_hand.at[h], gs_sem.at[a, h], hr_sem.at[h], y, 2 * (1 - x) + k)

        def hand_on(self, h):
            return remote(r_hand.at[h], r_xt.at[2 * k + y, h], hs_sem.at[h], gr_sem.at[y, h], 1 - y, col)

        def forward(self, a, h, slots):
            ref = r_xt.at[slots[a], h]
            return remote(ref, ref, fs_sem.at[a, h], fr_sem.at[a, h], y, mate)

        def start(self, h):
            for a in range(2):

                @pl.when(self.sends_to_self[a])
                def _():
                    r_xt[self.my_slot, h] = r_xs[h]

                if self.relays is not None:

                    @pl.when(self.sends_across[a])
                    def _():
                        self.across(a, h).start()

                @pl.when(jnp.logical_not(self.sends_to_self[a] | self.sends_across[a]))
                def _():
                    self.copy(a, h, self.src).start()

        def finish(self):
            for h in range(CHUNKS):
                if self.relays is not None:

                    @pl.when(self.relays)
                    def _():
                        self.across(0, h).wait_recv()
                        self.hand_on(h).start()

                for a in range(2):

                    @pl.when(jnp.logical_not(self.gets_from_self[a]))
                    def _():
                        self.copy(0, h, a).wait_recv()

                    self.forward(a, h, self.slots).start()
            for h in range(CHUNKS):
                for a in range(2):
                    self.forward(a, h, self.other_slots).wait_recv()

        def drain(self):
            for h in range(CHUNKS):
                for a in range(2):
                    self.forward(a, h, self.slots).wait_send()

                    @pl.when(jnp.logical_not(self.sends_to_self[a]))
                    def _():
                        self.copy(a, h, self.src).wait_send()

                if self.relays is not None:

                    @pl.when(self.relays)
                    def _():
                        self.hand_on(h).wait_send()

    def left_copy(b, slot):
        return remote(l_xs, l_xt.at[slot], lgs_sem.at[b], lgr_sem.at[slot], b, 2 * y + x)

    def left_self(b):
        return (b == y) & (y == x) & (x == k)

    def left_start():
        for b in range(2):

            @pl.when(left_self(b))
            def _():
                l_xt[k] = l_xs[...]

            @pl.when(jnp.logical_not(left_self(b)))
            def _():
                left_copy(b, k).start()

    def left_finish():
        for slot in range(2):

            @pl.when(jnp.logical_not((y == x) & (x == k) & (k == slot)))
            def _():
                left_copy(0, slot).wait_recv()

    def left_drain():
        for b in range(2):

            @pl.when(jnp.logical_not(left_self(b)))
            def _():
                left_copy(b, k).wait_send()

    def left_block(index):
        rows = pl.ds(pl.multiple_of(index * l_nb, l_nb), l_nb)
        return dot_nt(l_xt[0], l_a[rows, :l_nb]) + dot_nt(l_xt[1], l_a[rows, l_nb:])

    def left_mate(a):
        return remote(l_mate_s.at[a], l_mate_r.at[a], lms_sem.at[a], lmr_sem.at[a], y, mate)

    def left_side():
        return remote(l_side_s, l_side_r, lss_sem, lsr_sem, y, 2 * (1 - x) + k)

    def left_multiply():
        for a in (1 - x, x):
            l_mate_s[a] = left_block(2 * a + (1 - k))
            left_mate(a).start()
        l_side_s[...] = left_block(2 * (1 - x) + k)
        l_y[...] = left_block(2 * x + k)

    def left_reduce_start():
        left_mate(1 - x).wait_recv()
        l_side_s[...] = l_side_s[...] + l_mate_r[1 - x]
        left_side().start()
        left_mate(x).wait_recv()
        l_y[...] = l_y[...] + l_mate_r[x]

    def left_reduce_finish():
        left_side().wait_recv()
        l_y[...] = l_y[...] + l_side_r[...]
        left_side().wait_send()
        for a in range(2):
            left_mate(a).wait_send()

    def right_send(t):
        return remote(r_ps.at[t], r_pr.at[t], ps_sem.at[t], pr_sem.at[t], 1 - y, col)

    def right_tile(t):
        r_fetch(t).wait()
        b = t % RING
        total = None
        for s in range(4):
            for h in range(CHUNKS):
                part = dot(r_xt[s, h], r_a[b, s * r_nb + h * piece : s * r_nb + (h + 1) * piece, :])
                total = part if total is None else total + part
        return total

    def right_multiply(own, last):
        def one(i, carry):
            t = i + TILES * own
            res = right_tile(t)
            if own:
                r_y[:, pl.ds(pl.multiple_of(i * tile, tile), tile)] = res
            else:
                r_ps[i] = res
                right_send(i).start()
            ahead = t + RING
            if not (last and own):
                r_fetch(lax.rem(ahead, 2 * TILES)).start()
            return carry

        lax.fori_loop(0, TILES, one, 0)

    def right_reduce_finish():
        for t in range(TILES):
            right_send(t).wait_recv()
            r_y[:, t * tile : (t + 1) * tile] = r_y[:, t * tile : (t + 1) * tile] + r_pr[t]
        for t in range(TILES):
            right_send(t).wait_send()

    def all_reduce(par):
        half, other = pl.ds(pl.multiple_of(k * 64, 64), 64), pl.ds(pl.multiple_of((1 - k) * 64, 64), 64)
        one = remote(g_loc.at[:, other], g_one.at[par], a1s_sem.at[par], a1r_sem.at[par], y, mate)
        one.start()
        one.wait_recv()
        g_sum[...] = g_loc[:, half, :] + g_one[par]
        twos = []
        for q in (2, 1, 0):
            yd = y + ((q + 1) // 2) * (1 - 2 * y)
            xd = x + ((q + 1) % 2) * (1 - 2 * x)
            two = remote(g_sum, g_two.at[par, q], a2s_sem.at[par, q], a2r_sem.at[par, q], yd, 2 * xd + k)
            two.start()
            twos.append(two)
        for two in twos:
            two.wait_recv()
        g_tot[:, half, :] = (g_sum[...] + g_two[par, 0]) + (g_two[par, 1] + g_two[par, 2])
        three = remote(g_tot.at[:, half], g_tot.at[:, half], a3s_sem.at[par], a3r_sem.at[par], y, mate)
        three.start()
        remote(g_tot.at[:, other], g_tot.at[:, other], a3s_sem.at[par], a3r_sem.at[par], y, mate).wait_recv()
        one.wait_send()
        for two in twos:
            two.wait_send()
        three.wait_send()

    def factor():
        for o in ops:
            o.m[...] = g_tot[o.i] / float(o.n)
        inverse_factors([o.m for o in ops])

    def apply_piece(o, lhs, start, width):
        high, mid, low = split(o.y[:, start : start + width])
        rhs = jnp.concatenate([high, high, mid, mid, low, high], axis=0)
        return dot(lhs, rhs)

    def apply_lhs(o):
        high, mid, low = split(o.m[...])
        return jnp.concatenate([high, mid, high, mid, high, low], axis=1)

    def second_gram(o):
        lhs = apply_lhs(o)
        for start in range(0, o.nb, 256):
            res = apply_piece(o, lhs, start, 256)
            o.y[:, start : start + 256] = res
            parts = split(res)
            for q in range(3):
                o.sp[q * S : (q + 1) * S, start : start + 256] = parts[q]
        both = dot_nt(o.sp[: 2 * S, :], o.sp[: 2 * S, :])
        cross = dot_nt(o.sp[:S, :], o.sp[2 * S :, :])
        g_loc[o.i] = both[:S, :S] + ((both[:S, S:] + both[S:, :S]) + (both[S:, S:] + (cross + cross.T)))

    def rayleigh(o, basis):
        g_loc[o.i] = lax.dot_general(basis, o.y[...], NT, precision=lax.Precision.HIGHEST, preferred_element_type=F32)

    def new_basis(gather):
        lhs = apply_lhs(right)
        for h in range(CHUNKS):
            for start in range(h * piece, (h + 1) * piece, 256):
                res = apply_piece(right, lhs, start, 256)
                r_y[:, start : start + 256] = res
                r_xs[h, :, start - h * piece : start - h * piece + 256] = res.astype(BF16)
            gather.start(h)
        lhs = apply_lhs(left)
        for start in range(0, l_nb, 256):
            res = apply_piece(left, lhs, start, 256)
            l_y[:, start : start + 256] = res
            l_xs[:, start : start + 256] = res.astype(BF16)
        left_start()

    def multiply(gather, last):
        gather.finish()
        right_multiply(0, last)
        left_finish()
        left_multiply()
        right_multiply(1, last)
        left_reduce_start()
        right_reduce_finish()
        left_reduce_finish()
        gather.drain()
        left_drain()

    first, later = Gather(True), Gather(False)
    for h in range(CHUNKS):
        for b in range(piece // S):
            r_xs[h, :, b * S : (b + 1) * S] = r_start[h * piece + b * S : h * piece + (b + 1) * S, :].T.astype(BF16)
        first.start(h)
    for b in range(l_nb // S):
        l_xs[:, b * S : (b + 1) * S] = l_start[b * S : (b + 1) * S, :].T.astype(BF16)
    left_start()
    first.finish()
    first.drain()
    l_load.wait()

    class Ready:
        def finish(self):
            pass

        def drain(self):
            pass

    def sweep(i, carry):
        multiply(Ready(), False)
        for o in ops:
            half = o.y[...].astype(BF16)
            g_loc[o.i] = dot_nt(half, half)
        all_reduce(0)
        factor()
        for o in ops:
            second_gram(o)
        all_reduce(1)
        factor()
        new_basis(later)
        later.finish()
        later.drain()
        return carry

    lax.fori_loop(0, SWEEPS, sweep, 0)

    stays = (x == y) & (col == 2 * k + y)
    home = remote(r_keep.at[0], r_keep.at[1], xs_sem, xr_sem, x, 2 * k + y)
    r_keep[0] = r_y[...]

    @pl.when(stays)
    def _():
        r_keep[1] = r_y[...]

    @pl.when(jnp.logical_not(stays))
    def _():
        home.start()

    l_out[...] = l_y[...]
    multiply(Ready(), True)
    rayleigh(left, l_out[...])
    rayleigh(right, r_keep[0])
    all_reduce(0)
    for o in ops:
        ray_out[o.i] = g_tot[o.i] / float(o.n)

    @pl.when(jnp.logical_not(stays))
    def _():
        home.wait_recv()
        home.wait_send()

    r_out[...] = r_keep[1]


def finish_kernel(l_in, r_in, ray_in, l_out, l_ray, r_out, r_ray):
    for src, dst in ((l_in, l_out), (r_in, r_out)):
        for b in range(dst.shape[0] // S):
            dst[b * S : (b + 1) * S, :] = src[:, b * S : (b + 1) * S].T
    l_ray[...] = ray_in[0]
    r_ray[...] = ray_in[1]


def solution(mesh):
    def local_program(left_op, left_start, right_op, right_start):
        l_nb, r_nb = left_op.shape[0] // 4, right_op.shape[0] // 4
        dma = pltpu.SemaphoreType.DMA
        vmem = pl.BlockSpec(memory_space=pltpu.VMEM)
        hbm = pl.BlockSpec(memory_space=pl.ANY)
        shape = jax.ShapeDtypeStruct
        left_t, right_t, rayleigh = pl.pallas_call(
            kernel,
            out_shape=(shape((S, l_nb), F32), shape((S, r_nb), F32), shape((2, S, S), F32)),
            in_specs=[hbm, vmem, hbm, vmem],
            out_specs=(vmem, vmem, vmem),
            scratch_shapes=[
                pltpu.VMEM(left_op.shape, BF16),
                pltpu.VMEM((RING, right_op.shape[0], r_nb // TILES), BF16),
                pltpu.VMEM((S, l_nb), BF16),
                pltpu.VMEM((2, S, l_nb), BF16),
                pltpu.VMEM((2, S, l_nb), F32),
                pltpu.VMEM((2, S, l_nb), F32),
                pltpu.VMEM((S, l_nb), F32),
                pltpu.VMEM((S, l_nb), F32),
                pltpu.VMEM((S, l_nb), F32),
                pltpu.VMEM((S, S), F32),
                pltpu.VMEM((3 * S, l_nb), BF16),
                pltpu.VMEM((CHUNKS, S, r_nb // CHUNKS), BF16),
                pltpu.VMEM((4, CHUNKS, S, r_nb // CHUNKS), BF16),
                pltpu.VMEM((CHUNKS, S, r_nb // CHUNKS), BF16),
                pltpu.VMEM((TILES, S, r_nb // TILES), F32),
                pltpu.VMEM((TILES, S, r_nb // TILES), F32),
                pltpu.VMEM((S, r_nb), F32),
                pltpu.VMEM((S, S), F32),
                pltpu.VMEM((3 * S, r_nb), BF16),
                pltpu.VMEM((2, S, r_nb), F32),
                pltpu.VMEM((2, S, S), F32),
                pltpu.VMEM((2, 2, 64, S), F32),
                pltpu.VMEM((2, 64, S), F32),
                pltpu.VMEM((2, 3, 2, 64, S), F32),
                pltpu.VMEM((2, S, S), F32),
                dma, dma((RING,)),
                dma((2, CHUNKS)), dma((2, CHUNKS)), dma((2, CHUNKS)), dma((2, CHUNKS)), dma((CHUNKS,)), dma((CHUNKS,)),
                dma((TILES,)), dma((TILES,)), dma, dma,
                dma((2,)), dma((2,)), dma((2,)), dma((2,)), dma, dma,
                dma((2,)), dma((2,)), dma((2, 3)), dma((2, 3)), dma((2,)), dma((2,)),
            ],
            compiler_params=pltpu.CompilerParams(has_side_effects=True, vmem_limit_bytes=64 * 1024 * 1024 - 65536),
        )(left_op, left_start, right_op, right_start)
        left_basis, left_ray, right_basis, right_ray = pl.pallas_call(
            finish_kernel,
            out_shape=(shape((l_nb, S), F32), shape((S, S), F32), shape((r_nb, S), F32), shape((S, S), F32)),
            in_specs=[vmem] * 3,
            out_specs=(vmem,) * 4,
        )(left_t, right_t, rayleigh)
        return left_basis, left_ray, right_basis, right_ray

    op_spec = P(("batch", "row"), "col")
    vec_spec = P(("batch", "row", "col"), None)
    small_spec = P("batch", None)
    return jax.shard_map(
        local_program, mesh=mesh, in_specs=(op_spec, vec_spec, op_spec, vec_spec),
        out_specs=(vec_spec, small_spec, vec_spec, small_spec), check_vma=False,
    )
```

```python
import jax
import jax.numpy as jnp
from jax import lax
from jax.experimental import pallas as pl
from jax.experimental.pallas import tpu as pltpu
from jax.sharding import PartitionSpec as P

SWEEPS = 4
S = 128
RING = 4
TILES = 4
CHUNKS = 2
PANEL = 16
MESH = pl.DeviceIdType.MESH
F32, BF16 = jnp.float32, jnp.bfloat16
NT = (((1,), (1,)), ((), ()))
TN = (((0,), (0,)), ((), ()))


def dot(lhs, rhs):
    return jnp.dot(lhs, rhs, preferred_element_type=F32)


def dot_nt(lhs, rhs):
    return lax.dot_general(lhs, rhs, NT, preferred_element_type=F32)


def split(value):
    high = value.astype(BF16)
    rest = value - high.astype(F32)
    mid = rest.astype(BF16)
    low = (rest - mid.astype(F32)).astype(BF16)
    return high, mid, low


def remote(src, dst, send_sem, recv_sem, row, col):
    return pltpu.make_async_remote_copy(
        src_ref=src, dst_ref=dst, send_sem=send_sem, recv_sem=recv_sem,
        device_id={"row": row, "col": col}, device_id_type=MESH,
    )


def inverse_factor(ref):
    sub = lax.broadcasted_iota(jnp.int32, (PANEL, S), 0)
    lane = lax.broadcasted_iota(jnp.int32, (PANEL, S), 1)

    tall_row = lax.broadcasted_iota(jnp.int32, (S, S), 0)
    tall_lane = lax.broadcasted_iota(jnp.int32, (S, S), 1)

    def panel(p, carry):
        k0 = pl.multiple_of(p * PANEL, PANEL)
        inside = (tall_lane >= k0) & (tall_lane < k0 + PANEL) & (tall_row >= k0 + PANEL)
        at = lane - k0
        rows = ref[pl.ds(k0, PANEL), :]
        heads = jnp.stack(
            [
                jnp.broadcast_to(jnp.sum(jnp.where(at == j, rows, 0.0), axis=1, keepdims=True), (PANEL, S))
                for j in range(PANEL)
            ]
        )
        high, mid, low = split(jnp.where(at >= PANEL, rows, 0.0))
        cols = jnp.concatenate([high, mid, high, mid, high, low], axis=0)
        rows = jnp.where((at >= 0) & (at < PANEL), jnp.where(at == sub, 1.0, 0.0), rows)
        done = rows
        piv = heads[0, 0:1, :]
        for j in range(PANEL):
            here = sub == j
            root = lax.rsqrt(piv)
            inv = root * root
            done = jnp.where(here, rows * root, done)
            mult = jnp.where(here, 0.0, heads[0])
            if j < PANEL - 1:
                head_rows = heads[1:, j : j + 1, :] * inv
                piv = heads[1, j + 1 : j + 2, :] - heads[0, j + 1 : j + 2, :] * head_rows[0]
                heads = jnp.where(here[None], head_rows, heads[1:] - mult[None] * head_rows)
            scaled = rows[j : j + 1, :] * inv
            rows = jnp.where(here, scaled, rows - mult * scaled)
        high, mid, low = split(rows)
        rhs = jnp.concatenate([high, high, mid, mid, low, high], axis=0)
        change = lax.dot_general(cols, rhs, TN, preferred_element_type=F32)
        ref[...] = jnp.where(inside, 0.0, ref[...]) - change
        ref[pl.ds(k0, PANEL), :] = done
        return carry

    lax.fori_loop(0, S // PANEL, panel, 0)


class Op:
    def __init__(self, **refs):
        self.__dict__.update(refs)


def kernel(
    l_op, l_start, r_op, r_start,
    l_out, r_out, ray_out,
    l_a, r_a,
    l_xs, l_xt, l_mate_s, l_mate_r, l_side_s, l_side_r, l_hand, l_y, l_sp,
    r_xs, r_xt, r_ps, r_pr, r_y, r_sp, r_keep,
    g_loc, g_one, g_sum, g_two, g_m, g_fac,
    l_asem, r_asem,
    gs_sem, gr_sem, fs_sem, fr_sem, ps_sem, pr_sem, xs_sem, xr_sem,
    lgs_sem, lgr_sem, lhs_sem, lhr_sem, lms_sem, lmr_sem, lss_sem, lsr_sem,
    a1s_sem, a1r_sem, a2s_sem, a2r_sem, a3s_sem, a3r_sem,
):
    y = lax.axis_index("row")
    col = lax.axis_index("col")
    x = col // 2
    k = col % 2
    mate = x * 2 + (1 - k)
    l_n, r_n = l_op.shape[0] * 2, r_op.shape[0] * 2
    l_nb, r_nb = l_n // 8, r_n // 8
    tile = r_nb // TILES
    piece = r_nb // CHUNKS

    left = Op(i=0, n=l_n, nb=l_nb, y=l_y, sp=l_sp)
    right = Op(i=1, n=r_n, nb=r_nb, y=r_y, sp=r_sp)
    ops = [left, right]

    l_load = pltpu.make_async_copy(l_op, l_a, l_asem)
    l_load.start()

    def r_fetch(t):
        half = jnp.where(t < TILES, 1 - y, y)
        start = pl.multiple_of(half * r_nb + (t % TILES) * tile, tile)
        return pltpu.make_async_copy(r_op.at[:, pl.ds(start, tile)], r_a.at[t % RING], r_asem.at[t % RING])

    for t in range(RING):
        r_fetch(t).start()

    class Gather:
        def __init__(self, first):
            self.dest_row = y if first else x
            self.my_slot = 2 * x + k if first else 2 * k + y
            self.src = x if first else y
            self.slots = [2 * a + k if first else 2 * k + a for a in range(2)]
            self.other_slots = [2 * a + (1 - k) if first else 2 * (1 - k) + a for a in range(2)]
            self.sends_to_self = [(self.dest_row == y) & (x == a) for a in range(2)]
            self.gets_from_self = [(x == a) if first else ((x == y) & (y == a)) for a in range(2)]

        def copy(self, a, h, recv):
            return remote(
                r_xs.at[h], r_xt.at[self.my_slot, h], gs_sem.at[a, h], gr_sem.at[recv, h], self.dest_row, 2 * a + k
            )

        def forward(self, a, h, slots):
            ref = r_xt.at[slots[a], h]
            return remote(ref, ref, fs_sem.at[a, h], fr_sem.at[a, h], y, mate)

        def start(self, h):
            for a in range(2):

                @pl.when(self.sends_to_self[a])
                def _():
                    r_xt[self.my_slot, h] = r_xs[h]

                @pl.when(jnp.logical_not(self.sends_to_self[a]))
                def _():
                    self.copy(a, h, self.src).start()

        def finish(self):
            for h in range(CHUNKS):
                for a in range(2):

                    @pl.when(jnp.logical_not(self.gets_from_self[a]))
                    def _():
                        self.copy(0, h, a).wait_recv()

                    self.forward(a, h, self.slots).start()
            for h in range(CHUNKS):
                for a in range(2):
                    self.forward(a, h, self.other_slots).wait_recv()

        def drain(self):
            for h in range(CHUNKS):
                for a in range(2):
                    self.forward(a, h, self.slots).wait_send()

                    @pl.when(jnp.logical_not(self.sends_to_self[a]))
                    def _():
                        self.copy(a, h, self.src).wait_send()

    def left_copy(b, slot):
        return remote(l_xs, l_xt.at[slot], lgs_sem.at[b], lgr_sem.at[slot], b, 2 * y + x)

    def left_across(b):
        return remote(l_xs, l_hand, lgs_sem.at[b], lhr_sem, 1 - y, col)

    def left_hand_on():
        return remote(l_hand, l_xt.at[k], lhs_sem, lgr_sem.at[k], y, 2 * (1 - x) + x)

    def left_self(b):
        return (b == y) & (y == x) & (x == k)

    def left_start():
        for b in (1 - y, y):
            across = (b != y) & (x != y)

            @pl.when(left_self(b))
            def _():
                l_xt[k] = l_xs[...]

            @pl.when(across)
            def _():
                left_across(b).start()

            @pl.when(jnp.logical_not(left_self(b) | across))
            def _():
                left_copy(b, k).start()

    def left_relay():
        @pl.when(x == y)
        def _():
            left_across(0).wait_recv()
            left_hand_on().start()

    def left_finish():
        for slot in range(2):

            @pl.when(jnp.logical_not((y == x) & (x == k) & (k == slot)))
            def _():
                left_copy(0, slot).wait_recv()

    def left_drain():
        for b in range(2):

            @pl.when(jnp.logical_not(left_self(b)))
            def _():
                left_copy(b, k).wait_send()

        @pl.when(x == y)
        def _():
            left_hand_on().wait_send()

    def left_block(index):
        rows = pl.ds(pl.multiple_of(index * l_nb, l_nb), l_nb)
        return dot_nt(l_xt[0], l_a[rows, :l_nb]) + dot_nt(l_xt[1], l_a[rows, l_nb:])

    def left_mate(a):
        return remote(l_mate_s.at[a], l_mate_r.at[a], lms_sem.at[a], lmr_sem.at[a], y, mate)

    def left_side():
        return remote(l_side_s, l_side_r, lss_sem, lsr_sem, y, 2 * (1 - x) + k)

    def left_multiply():
        for a in (1 - x, x):
            l_mate_s[a] = left_block(2 * a + (1 - k))
            left_mate(a).start()
        l_side_s[...] = left_block(2 * (1 - x) + k)
        l_y[...] = left_block(2 * x + k)

    def left_reduce_start():
        left_mate(1 - x).wait_recv()
        l_side_s[...] = l_side_s[...] + l_mate_r[1 - x]
        left_side().start()
        left_mate(x).wait_recv()
        l_y[...] = l_y[...] + l_mate_r[x]

    def left_reduce_finish():
        left_side().wait_recv()
        l_y[...] = l_y[...] + l_side_r[...]
        left_side().wait_send()
        for a in range(2):
            left_mate(a).wait_send()

    def right_send(t):
        return remote(r_ps.at[t], r_pr.at[t], ps_sem.at[t], pr_sem.at[t], 1 - y, col)

    def right_tile(t):
        r_fetch(t).wait()
        b = t % RING
        total = None
        for s in range(4):
            for h in range(CHUNKS):
                part = dot(r_xt[s, h], r_a[b, s * r_nb + h * piece : s * r_nb + (h + 1) * piece, :])
                total = part if total is None else total + part
        return total

    def right_multiply(own, last):
        def one(i, carry):
            t = i + TILES * own
            res = right_tile(t)
            if own:
                r_y[:, pl.ds(pl.multiple_of(i * tile, tile), tile)] = res
            else:
                r_ps[i] = res
                right_send(i).start()
            ahead = t + RING
            if not (last and own):
                r_fetch(lax.rem(ahead, 2 * TILES)).start()
            return carry

        lax.fori_loop(0, TILES, one, 0)

    def right_reduce_finish():
        for t in range(TILES):
            right_send(t).wait_recv()
            r_y[:, t * tile : (t + 1) * tile] = r_y[:, t * tile : (t + 1) * tile] + r_pr[t]
        for t in range(TILES):
            right_send(t).wait_send()

    low_lane = lax.broadcasted_iota(jnp.int32, (32, S), 1)
    tall_row = lax.broadcasted_iota(jnp.int32, (S, S), 0)
    tall_lane = lax.broadcasted_iota(jnp.int32, (S, S), 1)
    count = jnp.where(k == 0, float(l_n), float(r_n))

    def pack(i, gram):
        g_loc[i, :64, :] = gram[:64]
        g_loc[i, 64:96, :] = jnp.where(low_lane < 64, pltpu.roll(gram[64:96], 64, axis=1), gram[96:])

    def sum_across(par, rows, after_sends):
        part = pl.ds(0, rows)
        one = remote(g_loc.at[1 - k, part], g_one.at[par, part], a1s_sem.at[par], a1r_sem.at[par], y, mate)
        one.start()
        one.wait_recv()
        g_sum[part, :] = g_loc[k, part, :] + g_one[par, part, :]
        twos = []
        for q in (2, 1, 0):
            yd = y + ((q + 1) // 2) * (1 - 2 * y)
            xd = x + ((q + 1) % 2) * (1 - 2 * x)
            two = remote(
                g_sum.at[part], g_two.at[par, q, part], a2s_sem.at[par, q], a2r_sem.at[par, q], yd, 2 * xd + k
            )
            two.start()
            twos.append(two)
        after_sends()
        for two in twos:
            two.wait_recv()
        total = (g_sum[part, :] + g_two[par, 0, part, :]) + (g_two[par, 1, part, :] + g_two[par, 2, part, :])
        one.wait_send()
        for two in twos:
            two.wait_send()
        return total / count

    def hand_over(par):
        mine, other = g_fac.at[k], g_fac.at[1 - k]
        copy = remote(mine, mine, a3s_sem.at[par], a3r_sem.at[par], y, mate)
        copy.start()
        remote(other, other, a3s_sem.at[par], a3r_sem.at[par], y, mate).wait_recv()
        copy.wait_send()

    def factor(par):
        gram = sum_across(par, 96, lambda: None)
        g_m[:64, :] = gram[:64]
        g_m[64:96, :] = pltpu.roll(gram[64:], 64, axis=1)
        g_m[96:, :] = gram[64:]
        inverse_factor(g_m)
        g_fac[k] = jnp.where(tall_lane <= tall_row, g_m[...], 0.0)
        hand_over(par)

    def apply_piece(o, lhs, start, width):
        high, mid, low = split(o.y[:, start : start + width])
        rhs = jnp.concatenate([high, high, mid, mid, low, high], axis=0)
        return dot(lhs, rhs)

    def apply_lhs(o):
        high, mid, low = split(g_fac[o.i])
        return jnp.concatenate([high, mid, high, mid, high, low], axis=1)

    def second_gram(o):
        lhs = apply_lhs(o)
        for start in range(0, o.nb, 256):
            res = apply_piece(o, lhs, start, 256)
            o.y[:, start : start + 256] = res
            parts = split(res)
            for q in range(3):
                o.sp[q * S : (q + 1) * S, start : start + 256] = parts[q]
        both = dot_nt(o.sp[: 2 * S, :], o.sp[: 2 * S, :])
        cross = dot_nt(o.sp[:S, :], o.sp[2 * S :, :])
        pack(o.i, both[:S, :S] + ((both[:S, S:] + both[S:, :S]) + (both[S:, S:] + (cross + cross.T))))

    def rayleigh(o, basis):
        g_loc[o.i] = lax.dot_general(basis, o.y[...], NT, precision=lax.Precision.HIGHEST, preferred_element_type=F32)

    def new_basis(gather):
        lhs = apply_lhs(right)
        for h in range(CHUNKS):
            for start in range(h * piece, (h + 1) * piece, 256):
                res = apply_piece(right, lhs, start, 256)
                r_y[:, start : start + 256] = res
                r_xs[h, :, start - h * piece : start - h * piece + 256] = res.astype(BF16)
            gather.start(h)
        lhs = apply_lhs(left)
        for start in range(0, l_nb, 256):
            res = apply_piece(left, lhs, start, 256)
            l_y[:, start : start + 256] = res
            l_xs[:, start : start + 256] = res.astype(BF16)
        left_start()

    def multiply(last):
        right_multiply(0, last)
        left_relay()
        right_multiply(1, last)
        left_finish()
        left_multiply()
        left_reduce_start()
        right_reduce_finish()
        left_reduce_finish()
        left_drain()

    first, later = Gather(True), Gather(False)
    for h in range(CHUNKS):
        for b in range(piece // S):
            r_xs[h, :, b * S : (b + 1) * S] = r_start[h * piece + b * S : h * piece + (b + 1) * S, :].T.astype(BF16)
        first.start(h)
    for b in range(l_nb // S):
        l_xs[:, b * S : (b + 1) * S] = l_start[b * S : (b + 1) * S, :].T.astype(BF16)
    left_start()
    first.finish()
    first.drain()
    l_load.wait()

    def sweep(i, carry):
        multiply(False)
        for o in ops:
            half = o.y[...].astype(BF16)
            pack(o.i, dot_nt(half, half))
        factor(0)
        for o in ops:
            second_gram(o)
        factor(1)
        new_basis(later)
        later.finish()
        later.drain()
        return carry

    lax.fori_loop(0, SWEEPS, sweep, 0)

    stays = (x == y) & (col == 2 * k + y)
    home = remote(r_keep.at[0], r_keep.at[1], xs_sem, xr_sem, x, 2 * k + y)
    r_keep[0] = r_y[...]

    def start_home():
        @pl.when(stays)
        def _():
            r_keep[1] = r_keep[0]

        @pl.when(jnp.logical_not(stays))
        def _():
            home.start()

    l_out[...] = l_y[...]
    multiply(True)
    rayleigh(left, l_out[...])
    rayleigh(right, r_keep[0])
    g_fac[k] = sum_across(2, S, start_home)
    hand_over(2)
    ray_out[...] = g_fac[...]

    @pl.when(jnp.logical_not(stays))
    def _():
        home.wait_recv()
        home.wait_send()

    r_out[...] = r_keep[1]


def finish_kernel(l_in, r_in, ray_in, l_out, l_ray, r_out, r_ray):
    for src, dst in ((l_in, l_out), (r_in, r_out)):
        for b in range(dst.shape[0] // S):
            dst[b * S : (b + 1) * S, :] = src[:, b * S : (b + 1) * S].T
    l_ray[...] = ray_in[0]
    r_ray[...] = ray_in[1]


def solution(mesh):
    def local_program(left_op, left_start, right_op, right_start):
        l_nb, r_nb = left_op.shape[0] // 4, right_op.shape[0] // 4
        dma = pltpu.SemaphoreType.DMA
        vmem = pl.BlockSpec(memory_space=pltpu.VMEM)
        hbm = pl.BlockSpec(memory_space=pl.ANY)
        shape = jax.ShapeDtypeStruct
        left_t, right_t, rayleigh = pl.pallas_call(
            kernel,
            out_shape=(shape((S, l_nb), F32), shape((S, r_nb), F32), shape((2, S, S), F32)),
            in_specs=[hbm, vmem, hbm, vmem],
            out_specs=(vmem, vmem, vmem),
            scratch_shapes=[
                pltpu.VMEM(left_op.shape, BF16),
                pltpu.VMEM((RING, right_op.shape[0], r_nb // TILES), BF16),
                pltpu.VMEM((S, l_nb), BF16),
                pltpu.VMEM((2, S, l_nb), BF16),
                pltpu.VMEM((2, S, l_nb), F32),
                pltpu.VMEM((2, S, l_nb), F32),
                pltpu.VMEM((S, l_nb), F32),
                pltpu.VMEM((S, l_nb), F32),
                pltpu.VMEM((S, l_nb), BF16),
                pltpu.VMEM((S, l_nb), F32),
                pltpu.VMEM((3 * S, l_nb), BF16),
                pltpu.VMEM((CHUNKS, S, r_nb // CHUNKS), BF16),
                pltpu.VMEM((4, CHUNKS, S, r_nb // CHUNKS), BF16),
                pltpu.VMEM((TILES, S, r_nb // TILES), F32),
                pltpu.VMEM((TILES, S, r_nb // TILES), F32),
                pltpu.VMEM((S, r_nb), F32),
                pltpu.VMEM((3 * S, r_nb), BF16),
                pltpu.VMEM((2, S, r_nb), F32),
                pltpu.VMEM((2, S, S), F32),
                pltpu.VMEM((3, S, S), F32),
                pltpu.VMEM((S, S), F32),
                pltpu.VMEM((3, 3, S, S), F32),
                pltpu.VMEM((S, S), F32),
                pltpu.VMEM((2, S, S), F32),
                dma, dma((RING,)),
                dma((2, CHUNKS)), dma((2, CHUNKS)), dma((2, CHUNKS)), dma((2, CHUNKS)),
                dma((TILES,)), dma((TILES,)), dma, dma,
                dma((2,)), dma((2,)), dma, dma, dma((2,)), dma((2,)), dma, dma,
                dma((3,)), dma((3,)), dma((3, 3)), dma((3, 3)), dma((3,)), dma((3,)),
            ],
            compiler_params=pltpu.CompilerParams(has_side_effects=True, vmem_limit_bytes=64 * 1024 * 1024 - 65536),
        )(left_op, left_start, right_op, right_start)
        left_basis, left_ray, right_basis, right_ray = pl.pallas_call(
            finish_kernel,
            out_shape=(shape((l_nb, S), F32), shape((S, S), F32), shape((r_nb, S), F32), shape((S, S), F32)),
            in_specs=[vmem] * 3,
            out_specs=(vmem,) * 4,
        )(left_t, right_t, rayleigh)
        return left_basis, left_ray, right_basis, right_ray

    op_spec = P(("batch", "row"), "col")
    vec_spec = P(("batch", "row", "col"), None)
    small_spec = P("batch", None)
    return jax.shard_map(
        local_program, mesh=mesh, in_specs=(op_spec, vec_spec, op_spec, vec_spec),
        out_specs=(vec_spec, small_spec, vec_spec, small_spec), check_vma=False,
    )
```

```python
import functools

import jax
import jax.numpy as jnp
from jax import lax
from jax.experimental import pallas as pl
from jax.experimental.pallas import tpu as pltpu
from jax.sharding import PartitionSpec as P

SWEEPS = 4
S = 128
RING = 4
TILES = 4
CHUNKS = 2
PANEL = 16
MESH = pl.DeviceIdType.MESH
F32, BF16 = jnp.float32, jnp.bfloat16
NT = (((1,), (1,)), ((), ()))
TN = (((0,), (0,)), ((), ()))


def dot(lhs, rhs):
    return jnp.dot(lhs, rhs, preferred_element_type=F32)


def dot_nt(lhs, rhs):
    return lax.dot_general(lhs, rhs, NT, preferred_element_type=F32)


def split(value):
    high = value.astype(BF16)
    rest = value - high.astype(F32)
    mid = rest.astype(BF16)
    low = (rest - mid.astype(F32)).astype(BF16)
    return high, mid, low


def remote(src, dst, send_sem, recv_sem, row, col):
    return pltpu.make_async_remote_copy(
        src_ref=src, dst_ref=dst, send_sem=send_sem, recv_sem=recv_sem,
        device_id={"row": row, "col": col}, device_id_type=MESH,
    )


def inverse_factor(ref):
    sub = lax.broadcasted_iota(jnp.int32, (PANEL, S), 0)
    lane = lax.broadcasted_iota(jnp.int32, (PANEL, S), 1)

    tall_row = lax.broadcasted_iota(jnp.int32, (S, S), 0)
    tall_lane = lax.broadcasted_iota(jnp.int32, (S, S), 1)

    def panel(p, carry):
        k0 = pl.multiple_of(p * PANEL, PANEL)
        inside = (tall_lane >= k0) & (tall_lane < k0 + PANEL) & (tall_row >= k0 + PANEL)
        at = lane - k0
        rows = ref[pl.ds(k0, PANEL), :]
        heads = jnp.stack(
            [
                jnp.broadcast_to(jnp.sum(jnp.where(at == j, rows, 0.0), axis=1, keepdims=True), (PANEL, S))
                for j in range(PANEL)
            ]
        )
        high, mid, low = split(jnp.where(at >= PANEL, rows, 0.0))
        cols = jnp.concatenate([high, mid, high, mid, high, low], axis=0)
        rows = jnp.where((at >= 0) & (at < PANEL), jnp.where(at == sub, 1.0, 0.0), rows)
        done = rows
        piv = heads[0, 0:1, :]
        for j in range(PANEL):
            here = sub == j
            root = lax.rsqrt(piv)
            inv = root * root
            done = jnp.where(here, rows * root, done)
            mult = jnp.where(here, 0.0, heads[0])
            if j < PANEL - 1:
                head_rows = heads[1:, j : j + 1, :] * inv
                piv = heads[1, j + 1 : j + 2, :] - heads[0, j + 1 : j + 2, :] * head_rows[0]
                heads = jnp.where(here[None], head_rows, heads[1:] - mult[None] * head_rows)
            scaled = rows[j : j + 1, :] * inv
            rows = jnp.where(here, scaled, rows - mult * scaled)
        high, mid, low = split(rows)
        rhs = jnp.concatenate([high, high, mid, mid, low, high], axis=0)
        change = lax.dot_general(cols, rhs, TN, preferred_element_type=F32)
        ref[...] = jnp.where(inside, 0.0, ref[...]) - change
        ref[pl.ds(k0, PANEL), :] = done
        return carry

    lax.fori_loop(0, S // PANEL, panel, 0)


class Op:
    def __init__(self, **refs):
        self.__dict__.update(refs)


def kernel(
    l_op, l_start, r_op, r_start,
    l_out, r_out, ray_out,
    l_a, r_a,
    l_xs, l_xt, l_mate_s, l_mate_r, l_side_s, l_side_r, l_hand, l_y, l_sp,
    r_xs, r_xt, r_ps, r_pr, r_y, r_sp, r_keep,
    g_loc, g_one, g_sum, g_two, g_m, g_fac,
    l_asem, r_asem,
    gs_sem, gr_sem, fs_sem, fr_sem, ps_sem, pr_sem, xs_sem, xr_sem, es_sem, er_sem,
    lgs_sem, lgr_sem, lhs_sem, lhr_sem, lms_sem, lmr_sem, lss_sem, lsr_sem,
    a1s_sem, a1r_sem, a2s_sem, a2r_sem, a3s_sem, a3r_sem,
):
    y = lax.axis_index("row")
    col = lax.axis_index("col")
    x = col // 2
    k = col % 2
    mate = x * 2 + (1 - k)
    l_n, r_n = l_op.shape[0] * 2, r_op.shape[0] * 2
    l_nb, r_nb = l_n // 8, r_n // 8
    tile = r_nb // TILES
    piece = r_nb // CHUNKS

    left = Op(i=0, n=l_n, nb=l_nb, y=l_y, sp=l_sp)
    right = Op(i=1, n=r_n, nb=r_nb, y=r_y, sp=r_sp)
    ops = [left, right]

    l_load = pltpu.make_async_copy(l_op, l_a, l_asem)
    l_load.start()

    def r_fetch(t):
        half = jnp.where(t < TILES, 1 - y, y)
        start = pl.multiple_of(half * r_nb + (t % TILES) * tile, tile)
        return pltpu.make_async_copy(r_op.at[:, pl.ds(start, tile)], r_a.at[t % RING], r_asem.at[t % RING])

    for t in range(RING):
        r_fetch(t).start()

    class Gather:
        def __init__(self, first):
            self.dest_row = y if first else x
            self.my_slot = 2 * x + k if first else 2 * k + y
            self.src = x if first else y
            self.slots = [2 * a + k if first else 2 * k + a for a in range(2)]
            self.other_slots = [2 * a + (1 - k) if first else 2 * (1 - k) + a for a in range(2)]
            self.sends_to_self = [(self.dest_row == y) & (x == a) for a in range(2)]
            self.gets_from_self = [(x == a) if first else ((x == y) & (y == a)) for a in range(2)]

        def copy(self, a, h, recv):
            return remote(
                r_xs.at[h], r_xt.at[self.my_slot, h], gs_sem.at[a, h], gr_sem.at[recv, h], self.dest_row, 2 * a + k
            )

        def forward(self, a, h, slots):
            ref = r_xt.at[slots[a], h]
            return remote(ref, ref, fs_sem.at[a, h], fr_sem.at[a, h], y, mate)

        def start(self, h):
            for a in range(2):

                @pl.when(self.sends_to_self[a])
                def _():
                    r_xt[self.my_slot, h] = r_xs[h]

                @pl.when(jnp.logical_not(self.sends_to_self[a]))
                def _():
                    self.copy(a, h, self.src).start()

        def finish(self):
            for h in range(CHUNKS):
                for a in range(2):

                    @pl.when(jnp.logical_not(self.gets_from_self[a]))
                    def _():
                        self.copy(0, h, a).wait_recv()

                    self.forward(a, h, self.slots).start()
            for h in range(CHUNKS):
                for a in range(2):
                    self.forward(a, h, self.other_slots).wait_recv()

        def drain(self):
            for h in range(CHUNKS):
                for a in range(2):
                    self.forward(a, h, self.slots).wait_send()

                    @pl.when(jnp.logical_not(self.sends_to_self[a]))
                    def _():
                        self.copy(a, h, self.src).wait_send()

    def left_copy(b, slot):
        return remote(l_xs, l_xt.at[slot], lgs_sem.at[b], lgr_sem.at[slot], b, 2 * y + x)

    def left_across(b):
        return remote(l_xs, l_hand, lgs_sem.at[b], lhr_sem, 1 - y, col)

    def left_hand_on():
        return remote(l_hand, l_xt.at[k], lhs_sem, lgr_sem.at[k], y, 2 * (1 - x) + x)

    def left_self(b):
        return (b == y) & (y == x) & (x == k)

    def left_start():
        for b in (1 - y, y):
            across = (b != y) & (x != y)

            @pl.when(left_self(b))
            def _():
                l_xt[k] = l_xs[...]

            @pl.when(across)
            def _():
                left_across(b).start()

            @pl.when(jnp.logical_not(left_self(b) | across))
            def _():
                left_copy(b, k).start()

    def left_relay():
        @pl.when(x == y)
        def _():
            left_across(0).wait_recv()
            left_hand_on().start()

    def left_finish():
        for slot in range(2):

            @pl.when(jnp.logical_not((y == x) & (x == k) & (k == slot)))
            def _():
                left_copy(0, slot).wait_recv()

    def left_drain():
        for b in range(2):

            @pl.when(jnp.logical_not(left_self(b)))
            def _():
                left_copy(b, k).wait_send()

        @pl.when(x == y)
        def _():
            left_hand_on().wait_send()

    def left_block(index):
        rows = pl.ds(pl.multiple_of(index * l_nb, l_nb), l_nb)
        return dot_nt(l_xt[0], l_a[rows, :l_nb]) + dot_nt(l_xt[1], l_a[rows, l_nb:])

    def left_mate(a):
        return remote(l_mate_s.at[a], l_mate_r.at[a], lms_sem.at[a], lmr_sem.at[a], y, mate)

    def left_side():
        return remote(l_side_s, l_side_r, lss_sem, lsr_sem, y, 2 * (1 - x) + k)

    def left_multiply():
        l_mate_s[1 - x] = left_block(2 * (1 - x) + (1 - k))
        left_mate(1 - x).start()
        l_side_s[...] = left_block(2 * (1 - x) + k)
        l_mate_s[x] = left_block(2 * x + (1 - k))
        left_mate(x).start()
        left_mate(1 - x).wait_recv()
        l_side_s[...] = l_side_s[...] + l_mate_r[1 - x]
        left_side().start()
        l_y[...] = left_block(2 * x + k)

    def left_reduce_finish():
        left_mate(x).wait_recv()
        l_y[...] = l_y[...] + l_mate_r[x]
        left_side().wait_recv()
        l_y[...] = l_y[...] + l_side_r[...]
        left_side().wait_send()
        for a in range(2):
            left_mate(a).wait_send()

    def right_send(t):
        return remote(r_ps.at[t], r_pr.at[t], ps_sem.at[t], pr_sem.at[t], 1 - y, col)

    def right_tile(t):
        r_fetch(t).wait()
        b = t % RING
        total = None
        for s in range(4):
            for h in range(CHUNKS):
                part = dot(r_xt[s, h], r_a[b, s * r_nb + h * piece : s * r_nb + (h + 1) * piece, :])
                total = part if total is None else total + part
        return total

    def right_multiply(own, last, begin=0, end=TILES):
        def one(i, carry):
            t = i + TILES * own
            res = right_tile(t)
            if own:
                r_y[:, pl.ds(pl.multiple_of(i * tile, tile), tile)] = res
            else:
                r_ps[i] = res
                if not last:
                    right_send(i).start()
            ahead = t + RING
            if not (last and own):
                r_fetch(lax.rem(ahead, 2 * TILES)).start()
            return carry

        lax.fori_loop(begin, end, one, 0)

    def right_reduce_finish():
        for t in range(TILES):
            right_send(t).wait_recv()
            r_y[:, t * tile : (t + 1) * tile] = r_y[:, t * tile : (t + 1) * tile] + r_pr[t]
        for t in range(TILES):
            right_send(t).wait_send()

    low_lane = lax.broadcasted_iota(jnp.int32, (32, S), 1)
    tall_row = lax.broadcasted_iota(jnp.int32, (S, S), 0)
    tall_lane = lax.broadcasted_iota(jnp.int32, (S, S), 1)
    count = jnp.where(k == 0, float(l_n), float(r_n))

    def pack(i, gram):
        g_loc[i, :64, :] = gram[:64]
        g_loc[i, 64:96, :] = jnp.where(low_lane < 64, pltpu.roll(gram[64:96], 64, axis=1), gram[96:])

    def sum_across(par, rows):
        part = pl.ds(0, rows)
        one = remote(g_loc.at[1 - k, part], g_one.at[par, part], a1s_sem.at[par], a1r_sem.at[par], y, mate)
        one.start()
        with jax.named_scope("ar_one"):
            one.wait_recv()
        g_sum[part, :] = g_loc[k, part, :] + g_one[par, part, :]
        twos = []
        for q in (2, 1, 0):
            yd = y + ((q + 1) // 2) * (1 - 2 * y)
            xd = x + ((q + 1) % 2) * (1 - 2 * x)
            two = remote(
                g_sum.at[part], g_two.at[par, q, part], a2s_sem.at[par, q], a2r_sem.at[par, q], yd, 2 * xd + k
            )
            two.start()
            twos.append(two)
        with jax.named_scope("ar_two"):
            for two in twos:
                two.wait_recv()
        total = (g_sum[part, :] + g_two[par, 0, part, :]) + (g_two[par, 1, part, :] + g_two[par, 2, part, :])
        one.wait_send()
        for two in twos:
            two.wait_send()
        return total / count

    def hand_over(par, left_work, right_work):
        mine, other = g_fac.at[k], g_fac.at[1 - k]
        copy = remote(mine, mine, a3s_sem.at[par], a3r_sem.at[par], y, mate)
        back = remote(other, other, a3s_sem.at[par], a3r_sem.at[par], y, mate)
        copy.start()

        @pl.when(k == 0)
        def _():
            left_work()
            back.wait_recv()
            right_work()

        @pl.when(k == 1)
        def _():
            right_work()
            back.wait_recv()
            left_work()

        copy.wait_send()

    def factor(par):
        gram = sum_across(par, 96)
        g_m[:64, :] = gram[:64]
        g_m[64:96, :] = pltpu.roll(gram[64:], 64, axis=1)
        g_m[96:, :] = gram[64:]
        with jax.named_scope("chol"):
            inverse_factor(g_m)
        g_fac[k] = jnp.where(tall_lane <= tall_row, g_m[...], 0.0)

    def apply_piece(o, lhs, start, width):
        high, mid, low = split(o.y[:, start : start + width])
        rhs = jnp.concatenate([high, high, mid, mid, low, high], axis=0)
        return dot(lhs, rhs)

    def apply_lhs(o):
        high, mid, low = split(g_fac[o.i])
        return jnp.concatenate([high, mid, high, mid, high, low], axis=1)

    def second_gram(o):
        lhs = apply_lhs(o)
        for start in range(0, o.nb, 256):
            res = apply_piece(o, lhs, start, 256)
            o.y[:, start : start + 256] = res
            parts = split(res)
            for q in range(3):
                o.sp[q * S : (q + 1) * S, start : start + 256] = parts[q]
        both = dot_nt(o.sp[: 2 * S, :], o.sp[: 2 * S, :])
        cross = dot_nt(o.sp[:S, :], o.sp[2 * S :, :])
        pack(o.i, both[:S, :S] + ((both[:S, S:] + both[S:, :S]) + (both[S:, S:] + (cross + cross.T))))

    def high_dot_nt(lhs, rhs):
        return lax.dot_general(lhs, rhs, NT, precision=lax.Precision.HIGHEST, preferred_element_type=F32)

    def new_left():
        lhs = apply_lhs(left)
        for start in range(0, l_nb, 256):
            res = apply_piece(left, lhs, start, 256)
            l_y[:, start : start + 256] = res
            l_xs[:, start : start + 256] = res.astype(BF16)

    def new_right():
        lhs = apply_lhs(right)
        for h in range(CHUNKS):
            for start in range(h * piece, (h + 1) * piece, 256):
                res = apply_piece(right, lhs, start, 256)
                r_y[:, start : start + 256] = res
                r_xs[h, :, start - h * piece : start - h * piece + 256] = res.astype(BF16)
            later.start(h)

    def multiply(drain, last):
        with jax.named_scope("r_mul0"):
            right_multiply(0, last)
        with jax.named_scope("l_relay"):
            left_relay()
        with jax.named_scope("r_mul1"):
            right_multiply(1, last, 0, 2)
        with jax.named_scope("l_fin"):
            left_finish()
        with jax.named_scope("l_mul"):
            left_multiply()
        with jax.named_scope("r_mul2"):
            right_multiply(1, last, 2, TILES)
        if not last:
            with jax.named_scope("r_red"):
                right_reduce_finish()
        with jax.named_scope("l_red"):
            left_reduce_finish()
        left_drain()
        drain()

    first, later = Gather(True), Gather(False)
    for h in range(CHUNKS):
        for b in range(piece // S):
            r_xs[h, :, b * S : (b + 1) * S] = r_start[h * piece + b * S : h * piece + (b + 1) * S, :].T.astype(BF16)
        first.start(h)
    for b in range(l_nb // S):
        l_xs[:, b * S : (b + 1) * S] = l_start[b * S : (b + 1) * S, :].T.astype(BF16)
    left_start()
    with jax.named_scope("gather_first"):
        first.finish()
    first.drain()
    l_load.wait()

    def sweep(i, carry):
        multiply(functools.partial(pl.when(i > 0), later.drain), False)
        with jax.named_scope("gram1"):
            for o in ops:
                half = o.y[...].astype(BF16)
                pack(o.i, dot_nt(half, half))
        with jax.named_scope("factor0"):
            factor(0)
        with jax.named_scope("gram2"):
            hand_over(0, lambda: second_gram(left), lambda: second_gram(right))
        with jax.named_scope("factor1"):
            factor(1)
        with jax.named_scope("new_basis"):
            hand_over(1, new_left, new_right)
            left_start()
        with jax.named_scope("gather"):
            later.finish()
        return carry

    lax.fori_loop(0, SWEEPS, sweep, 0)

    stays = (x == y) & (k == y)

    def swap(c):
        return remote(r_keep.at[0, c], r_keep.at[1, c], es_sem.at[c], er_sem.at[c], 1 - y, col)

    def home(q, c):
        place = 2 * k + (y if q == 0 else 1 - y)
        return remote(r_keep.at[q, c], r_pr.at[c], xs_sem.at[q, c], xr_sem.at[c], y, place)

    for c in range(TILES):
        r_keep[0, c] = r_y[:, c * tile : (c + 1) * tile]
        swap(c).start()

        @pl.when((x == y) & (k != y))
        def _():
            home(0, c).start()

    l_out[...] = l_y[...]
    with jax.named_scope("last_mul"):
        multiply(later.drain, True)
    with jax.named_scope("ray"):
        g_loc[0] = high_dot_nt(l_out[...], l_y[...])
        total = None
        for c in range(TILES):
            part = high_dot_nt(r_keep[0, c], r_y[:, c * tile : (c + 1) * tile])
            total = part if total is None else total + part
        for c in range(TILES):
            swap(c).wait_recv()

            @pl.when(x == y)
            def _():
                home(1, c).start()

            total = total + high_dot_nt(r_keep[1, c], r_ps[c])
        g_loc[1] = total
    with jax.named_scope("last_sum"):
        g_fac[k] = sum_across(2, S)
    with jax.named_scope("last_hand"):
        hand_over(2, lambda: None, lambda: None)
    ray_out[...] = g_fac[...]
    with jax.named_scope("home"):
        for c in range(TILES):
            swap(c).wait_send()

            @pl.when(x == y)
            def _():
                home(1, c).wait_send()

            @pl.when((x == y) & (k != y))
            def _():
                home(0, c).wait_send()

            @pl.when(stays)
            def _():
                r_out[:, c * tile : (c + 1) * tile] = r_keep[0, c]

            @pl.when(jnp.logical_not(stays))
            def _():
                home(0, c).wait_recv()
                r_out[:, c * tile : (c + 1) * tile] = r_pr[c]


def finish_kernel(l_in, r_in, ray_in, l_out, l_ray, r_out, r_ray):
    for src, dst in ((l_in, l_out), (r_in, r_out)):
        for b in range(dst.shape[0] // S):
            dst[b * S : (b + 1) * S, :] = src[:, b * S : (b + 1) * S].T
    l_ray[...] = ray_in[0]
    r_ray[...] = ray_in[1]


def solution(mesh):
    def local_program(left_op, left_start, right_op, right_start):
        l_nb, r_nb = left_op.shape[0] // 4, right_op.shape[0] // 4
        dma = pltpu.SemaphoreType.DMA
        vmem = pl.BlockSpec(memory_space=pltpu.VMEM)
        hbm = pl.BlockSpec(memory_space=pl.ANY)
        shape = jax.ShapeDtypeStruct
        left_t, right_t, rayleigh = pl.pallas_call(
            kernel,
            out_shape=(shape((S, l_nb), F32), shape((S, r_nb), F32), shape((2, S, S), F32)),
            in_specs=[hbm, vmem, hbm, vmem],
            out_specs=(vmem, vmem, vmem),
            scratch_shapes=[
                pltpu.VMEM(left_op.shape, BF16),
                pltpu.VMEM((RING, right_op.shape[0], r_nb // TILES), BF16),
                pltpu.VMEM((S, l_nb), BF16),
                pltpu.VMEM((2, S, l_nb), BF16),
                pltpu.VMEM((2, S, l_nb), F32),
                pltpu.VMEM((2, S, l_nb), F32),
                pltpu.VMEM((S, l_nb), F32),
                pltpu.VMEM((S, l_nb), F32),
                pltpu.VMEM((S, l_nb), BF16),
                pltpu.VMEM((S, l_nb), F32),
                pltpu.VMEM((3 * S, l_nb), BF16),
                pltpu.VMEM((CHUNKS, S, r_nb // CHUNKS), BF16),
                pltpu.VMEM((4, CHUNKS, S, r_nb // CHUNKS), BF16),
                pltpu.VMEM((TILES, S, r_nb // TILES), F32),
                pltpu.VMEM((TILES, S, r_nb // TILES), F32),
                pltpu.VMEM((S, r_nb), F32),
                pltpu.VMEM((3 * S, r_nb), BF16),
                pltpu.VMEM((2, TILES, S, r_nb // TILES), F32),
                pltpu.VMEM((2, S, S), F32),
                pltpu.VMEM((3, S, S), F32),
                pltpu.VMEM((S, S), F32),
                pltpu.VMEM((3, 3, S, S), F32),
                pltpu.VMEM((S, S), F32),
                pltpu.VMEM((2, S, S), F32),
                dma, dma((RING,)),
                dma((2, CHUNKS)), dma((2, CHUNKS)), dma((2, CHUNKS)), dma((2, CHUNKS)),
                dma((TILES,)), dma((TILES,)), dma((2, TILES)), dma((TILES,)), dma((TILES,)), dma((TILES,)),
                dma((2,)), dma((2,)), dma, dma, dma((2,)), dma((2,)), dma, dma,
                dma((3,)), dma((3,)), dma((3, 3)), dma((3, 3)), dma((3,)), dma((3,)),
            ],
            compiler_params=pltpu.CompilerParams(has_side_effects=True, vmem_limit_bytes=64 * 1024 * 1024 - 65536),
        )(left_op, left_start, right_op, right_start)
        left_basis, left_ray, right_basis, right_ray = pl.pallas_call(
            finish_kernel,
            out_shape=(shape((l_nb, S), F32), shape((S, S), F32), shape((r_nb, S), F32), shape((S, S), F32)),
            in_specs=[vmem] * 3,
            out_specs=(vmem,) * 4,
        )(left_t, right_t, rayleigh)
        return left_basis, left_ray, right_basis, right_ray

    op_spec = P(("batch", "row"), "col")
    vec_spec = P(("batch", "row", "col"), None)
    small_spec = P("batch", None)
    return jax.shard_map(
        local_program, mesh=mesh, in_specs=(op_spec, vec_spec, op_spec, vec_spec),
        out_specs=(vec_spec, small_spec, vec_spec, small_spec), check_vma=False,
    )
```

```python
import functools

import jax
import jax.numpy as jnp
from jax import lax
from jax.experimental import pallas as pl
from jax.experimental.pallas import tpu as pltpu
from jax.sharding import PartitionSpec as P


SWEEPS = 4
S = 128
RING = 4
TILES = 4
CHUNKS = 4
PANEL = 16
MESH = pl.DeviceIdType.MESH
F32, BF16 = jnp.float32, jnp.bfloat16
NT = (((1,), (1,)), ((), ()))
TN = (((0,), (0,)), ((), ()))


def dot(lhs, rhs):
    return jnp.dot(lhs, rhs, preferred_element_type=F32)


def dot_nt(lhs, rhs):
    return lax.dot_general(lhs, rhs, NT, preferred_element_type=F32)


def split(value):
    high = value.astype(BF16)
    rest = value - high.astype(F32)
    mid = rest.astype(BF16)
    low = (rest - mid.astype(F32)).astype(BF16)
    return high, mid, low


def remote(src, dst, send_sem, recv_sem, row, col):
    return pltpu.make_async_remote_copy(
        src_ref=src, dst_ref=dst, send_sem=send_sem, recv_sem=recv_sem,
        device_id={"row": row, "col": col}, device_id_type=MESH,
    )


def inverse_factor(ref):
    sub = lax.broadcasted_iota(jnp.int32, (PANEL, S), 0)
    lane = lax.broadcasted_iota(jnp.int32, (PANEL, S), 1)

    tall_row = lax.broadcasted_iota(jnp.int32, (S, S), 0)
    tall_lane = lax.broadcasted_iota(jnp.int32, (S, S), 1)

    def panel(p, carry):
        k0 = pl.multiple_of(p * PANEL, PANEL)
        inside = (tall_lane >= k0) & (tall_lane < k0 + PANEL) & (tall_row >= k0 + PANEL)
        at = lane - k0
        rows = ref[pl.ds(k0, PANEL), :]
        heads = jnp.stack(
            [
                jnp.broadcast_to(jnp.sum(jnp.where(at == j, rows, 0.0), axis=1, keepdims=True), (PANEL, S))
                for j in range(PANEL)
            ]
        )
        high, mid, low = split(jnp.where(at >= PANEL, rows, 0.0))
        cols = jnp.concatenate([high, mid, high, mid, high, low], axis=0)
        rows = jnp.where((at >= 0) & (at < PANEL), jnp.where(at == sub, 1.0, 0.0), rows)
        done = rows
        piv = heads[0, 0:1, :]
        for j in range(PANEL):
            here = sub == j
            root = lax.rsqrt(piv)
            inv = root * root
            done = jnp.where(here, rows * root, done)
            mult = jnp.where(here, 0.0, heads[0])
            if j < PANEL - 1:
                head_rows = heads[1:, j : j + 1, :] * inv
                piv = heads[1, j + 1 : j + 2, :] - heads[0, j + 1 : j + 2, :] * head_rows[0]
                heads = jnp.where(here[None], head_rows, heads[1:] - mult[None] * head_rows)
            scaled = rows[j : j + 1, :] * inv
            rows = jnp.where(here, scaled, rows - mult * scaled)
        high, mid, low = split(rows)
        rhs = jnp.concatenate([high, high, mid, mid, low, high], axis=0)
        change = lax.dot_general(cols, rhs, TN, preferred_element_type=F32)
        ref[...] = jnp.where(inside, 0.0, ref[...]) - change
        ref[pl.ds(k0, PANEL), :] = done
        return carry

    lax.fori_loop(0, S // PANEL, panel, 0)


class Op:
    def __init__(self, **refs):
        self.__dict__.update(refs)


def kernel(
    l_op, l_start, r_op, r_start,
    l_out, r_out, ray_out,
    l_a, r_a,
    l_xs, l_xt, l_mate_s, l_mate_r, l_side_s, l_side_r, l_hand, l_y, l_sp,
    r_xs, r_xt, r_ps, r_pr, r_y, r_sp, r_keep,
    g_loc, g_one, g_sum, g_two, g_m, g_fac,
    l_asem, r_asem,
    gs_sem, gr_sem, fs_sem, fr_sem, ps_sem, pr_sem, xs_sem, xr_sem, es_sem, er_sem,
    lgs_sem, lgr_sem, lhs_sem, lhr_sem, lms_sem, lmr_sem, lss_sem, lsr_sem,
    a1s_sem, a1r_sem, a2s_sem, a2r_sem, a3s_sem, a3r_sem,
):
    y = lax.axis_index("row")
    col = lax.axis_index("col")
    x = col // 2
    k = col % 2
    mate = x * 2 + (1 - k)
    l_n, r_n = l_op.shape[0] * 2, r_op.shape[0] * 2
    l_nb, r_nb = l_n // 8, r_n // 8
    tile = r_nb // TILES
    piece = r_nb // CHUNKS

    left = Op(i=0, n=l_n, nb=l_nb, y=l_y, sp=l_sp)
    right = Op(i=1, n=r_n, nb=r_nb, y=r_y, sp=r_sp)
    ops = [left, right]

    l_load = pltpu.make_async_copy(l_op, l_a, l_asem)
    l_load.start()

    def r_fetch(t):
        half = jnp.where(t < TILES, 1 - y, y)
        start = pl.multiple_of(half * r_nb + (t % TILES) * tile, tile)
        return pltpu.make_async_copy(r_op.at[:, pl.ds(start, tile)], r_a.at[t % RING], r_asem.at[t % RING])

    for t in range(RING):
        r_fetch(t).start()

    class Gather:
        def __init__(self, first):
            self.dest_row = y if first else x
            self.my_slot = 2 * x + k if first else 2 * k + y
            self.src = x if first else y
            self.slots = [2 * a + k if first else 2 * k + a for a in range(2)]
            self.other_slots = [2 * a + (1 - k) if first else 2 * (1 - k) + a for a in range(2)]
            self.sends_to_self = [(self.dest_row == y) & (x == a) for a in range(2)]
            self.gets_from_self = [(x == a) if first else ((x == y) & (y == a)) for a in range(2)]

        def copy(self, a, h, recv):
            return remote(
                r_xs.at[h], r_xt.at[self.my_slot, h], gs_sem.at[a, h], gr_sem.at[recv, h], self.dest_row, 2 * a + k
            )

        def forward(self, a, h, slots):
            ref = r_xt.at[slots[a], h]
            return remote(ref, ref, fs_sem.at[a, h], fr_sem.at[a, h], y, mate)

        def start(self, h):
            for a in range(2):

                @pl.when(self.sends_to_self[a])
                def _():
                    r_xt[self.my_slot, h] = r_xs[h]

                @pl.when(jnp.logical_not(self.sends_to_self[a]))
                def _():
                    self.copy(a, h, self.src).start()

        def finish(self):
            for h in range(CHUNKS):
                for a in range(2):

                    @pl.when(jnp.logical_not(self.gets_from_self[a]))
                    def _():
                        self.copy(0, h, a).wait_recv()

                    self.forward(a, h, self.slots).start()
                for a in range(2):
                    self.forward(a, h, self.other_slots).wait_recv()
                if h < CHUNKS - 1:
                    right_early(h)

        def drain(self):
            for h in range(CHUNKS):
                for a in range(2):
                    self.forward(a, h, self.slots).wait_send()

                    @pl.when(jnp.logical_not(self.sends_to_self[a]))
                    def _():
                        self.copy(a, h, self.src).wait_send()

    def left_copy(b, slot):
        return remote(l_xs, l_xt.at[slot], lgs_sem.at[b], lgr_sem.at[slot], b, 2 * y + x)

    def left_across(b):
        return remote(l_xs, l_hand, lgs_sem.at[b], lhr_sem, 1 - y, col)

    def left_hand_on():
        return remote(l_hand, l_xt.at[k], lhs_sem, lgr_sem.at[k], y, 2 * (1 - x) + x)

    def left_self(b):
        return (b == y) & (y == x) & (x == k)

    def left_start():
        for b in (1 - y, y):
            across = (b != y) & (x != y)

            @pl.when(left_self(b))
            def _():
                l_xt[k] = l_xs[...]

            @pl.when(across)
            def _():
                left_across(b).start()

            @pl.when(jnp.logical_not(left_self(b) | across))
            def _():
                left_copy(b, k).start()

    def left_relay():
        @pl.when(x == y)
        def _():
            left_across(0).wait_recv()
            left_hand_on().start()

    def left_finish():
        for slot in range(2):

            @pl.when(jnp.logical_not((y == x) & (x == k) & (k == slot)))
            def _():
                left_copy(0, slot).wait_recv()

    def left_drain():
        for b in range(2):

            @pl.when(jnp.logical_not(left_self(b)))
            def _():
                left_copy(b, k).wait_send()

        @pl.when(x == y)
        def _():
            left_hand_on().wait_send()

    def left_block(index):
        rows = pl.ds(pl.multiple_of(index * l_nb, l_nb), l_nb)
        return dot_nt(l_xt[0], l_a[rows, :l_nb]) + dot_nt(l_xt[1], l_a[rows, l_nb:])

    def left_mate(a):
        return remote(l_mate_s.at[a], l_mate_r.at[a], lms_sem.at[a], lmr_sem.at[a], y, mate)

    def left_side():
        return remote(l_side_s, l_side_r, lss_sem, lsr_sem, y, 2 * (1 - x) + k)

    def left_multiply():
        l_mate_s[1 - x] = left_block(2 * (1 - x) + (1 - k))
        left_mate(1 - x).start()
        l_side_s[...] = left_block(2 * (1 - x) + k)
        l_mate_s[x] = left_block(2 * x + (1 - k))
        left_mate(x).start()
        left_mate(1 - x).wait_recv()
        l_side_s[...] = l_side_s[...] + l_mate_r[1 - x]
        left_side().start()
        l_y[...] = left_block(2 * x + k)

    def left_reduce_finish():
        left_mate(x).wait_recv()
        l_y[...] = l_y[...] + l_mate_r[x]
        left_side().wait_recv()
        l_y[...] = l_y[...] + l_side_r[...]
        left_side().wait_send()
        for a in range(2):
            left_mate(a).wait_send()

    def right_send(t):
        return remote(r_ps.at[t], r_pr.at[t], ps_sem.at[t], pr_sem.at[t], 1 - y, col)

    def right_part(b, h):
        total = None
        for s in range(4):
            part = dot(r_xt[s, h], r_a[b, s * r_nb + h * piece : s * r_nb + (h + 1) * piece, :])
            total = part if total is None else total + part
        return total

    def right_early(h):
        def one(t, carry):
            if h == 0:
                r_fetch(t).wait()
                r_ps[t] = right_part(t, h)
            else:
                r_ps[t] = r_ps[t] + right_part(t, h)
            return carry

        lax.fori_loop(0, TILES, one, 0)

    def right_others(last):
        def one(t, carry):
            r_ps[t] = r_ps[t] + right_part(t, CHUNKS - 1)
            if not last:
                right_send(t).start()
            r_fetch(t + RING).start()
            return carry

        lax.fori_loop(0, TILES, one, 0)

    def right_own(last, begin, end):
        def one(i, carry):
            t = i + TILES
            r_fetch(t).wait()
            b = t % RING
            total = None
            for h in range(CHUNKS):
                part = right_part(b, h)
                total = part if total is None else total + part
            r_y[:, pl.ds(pl.multiple_of(i * tile, tile), tile)] = total
            if not last:
                r_fetch(lax.rem(t + RING, 2 * TILES)).start()
            return carry

        lax.fori_loop(begin, end, one, 0)

    def right_reduce_finish():
        gram = None
        for t in range(TILES):
            right_send(t).wait_recv()
            res = r_y[:, t * tile : (t + 1) * tile] + r_pr[t]
            r_y[:, t * tile : (t + 1) * tile] = res
            half = res.astype(BF16)
            part = dot_nt(half, half)
            gram = part if gram is None else gram + part
        pack(1, gram)
        for t in range(TILES):
            right_send(t).wait_send()

    low_lane = lax.broadcasted_iota(jnp.int32, (32, S), 1)
    tall_row = lax.broadcasted_iota(jnp.int32, (S, S), 0)
    tall_lane = lax.broadcasted_iota(jnp.int32, (S, S), 1)
    count = jnp.where(k == 0, float(l_n), float(r_n))

    def pack(i, gram):
        g_loc[i, :64, :] = gram[:64]
        g_loc[i, 64:96, :] = jnp.where(low_lane < 64, pltpu.roll(gram[64:96], 64, axis=1), gram[96:])

    def sum_across(par, rows):
        part = pl.ds(0, rows)
        one = remote(g_loc.at[1 - k, part], g_one.at[par, part], a1s_sem.at[par], a1r_sem.at[par], y, mate)
        one.start()
        with jax.named_scope("ar_one"):
            one.wait_recv()
        g_sum[part, :] = g_loc[k, part, :] + g_one[par, part, :]
        twos = []
        for q in (2, 1, 0):
            yd = y + ((q + 1) // 2) * (1 - 2 * y)
            xd = x + ((q + 1) % 2) * (1 - 2 * x)
            two = remote(
                g_sum.at[part], g_two.at[par, q, part], a2s_sem.at[par, q], a2r_sem.at[par, q], yd, 2 * xd + k
            )
            two.start()
            twos.append(two)
        with jax.named_scope("ar_two"):
            for two in twos:
                two.wait_recv()
        total = (g_sum[part, :] + g_two[par, 0, part, :]) + (g_two[par, 1, part, :] + g_two[par, 2, part, :])
        one.wait_send()
        for two in twos:
            two.wait_send()
        return total / count

    def hand_over(par, left_work, right_work):
        mine, other = g_fac.at[k], g_fac.at[1 - k]
        copy = remote(mine, mine, a3s_sem.at[par], a3r_sem.at[par], y, mate)
        back = remote(other, other, a3s_sem.at[par], a3r_sem.at[par], y, mate)
        copy.start()

        @pl.when(k == 0)
        def _():
            left_work()
            back.wait_recv()
            right_work()

        @pl.when(k == 1)
        def _():
            right_work()
            back.wait_recv()
            left_work()

        copy.wait_send()

    def factor(par):
        gram = sum_across(par, 96)
        g_m[:64, :] = gram[:64]
        g_m[64:96, :] = pltpu.roll(gram[64:], 64, axis=1)
        g_m[96:, :] = gram[64:]
        with jax.named_scope("chol"):
            inverse_factor(g_m)
        g_fac[k] = jnp.where(tall_lane <= tall_row, g_m[...], 0.0)

    def apply_piece(o, lhs, start, width):
        high, mid, low = split(o.y[:, start : start + width])
        rhs = jnp.concatenate([high, high, mid, mid, low, high], axis=0)
        return dot(lhs, rhs)

    def apply_lhs(o):
        high, mid, low = split(g_fac[o.i])
        return jnp.concatenate([high, mid, high, mid, high, low], axis=1)

    def second_gram(o):
        lhs = apply_lhs(o)
        for start in range(0, o.nb, 256):
            res = apply_piece(o, lhs, start, 256)
            o.y[:, start : start + 256] = res
            parts = split(res)
            for q in range(3):
                o.sp[q * S : (q + 1) * S, start : start + 256] = parts[q]
        both = dot_nt(o.sp[: 2 * S, :], o.sp[: 2 * S, :])
        cross = dot_nt(o.sp[:S, :], o.sp[2 * S :, :])
        pack(o.i, both[:S, :S] + ((both[:S, S:] + both[S:, :S]) + (both[S:, S:] + (cross + cross.T))))

    def high_dot_nt(lhs, rhs):
        return lax.dot_general(lhs, rhs, NT, precision=lax.Precision.HIGHEST, preferred_element_type=F32)

    def new_left():
        lhs = apply_lhs(left)
        for start in range(0, l_nb, 256):
            res = apply_piece(left, lhs, start, 256)
            l_y[:, start : start + 256] = res
            l_xs[:, start : start + 256] = res.astype(BF16)

    def new_right():
        lhs = apply_lhs(right)
        for h in range(CHUNKS):
            for start in range(h * piece, (h + 1) * piece, 256):
                res = apply_piece(right, lhs, start, 256)
                r_y[:, start : start + 256] = res
                r_xs[h, :, start - h * piece : start - h * piece + 256] = res.astype(BF16)
            later.start(h)

    def multiply(drain, last):
        with jax.named_scope("r_mul0"):
            right_others(last)
        with jax.named_scope("l_relay"):
            left_relay()
        with jax.named_scope("r_mul1"):
            right_own(last, 0, 2)
        with jax.named_scope("l_fin"):
            left_finish()
        with jax.named_scope("l_mul"):
            left_multiply()
        with jax.named_scope("r_mul2"):
            right_own(last, 2, TILES)
        if not last:
            with jax.named_scope("r_red"):
                right_reduce_finish()
        with jax.named_scope("l_red"):
            left_reduce_finish()
        left_drain()
        drain()

    first, later = Gather(True), Gather(False)
    for h in range(CHUNKS):
        for b in range(piece // S):
            r_xs[h, :, b * S : (b + 1) * S] = r_start[h * piece + b * S : h * piece + (b + 1) * S, :].T.astype(BF16)
        first.start(h)
    for b in range(l_nb // S):
        l_xs[:, b * S : (b + 1) * S] = l_start[b * S : (b + 1) * S, :].T.astype(BF16)
    left_start()
    with jax.named_scope("gather_first"):
        first.finish()
    first.drain()
    l_load.wait()

    def sweep(i, carry):
        multiply(functools.partial(pl.when(i > 0), later.drain), False)
        with jax.named_scope("gram1"):
            half = l_y[...].astype(BF16)
            pack(0, dot_nt(half, half))
        with jax.named_scope("factor0"):
            factor(0)
        with jax.named_scope("gram2"):
            hand_over(0, lambda: second_gram(left), lambda: second_gram(right))
        with jax.named_scope("factor1"):
            factor(1)
        with jax.named_scope("new_basis"):
            hand_over(1, new_left, new_right)
            left_start()
        with jax.named_scope("gather"):
            later.finish()
        return carry

    lax.fori_loop(0, SWEEPS, sweep, 0)

    stays = (x == y) & (k == y)

    def swap(c):
        return remote(r_keep.at[0, c], r_keep.at[1, c], es_sem.at[c], er_sem.at[c], 1 - y, col)

    def home(q, c):
        place = 2 * k + (y if q == 0 else 1 - y)
        return remote(r_keep.at[q, c], r_pr.at[c], xs_sem.at[q, c], xr_sem.at[c], y, place)

    for c in range(TILES):
        r_keep[0, c] = r_y[:, c * tile : (c + 1) * tile]
        swap(c).start()

        @pl.when((x == y) & (k != y))
        def _():
            home(0, c).start()

    l_out[...] = l_y[...]
    with jax.named_scope("last_mul"):
        multiply(later.drain, True)
    with jax.named_scope("ray"):
        g_loc[0] = high_dot_nt(l_out[...], l_y[...])
        total = None
        for c in range(TILES):
            part = high_dot_nt(r_keep[0, c], r_y[:, c * tile : (c + 1) * tile])
            total = part if total is None else total + part
        for c in range(TILES):
            swap(c).wait_recv()

            @pl.when(x == y)
            def _():
                home(1, c).start()

            total = total + high_dot_nt(r_keep[1, c], r_ps[c])
        g_loc[1] = total
    with jax.named_scope("last_sum"):
        g_fac[k] = sum_across(2, S)
    with jax.named_scope("last_hand"):
        hand_over(2, lambda: None, lambda: None)
    ray_out[...] = g_fac[...]
    with jax.named_scope("home"):
        for c in range(TILES):
            swap(c).wait_send()

            @pl.when(x == y)
            def _():
                home(1, c).wait_send()

            @pl.when((x == y) & (k != y))
            def _():
                home(0, c).wait_send()

            @pl.when(stays)
            def _():
                r_out[:, c * tile : (c + 1) * tile] = r_keep[0, c]

            @pl.when(jnp.logical_not(stays))
            def _():
                home(0, c).wait_recv()
                r_out[:, c * tile : (c + 1) * tile] = r_pr[c]


def finish_kernel(l_in, r_in, ray_in, l_out, l_ray, r_out, r_ray):
    for src, dst in ((l_in, l_out), (r_in, r_out)):
        for b in range(dst.shape[0] // S):
            dst[b * S : (b + 1) * S, :] = src[:, b * S : (b + 1) * S].T
    l_ray[...] = ray_in[0]
    r_ray[...] = ray_in[1]


def solution(mesh):
    def local_program(left_op, left_start, right_op, right_start):
        l_nb, r_nb = left_op.shape[0] // 4, right_op.shape[0] // 4
        dma = pltpu.SemaphoreType.DMA
        vmem = pl.BlockSpec(memory_space=pltpu.VMEM)
        hbm = pl.BlockSpec(memory_space=pl.ANY)
        shape = jax.ShapeDtypeStruct
        left_t, right_t, rayleigh = pl.pallas_call(
            kernel,
            out_shape=(shape((S, l_nb), F32), shape((S, r_nb), F32), shape((2, S, S), F32)),
            in_specs=[hbm, vmem, hbm, vmem],
            out_specs=(vmem, vmem, vmem),
            scratch_shapes=[
                pltpu.VMEM(left_op.shape, BF16),
                pltpu.VMEM((RING, right_op.shape[0], r_nb // TILES), BF16),
                pltpu.VMEM((S, l_nb), BF16),
                pltpu.VMEM((2, S, l_nb), BF16),
                pltpu.VMEM((2, S, l_nb), F32),
                pltpu.VMEM((2, S, l_nb), F32),
                pltpu.VMEM((S, l_nb), F32),
                pltpu.VMEM((S, l_nb), F32),
                pltpu.VMEM((S, l_nb), BF16),
                pltpu.VMEM((S, l_nb), F32),
                pltpu.VMEM((3 * S, l_nb), BF16),
                pltpu.VMEM((CHUNKS, S, r_nb // CHUNKS), BF16),
                pltpu.VMEM((4, CHUNKS, S, r_nb // CHUNKS), BF16),
                pltpu.VMEM((TILES, S, r_nb // TILES), F32),
                pltpu.VMEM((TILES, S, r_nb // TILES), F32),
                pltpu.VMEM((S, r_nb), F32),
                pltpu.VMEM((3 * S, r_nb), BF16),
                pltpu.VMEM((2, TILES, S, r_nb // TILES), F32),
                pltpu.VMEM((2, S, S), F32),
                pltpu.VMEM((3, S, S), F32),
                pltpu.VMEM((S, S), F32),
                pltpu.VMEM((3, 3, S, S), F32),
                pltpu.VMEM((S, S), F32),
                pltpu.VMEM((2, S, S), F32),
                dma, dma((RING,)),
                dma((2, CHUNKS)), dma((2, CHUNKS)), dma((2, CHUNKS)), dma((2, CHUNKS)),
                dma((TILES,)), dma((TILES,)), dma((2, TILES)), dma((TILES,)), dma((TILES,)), dma((TILES,)),
                dma((2,)), dma((2,)), dma, dma, dma((2,)), dma((2,)), dma, dma,
                dma((3,)), dma((3,)), dma((3, 3)), dma((3, 3)), dma((3,)), dma((3,)),
            ],
            compiler_params=pltpu.CompilerParams(has_side_effects=True, vmem_limit_bytes=64 * 1024 * 1024 - 65536),
        )(left_op, left_start, right_op, right_start)
        left_basis, left_ray, right_basis, right_ray = pl.pallas_call(
            finish_kernel,
            out_shape=(shape((l_nb, S), F32), shape((S, S), F32), shape((r_nb, S), F32), shape((S, S), F32)),
            in_specs=[vmem] * 3,
            out_specs=(vmem,) * 4,
        )(left_t, right_t, rayleigh)
        return left_basis, left_ray, right_basis, right_ray

    op_spec = P(("batch", "row"), "col")
    vec_spec = P(("batch", "row", "col"), None)
    small_spec = P("batch", None)
    return jax.shard_map(
        local_program, mesh=mesh, in_specs=(op_spec, vec_spec, op_spec, vec_spec),
        out_specs=(vec_spec, small_spec, vec_spec, small_spec), check_vma=False,
    )
```

```python
import jax
import jax.numpy as jnp
from jax import lax
from jax.experimental import pallas as pl
from jax.experimental.pallas import tpu as pltpu
from jax.sharding import PartitionSpec as P


SWEEPS = 4
S = 128
RING = 4
TILES = 4
CHUNKS = 4
PANEL = 16
MESH = pl.DeviceIdType.MESH
F32, BF16 = jnp.float32, jnp.bfloat16
NT = (((1,), (1,)), ((), ()))
TN = (((0,), (0,)), ((), ()))


def dot(lhs, rhs):
    return jnp.dot(lhs, rhs, preferred_element_type=F32)


def dot_nt(lhs, rhs):
    return lax.dot_general(lhs, rhs, NT, preferred_element_type=F32)


def split(value):
    high = value.astype(BF16)
    rest = value - high.astype(F32)
    mid = rest.astype(BF16)
    low = (rest - mid.astype(F32)).astype(BF16)
    return high, mid, low


def remote(src, dst, send_sem, recv_sem, row, col):
    return pltpu.make_async_remote_copy(
        src_ref=src, dst_ref=dst, send_sem=send_sem, recv_sem=recv_sem,
        device_id={"row": row, "col": col}, device_id_type=MESH,
    )


def inverse_factor(ref):
    sub = lax.broadcasted_iota(jnp.int32, (PANEL, S), 0)
    lane = lax.broadcasted_iota(jnp.int32, (PANEL, S), 1)

    tall_row = lax.broadcasted_iota(jnp.int32, (S, S), 0)
    tall_lane = lax.broadcasted_iota(jnp.int32, (S, S), 1)

    def panel(p, carry):
        k0 = pl.multiple_of(p * PANEL, PANEL)
        inside = (tall_lane >= k0) & (tall_lane < k0 + PANEL) & (tall_row >= k0 + PANEL)
        at = lane - k0
        rows = ref[pl.ds(k0, PANEL), :]
        heads = jnp.stack(
            [
                jnp.broadcast_to(jnp.sum(jnp.where(at == j, rows, 0.0), axis=1, keepdims=True), (PANEL, S))
                for j in range(PANEL)
            ]
        )
        high, mid, low = split(jnp.where(at >= PANEL, rows, 0.0))
        cols = jnp.concatenate([high, mid, high, mid, high, low], axis=0)
        rows = jnp.where((at >= 0) & (at < PANEL), jnp.where(at == sub, 1.0, 0.0), rows)
        done = rows
        piv = heads[0, 0:1, :]
        for j in range(PANEL):
            here = sub == j
            root = lax.rsqrt(piv)
            inv = root * root
            done = jnp.where(here, rows * root, done)
            mult = jnp.where(here, 0.0, heads[0])
            if j < PANEL - 1:
                head_rows = heads[1:, j : j + 1, :] * inv
                piv = heads[1, j + 1 : j + 2, :] - heads[0, j + 1 : j + 2, :] * head_rows[0]
                heads = jnp.where(here[None], head_rows, heads[1:] - mult[None] * head_rows)
            scaled = rows[j : j + 1, :] * inv
            rows = jnp.where(here, scaled, rows - mult * scaled)
        high, mid, low = split(rows)
        rhs = jnp.concatenate([high, high, mid, mid, low, high], axis=0)
        change = lax.dot_general(cols, rhs, TN, preferred_element_type=F32)
        ref[...] = jnp.where(inside, 0.0, ref[...]) - change
        ref[pl.ds(k0, PANEL), :] = done
        return carry

    lax.fori_loop(0, S // PANEL, panel, 0)


class Op:
    def __init__(self, **refs):
        self.__dict__.update(refs)


def kernel(
    l_op, l_start, r_op, r_start,
    l_out, r_out, ray_out,
    l_a, r_a,
    l_xs, l_xt, l_mate_s, l_mate_r, l_side_s, l_side_r, l_hand, l_y, l_sp,
    r_xs, r_xt, r_ps, r_pr, r_y, r_sp, r_keep,
    g_loc, g_one, g_sum, g_two, g_m, g_fac,
    l_asem, r_asem,
    gs_sem, gr_sem, fs_sem, fr_sem, ps_sem, pr_sem, xs_sem, xr_sem, es_sem, er_sem,
    lgs_sem, lgr_sem, lhs_sem, lhr_sem, lms_sem, lmr_sem, lss_sem, lsr_sem,
    a1s_sem, a1r_sem, a2s_sem, a2r_sem, a3s_sem, a3r_sem,
):
    y = lax.axis_index("row")
    col = lax.axis_index("col")
    x = col // 2
    k = col % 2
    mate = x * 2 + (1 - k)
    l_n, r_n = l_op.shape[0] * 2, r_op.shape[0] * 2
    l_nb, r_nb = l_n // 8, r_n // 8
    tile = r_nb // TILES
    piece = r_nb // CHUNKS

    left = Op(i=0, n=l_n, nb=l_nb, y=l_y, sp=l_sp)
    right = Op(i=1, n=r_n, nb=r_nb, y=r_y, sp=r_sp)
    ops = [left, right]

    def r_fetch(t):
        half = jnp.where(t < TILES, 1 - y, y)
        start = pl.multiple_of(half * r_nb + (t % TILES) * tile, tile)
        return pltpu.make_async_copy(r_op.at[:, pl.ds(start, tile)], r_a.at[t % RING], r_asem.at[t % RING])

    for t in range(RING):
        r_fetch(t).start()
    l_load = pltpu.make_async_copy(l_op, l_a, l_asem)
    l_load.start()

    class Gather:
        def __init__(self, first):
            self.dest_row = y if first else x
            self.my_slot = 2 * x + k if first else 2 * k + y
            self.src = x if first else y
            self.slots = [2 * a + k if first else 2 * k + a for a in range(2)]
            self.other_slots = [2 * a + (1 - k) if first else 2 * (1 - k) + a for a in range(2)]
            self.sends_to_self = [(self.dest_row == y) & (x == a) for a in range(2)]
            self.gets_from_self = [(x == a) if first else ((x == y) & (y == a)) for a in range(2)]

        def copy(self, a, h, recv):
            return remote(
                r_xs.at[h], r_xt.at[self.my_slot, h], gs_sem.at[a, h], gr_sem.at[recv, h], self.dest_row, 2 * a + k
            )

        def forward(self, a, h, slots):
            ref = r_xt.at[slots[a], h]
            return remote(ref, ref, fs_sem.at[a, h], fr_sem.at[a, h], y, mate)

        def start(self, h):
            for a in range(2):

                @pl.when(self.sends_to_self[a])
                def _():
                    r_xt[self.my_slot, h] = r_xs[h]

                @pl.when(jnp.logical_not(self.sends_to_self[a]))
                def _():
                    self.copy(a, h, self.src).start()

        def finish(self):
            for h in range(CHUNKS):
                for a in range(2):

                    @pl.when(jnp.logical_not(self.gets_from_self[a]))
                    def _():
                        self.copy(0, h, a).wait_recv()

                    self.forward(a, h, self.slots).start()
                for a in range(2):
                    self.forward(a, h, self.other_slots).wait_recv()
                if h < CHUNKS - 1:
                    right_early(h)

        def drain(self):
            for h in range(CHUNKS):
                for a in range(2):
                    self.forward(a, h, self.slots).wait_send()

                    @pl.when(jnp.logical_not(self.sends_to_self[a]))
                    def _():
                        self.copy(a, h, self.src).wait_send()

    def left_copy(b, slot):
        return remote(l_xs, l_xt.at[slot], lgs_sem.at[b], lgr_sem.at[slot], b, 2 * y + x)

    def left_across(b):
        return remote(l_xs, l_hand, lgs_sem.at[b], lhr_sem, 1 - y, col)

    def left_hand_on():
        return remote(l_hand, l_xt.at[k], lhs_sem, lgr_sem.at[k], y, 2 * (1 - x) + x)

    def left_self(b):
        return (b == y) & (y == x) & (x == k)

    def left_start():
        for b in (1 - y, y):
            across = (b != y) & (x != y)

            @pl.when(left_self(b))
            def _():
                l_xt[k] = l_xs[...]

            @pl.when(across)
            def _():
                left_across(b).start()

            @pl.when(jnp.logical_not(left_self(b) | across))
            def _():
                left_copy(b, k).start()

    def left_relay():
        @pl.when(x == y)
        def _():
            left_across(0).wait_recv()
            left_hand_on().start()

    def left_finish():
        for slot in range(2):

            @pl.when(jnp.logical_not((y == x) & (x == k) & (k == slot)))
            def _():
                left_copy(0, slot).wait_recv()

    def left_drain():
        for b in range(2):

            @pl.when(jnp.logical_not(left_self(b)))
            def _():
                left_copy(b, k).wait_send()

        @pl.when(x == y)
        def _():
            left_hand_on().wait_send()

    def left_block(index):
        rows = pl.ds(pl.multiple_of(index * l_nb, l_nb), l_nb)
        return dot_nt(l_xt[0], l_a[rows, :l_nb]) + dot_nt(l_xt[1], l_a[rows, l_nb:])

    def left_mate(a):
        return remote(l_mate_s.at[a], l_mate_r.at[a], lms_sem.at[a], lmr_sem.at[a], y, mate)

    def left_side():
        return remote(l_side_s, l_side_r, lss_sem, lsr_sem, y, 2 * (1 - x) + k)

    def left_multiply():
        l_mate_s[1 - x] = left_block(2 * (1 - x) + (1 - k))
        left_mate(1 - x).start()
        l_side_s[...] = left_block(2 * (1 - x) + k)
        l_mate_s[x] = left_block(2 * x + (1 - k))
        left_mate(x).start()
        left_mate(1 - x).wait_recv()
        l_side_s[...] = l_side_s[...] + l_mate_r[1 - x]
        left_side().start()
        l_y[...] = left_block(2 * x + k)

    def left_reduce_finish():
        left_mate(x).wait_recv()
        l_y[...] = l_y[...] + l_mate_r[x]
        left_side().wait_recv()
        l_y[...] = l_y[...] + l_side_r[...]
        left_side().wait_send()
        for a in range(2):
            left_mate(a).wait_send()

    def right_send(t):
        return remote(r_ps.at[t], r_pr.at[t], ps_sem.at[t], pr_sem.at[t], 1 - y, col)

    def right_part(b, h):
        total = None
        for s in range(4):
            part = dot(r_xt[s, h], r_a[b, s * r_nb + h * piece : s * r_nb + (h + 1) * piece, :])
            total = part if total is None else total + part
        return total

    def right_early(h):
        def one(t, carry):
            if h == 0:
                r_fetch(t).wait()
                r_ps[t] = right_part(t, h)
            else:
                r_ps[t] = r_ps[t] + right_part(t, h)
            return carry

        lax.fori_loop(0, TILES, one, 0)

    def right_others(last):
        def one(t, carry):
            r_ps[t] = r_ps[t] + right_part(t, CHUNKS - 1)
            if not last:
                right_send(t).start()
            r_fetch(t + RING).start()
            return carry

        lax.fori_loop(0, TILES, one, 0)

    def right_own(last, begin, end):
        def one(i, carry):
            t = i + TILES
            r_fetch(t).wait()
            b = t % RING
            total = None
            for h in range(CHUNKS):
                part = right_part(b, h)
                total = part if total is None else total + part
            r_y[:, pl.ds(pl.multiple_of(i * tile, tile), tile)] = total
            if not last:
                r_fetch(lax.rem(t + RING, 2 * TILES)).start()
            return carry

        lax.fori_loop(begin, end, one, 0)

    def right_reduce_finish():
        gram = None
        for t in range(TILES):
            right_send(t).wait_recv()
            res = r_y[:, t * tile : (t + 1) * tile] + r_pr[t]
            r_y[:, t * tile : (t + 1) * tile] = res
            half = res.astype(BF16)
            part = dot_nt(half, half)
            gram = part if gram is None else gram + part
        pack(1, gram)
        for t in range(TILES):
            right_send(t).wait_send()

    low_lane = lax.broadcasted_iota(jnp.int32, (32, S), 1)
    tall_row = lax.broadcasted_iota(jnp.int32, (S, S), 0)
    tall_lane = lax.broadcasted_iota(jnp.int32, (S, S), 1)
    count = jnp.where(k == 0, float(l_n), float(r_n))

    def pack(i, gram):
        g_loc[i, :64, :] = gram[:64]
        g_loc[i, 64:96, :] = jnp.where(low_lane < 64, pltpu.roll(gram[64:96], 64, axis=1), gram[96:])

    def sum_across(par, rows, after_sends=lambda: None):
        part = pl.ds(0, rows)
        one = remote(g_loc.at[1 - k, part], g_one.at[par, part], a1s_sem.at[par], a1r_sem.at[par], y, mate)
        one.start()
        with jax.named_scope("ar_one"):
            one.wait_recv()
        g_sum[part, :] = g_loc[k, part, :] + g_one[par, part, :]
        twos = []
        for q in (2, 1, 0):
            yd = y + ((q + 1) // 2) * (1 - 2 * y)
            xd = x + ((q + 1) % 2) * (1 - 2 * x)
            two = remote(
                g_sum.at[part], g_two.at[par, q, part], a2s_sem.at[par, q], a2r_sem.at[par, q], yd, 2 * xd + k
            )
            two.start()
            twos.append(two)
        after_sends()
        with jax.named_scope("ar_two"):
            for two in twos:
                two.wait_recv()
        total = (g_sum[part, :] + g_two[par, 0, part, :]) + (g_two[par, 1, part, :] + g_two[par, 2, part, :])
        one.wait_send()
        for two in twos:
            two.wait_send()
        return total / count

    def hand_over(par, left_work, right_work):
        mine, other = g_fac.at[k], g_fac.at[1 - k]
        copy = remote(mine, mine, a3s_sem.at[par], a3r_sem.at[par], y, mate)
        back = remote(other, other, a3s_sem.at[par], a3r_sem.at[par], y, mate)
        copy.start()

        @pl.when(k == 0)
        def _():
            left_work()
            back.wait_recv()
            right_work()

        @pl.when(k == 1)
        def _():
            right_work()
            back.wait_recv()
            left_work()

        copy.wait_send()

    def factor(par):
        gram = sum_across(par, 96)
        g_m[:64, :] = gram[:64]
        g_m[64:96, :] = pltpu.roll(gram[64:], 64, axis=1)
        g_m[96:, :] = gram[64:]
        with jax.named_scope("chol"):
            inverse_factor(g_m)
        g_fac[k] = jnp.where(tall_lane <= tall_row, g_m[...], 0.0)

    def apply_piece(o, lhs, start, width):
        high, mid, low = split(o.y[:, start : start + width])
        rhs = jnp.concatenate([high, high, mid, mid, low, high], axis=0)
        return dot(lhs, rhs)

    def apply_lhs(o):
        high, mid, low = split(g_fac[o.i])
        return jnp.concatenate([high, mid, high, mid, high, low], axis=1)

    def second_gram(o):
        lhs = apply_lhs(o)
        for start in range(0, o.nb, 256):
            res = apply_piece(o, lhs, start, 256)
            o.y[:, start : start + 256] = res
            parts = split(res)
            for q in range(3):
                o.sp[q * S : (q + 1) * S, start : start + 256] = parts[q]
        both = dot_nt(o.sp[: 2 * S, :], o.sp[: 2 * S, :])
        cross = dot_nt(o.sp[:S, :], o.sp[2 * S :, :])
        pack(o.i, both[:S, :S] + ((both[:S, S:] + both[S:, :S]) + (both[S:, S:] + (cross + cross.T))))

    def high_dot_nt(lhs, rhs):
        return lax.dot_general(lhs, rhs, NT, precision=lax.Precision.HIGHEST, preferred_element_type=F32)

    def new_left():
        lhs = apply_lhs(left)
        for start in range(0, l_nb, 256):
            res = apply_piece(left, lhs, start, 256)
            l_y[:, start : start + 256] = res
            l_xs[:, start : start + 256] = res.astype(BF16)

    def new_right():
        lhs = apply_lhs(right)
        for h in range(CHUNKS):
            for start in range(h * piece, (h + 1) * piece, 256):
                res = apply_piece(right, lhs, start, 256)
                r_y[:, start : start + 256] = res
                r_xs[h, :, start - h * piece : start - h * piece + 256] = res.astype(BF16)
            later.start(h)

    def multiply(last, after_relay=lambda: None, after_left=lambda: None):
        with jax.named_scope("r_mul0"):
            right_others(last)
        with jax.named_scope("l_relay"):
            left_relay()
            after_relay()
        with jax.named_scope("r_mul1"):
            right_own(last, 0, 2)
        with jax.named_scope("l_fin"):
            left_finish()
        with jax.named_scope("l_mul"):
            left_multiply()
            after_left()
        with jax.named_scope("r_mul2"):
            right_own(last, 2, TILES)

    first, later = Gather(True), Gather(False)
    for h in range(CHUNKS):
        for b in range(piece // S):
            r_xs[h, :, b * S : (b + 1) * S] = r_start[h * piece + b * S : h * piece + (b + 1) * S, :].T.astype(BF16)
        first.start(h)
    for b in range(l_nb // S):
        l_xs[:, b * S : (b + 1) * S] = l_start[b * S : (b + 1) * S, :].T.astype(BF16)
    left_start()
    with jax.named_scope("gather_first"):
        first.finish()
    first.drain()
    l_load.wait()

    def sweep(i, carry):
        multiply(False)
        with jax.named_scope("r_red"):
            right_reduce_finish()
        with jax.named_scope("l_red"):
            left_reduce_finish()
        left_drain()
        pl.when(i > 0)(later.drain)
        with jax.named_scope("gram1"):
            half = l_y[...].astype(BF16)
            pack(0, dot_nt(half, half))
        with jax.named_scope("factor0"):
            factor(0)
        with jax.named_scope("gram2"):
            hand_over(0, lambda: second_gram(left), lambda: second_gram(right))
        with jax.named_scope("factor1"):
            factor(1)
        with jax.named_scope("new_basis"):
            hand_over(1, new_left, new_right)
            left_start()
        with jax.named_scope("gather"):
            later.finish()
        return carry

    lax.fori_loop(0, SWEEPS, sweep, 0)

    stays = (x == y) & (k == y)

    def swap(c):
        return remote(r_keep.at[0, c], r_keep.at[1, c], es_sem.at[c], er_sem.at[c], 1 - y, col)

    def home(q, c):
        place = 2 * k + (y if q == 0 else 1 - y)
        return remote(r_keep.at[q, c], r_pr.at[c], xs_sem.at[q, c], xr_sem.at[c], y, place)

    def pass_on(c):
        @pl.when(x == y)
        def _():
            home(1, c).start()

    def own_home():
        for c in range(TILES):

            @pl.when((x == y) & (k != y))
            def _():
                home(0, c).start()

    def first_swapped():
        swap(0).wait_recv()
        pass_on(0)

    for c in range(TILES):
        r_keep[0, c] = r_y[:, c * tile : (c + 1) * tile]
        swap(c).start()
    l_out[...] = l_y[...]
    with jax.named_scope("last_mul"):
        multiply(True, own_home, first_swapped)
    with jax.named_scope("ray"):
        total = high_dot_nt(r_keep[1, 0], r_ps[0])
        for c in range(TILES):
            total = total + high_dot_nt(r_keep[0, c], r_y[:, c * tile : (c + 1) * tile])
        for c in range(1, TILES):
            if c == TILES - 1:
                with jax.named_scope("l_red"):
                    left_reduce_finish()
                g_loc[0] = high_dot_nt(l_out[...], l_y[...])
            with jax.named_scope("swap"):
                swap(c).wait_recv()
            if c == 1:
                pass_on(c)
            total = total + high_dot_nt(r_keep[1, c], r_ps[c])
        g_loc[1] = total

    def rest_home():
        for c in range(2, TILES):
            pass_on(c)

    with jax.named_scope("last_sum"):
        g_fac[k] = sum_across(2, S, rest_home)
    left_drain()
    later.drain()
    with jax.named_scope("last_hand"):
        hand_over(2, lambda: None, lambda: None)
    ray_out[...] = g_fac[...]
    with jax.named_scope("home"):
        for c in range(TILES):
            swap(c).wait_send()

            @pl.when(x == y)
            def _():
                home(1, c).wait_send()

            @pl.when((x == y) & (k != y))
            def _():
                home(0, c).wait_send()

            @pl.when(stays)
            def _():
                r_out[:, c * tile : (c + 1) * tile] = r_keep[0, c]

            @pl.when(jnp.logical_not(stays))
            def _():
                home(0, c).wait_recv()
                r_out[:, c * tile : (c + 1) * tile] = r_pr[c]


def finish_kernel(l_in, r_in, ray_in, l_out, l_ray, r_out, r_ray):
    for src, dst in ((l_in, l_out), (r_in, r_out)):
        for b in range(dst.shape[0] // S):
            dst[b * S : (b + 1) * S, :] = src[:, b * S : (b + 1) * S].T
    l_ray[...] = ray_in[0]
    r_ray[...] = ray_in[1]


def solution(mesh):
    def local_program(left_op, left_start, right_op, right_start):
        l_nb, r_nb = left_op.shape[0] // 4, right_op.shape[0] // 4
        dma = pltpu.SemaphoreType.DMA
        vmem = pl.BlockSpec(memory_space=pltpu.VMEM)
        hbm = pl.BlockSpec(memory_space=pl.ANY)
        shape = jax.ShapeDtypeStruct
        left_t, right_t, rayleigh = pl.pallas_call(
            kernel,
            out_shape=(shape((S, l_nb), F32), shape((S, r_nb), F32), shape((2, S, S), F32)),
            in_specs=[hbm, vmem, hbm, vmem],
            out_specs=(vmem, vmem, vmem),
            scratch_shapes=[
                pltpu.VMEM(left_op.shape, BF16),
                pltpu.VMEM((RING, right_op.shape[0], r_nb // TILES), BF16),
                pltpu.VMEM((S, l_nb), BF16),
                pltpu.VMEM((2, S, l_nb), BF16),
                pltpu.VMEM((2, S, l_nb), F32),
                pltpu.VMEM((2, S, l_nb), F32),
                pltpu.VMEM((S, l_nb), F32),
                pltpu.VMEM((S, l_nb), F32),
                pltpu.VMEM((S, l_nb), BF16),
                pltpu.VMEM((S, l_nb), F32),
                pltpu.VMEM((3 * S, l_nb), BF16),
                pltpu.VMEM((CHUNKS, S, r_nb // CHUNKS), BF16),
                pltpu.VMEM((4, CHUNKS, S, r_nb // CHUNKS), BF16),
                pltpu.VMEM((TILES, S, r_nb // TILES), F32),
                pltpu.VMEM((TILES, S, r_nb // TILES), F32),
                pltpu.VMEM((S, r_nb), F32),
                pltpu.VMEM((3 * S, r_nb), BF16),
                pltpu.VMEM((2, TILES, S, r_nb // TILES), F32),
                pltpu.VMEM((2, S, S), F32),
                pltpu.VMEM((3, S, S), F32),
                pltpu.VMEM((S, S), F32),
                pltpu.VMEM((3, 3, S, S), F32),
                pltpu.VMEM((S, S), F32),
                pltpu.VMEM((2, S, S), F32),
                dma, dma((RING,)),
                dma((2, CHUNKS)), dma((2, CHUNKS)), dma((2, CHUNKS)), dma((2, CHUNKS)),
                dma((TILES,)), dma((TILES,)), dma((2, TILES)), dma((TILES,)), dma((TILES,)), dma((TILES,)),
                dma((2,)), dma((2,)), dma, dma, dma((2,)), dma((2,)), dma, dma,
                dma((3,)), dma((3,)), dma((3, 3)), dma((3, 3)), dma((3,)), dma((3,)),
            ],
            compiler_params=pltpu.CompilerParams(has_side_effects=True, vmem_limit_bytes=64 * 1024 * 1024 - 65536),
        )(left_op, left_start, right_op, right_start)
        left_basis, left_ray, right_basis, right_ray = pl.pallas_call(
            finish_kernel,
            out_shape=(shape((l_nb, S), F32), shape((S, S), F32), shape((r_nb, S), F32), shape((S, S), F32)),
            in_specs=[vmem] * 3,
            out_specs=(vmem,) * 4,
        )(left_t, right_t, rayleigh)
        return left_basis, left_ray, right_basis, right_ray

    op_spec = P(("batch", "row"), "col")
    vec_spec = P(("batch", "row", "col"), None)
    small_spec = P("batch", None)
    return jax.shard_map(
        local_program, mesh=mesh, in_specs=(op_spec, vec_spec, op_spec, vec_spec),
        out_specs=(vec_spec, small_spec, vec_spec, small_spec), check_vma=False,
    )
```

```python
import jax
import jax.numpy as jnp
from jax import lax
from jax.experimental import pallas as pl
from jax.experimental.pallas import tpu as pltpu
from jax.sharding import PartitionSpec as P


SWEEPS = 4
S = 128
RING = 4
TILES = 4
CHUNKS = 2
PANEL = 16
MESH = pl.DeviceIdType.MESH
F32, BF16 = jnp.float32, jnp.bfloat16
NT = (((1,), (1,)), ((), ()))
TN = (((0,), (0,)), ((), ()))


def dot(lhs, rhs):
    return jnp.dot(lhs, rhs, preferred_element_type=F32)


def dot_nt(lhs, rhs):
    return lax.dot_general(lhs, rhs, NT, preferred_element_type=F32)


def split(value):
    high = value.astype(BF16)
    rest = value - high.astype(F32)
    mid = rest.astype(BF16)
    low = (rest - mid.astype(F32)).astype(BF16)
    return high, mid, low


def remote(src, dst, send_sem, recv_sem, row, col):
    return pltpu.make_async_remote_copy(
        src_ref=src, dst_ref=dst, send_sem=send_sem, recv_sem=recv_sem,
        device_id={"row": row, "col": col}, device_id_type=MESH,
    )


def inverse_factor(ref):
    sub = lax.broadcasted_iota(jnp.int32, (PANEL, S), 0)
    lane = lax.broadcasted_iota(jnp.int32, (PANEL, S), 1)

    tall_row = lax.broadcasted_iota(jnp.int32, (S, S), 0)
    tall_lane = lax.broadcasted_iota(jnp.int32, (S, S), 1)

    def panel(p, carry):
        k0 = pl.multiple_of(p * PANEL, PANEL)
        inside = (tall_lane >= k0) & (tall_lane < k0 + PANEL) & (tall_row >= k0 + PANEL)
        at = lane - k0
        rows = ref[pl.ds(k0, PANEL), :]
        heads = jnp.stack(
            [
                jnp.broadcast_to(jnp.sum(jnp.where(at == j, rows, 0.0), axis=1, keepdims=True), (PANEL, S))
                for j in range(PANEL)
            ]
        )
        high, mid, low = split(jnp.where(at >= PANEL, rows, 0.0))
        cols = jnp.concatenate([high, mid, high, mid, high, low], axis=0)
        rows = jnp.where((at >= 0) & (at < PANEL), jnp.where(at == sub, 1.0, 0.0), rows)
        done = rows
        piv = heads[0, 0:1, :]
        for j in range(PANEL):
            here = sub == j
            root = lax.rsqrt(piv)
            inv = root * root
            done = jnp.where(here, rows * root, done)
            mult = jnp.where(here, 0.0, heads[0])
            if j < PANEL - 1:
                head_rows = heads[1:, j : j + 1, :] * inv
                piv = heads[1, j + 1 : j + 2, :] - heads[0, j + 1 : j + 2, :] * head_rows[0]
                heads = jnp.where(here[None], head_rows, heads[1:] - mult[None] * head_rows)
            scaled = rows[j : j + 1, :] * inv
            rows = jnp.where(here, scaled, rows - mult * scaled)
        high, mid, low = split(rows)
        rhs = jnp.concatenate([high, high, mid, mid, low, high], axis=0)
        change = lax.dot_general(cols, rhs, TN, preferred_element_type=F32)
        ref[...] = jnp.where(inside, 0.0, ref[...]) - change
        ref[pl.ds(k0, PANEL), :] = done
        return carry

    lax.fori_loop(0, S // PANEL, panel, 0)


class Op:
    def __init__(self, **refs):
        self.__dict__.update(refs)


def kernel(
    l_op, l_start, r_op, r_start,
    l_out, r_out, ray_out,
    l_a, r_a,
    l_xs, l_xt, l_mate_s, l_mate_r, l_side_s, l_side_r, l_hand, l_y, l_sp,
    r_xs, r_xt, r_ps, r_pr, r_y, r_sp, r_keep,
    g_loc, g_one, g_sum, g_two, g_m, g_fac,
    l_asem, r_asem,
    gs_sem, gr_sem, fs_sem, fr_sem, ps_sem, pr_sem, xs_sem, xr_sem, es_sem, er_sem,
    lgs_sem, lgr_sem, lhs_sem, lhr_sem, lms_sem, lmr_sem, lss_sem, lsr_sem,
    a1s_sem, a1r_sem, a2s_sem, a2r_sem, a3s_sem, a3r_sem,
):
    y = lax.axis_index("row")
    col = lax.axis_index("col")
    x = col // 2
    k = col % 2
    mate = x * 2 + (1 - k)
    l_n, r_n = l_op.shape[0] * 2, r_op.shape[0] * 2
    l_nb, r_nb = l_n // 8, r_n // 8
    tile = r_nb // TILES
    piece = r_nb // CHUNKS

    left = Op(i=0, n=l_n, nb=l_nb, y=l_y, sp=l_sp)
    right = Op(i=1, n=r_n, nb=r_nb, y=r_y, sp=r_sp)
    ops = [left, right]

    def r_fetch(t):
        half = jnp.where(t < TILES, 1 - y, y)
        start = pl.multiple_of(half * r_nb + (t % TILES) * tile, tile)
        return pltpu.make_async_copy(r_op.at[:, pl.ds(start, tile)], r_a.at[t % RING], r_asem.at[t % RING])

    for t in range(RING):
        r_fetch(t).start()
    l_load = pltpu.make_async_copy(l_op, l_a, l_asem)
    l_load.start()

    class Gather:
        def __init__(self, first):
            self.dest_row = y if first else x
            self.my_slot = 2 * x + k if first else 2 * k + y
            self.src = x if first else y
            self.slots = [2 * a + k if first else 2 * k + a for a in range(2)]
            self.other_slots = [2 * a + (1 - k) if first else 2 * (1 - k) + a for a in range(2)]
            self.sends_to_self = [(self.dest_row == y) & (x == a) for a in range(2)]
            self.gets_from_self = [(x == a) if first else ((x == y) & (y == a)) for a in range(2)]

        def copy(self, a, h, recv):
            return remote(
                r_xs.at[h], r_xt.at[self.my_slot, h], gs_sem.at[a, h], gr_sem.at[recv, h], self.dest_row, 2 * a + k
            )

        def forward(self, a, h, slots):
            ref = r_xt.at[slots[a], h]
            return remote(ref, ref, fs_sem.at[a, h], fr_sem.at[a, h], y, mate)

        def start(self, h):
            for a in range(2):

                @pl.when(self.sends_to_self[a])
                def _():
                    r_xt[self.my_slot, h] = r_xs[h]

                @pl.when(jnp.logical_not(self.sends_to_self[a]))
                def _():
                    self.copy(a, h, self.src).start()

        def finish(self):
            for h in range(CHUNKS):
                for a in range(2):

                    @pl.when(jnp.logical_not(self.gets_from_self[a]))
                    def _():
                        self.copy(0, h, a).wait_recv()

                    self.forward(a, h, self.slots).start()
                for a in range(2):
                    self.forward(a, h, self.other_slots).wait_recv()
                if h < CHUNKS - 1:
                    right_early(h)

        def drain(self):
            for h in range(CHUNKS):
                for a in range(2):
                    self.forward(a, h, self.slots).wait_send()

                    @pl.when(jnp.logical_not(self.sends_to_self[a]))
                    def _():
                        self.copy(a, h, self.src).wait_send()

    def left_copy(b, slot):
        return remote(l_xs, l_xt.at[slot], lgs_sem.at[b], lgr_sem.at[slot], b, 2 * y + x)

    def left_across(b):
        return remote(l_xs, l_hand, lgs_sem.at[b], lhr_sem, 1 - y, col)

    def left_hand_on():
        return remote(l_hand, l_xt.at[k], lhs_sem, lgr_sem.at[k], y, 2 * (1 - x) + x)

    def left_self(b):
        return (b == y) & (y == x) & (x == k)

    def left_start():
        for b in (1 - y, y):
            across = (b != y) & (x != y)

            @pl.when(left_self(b))
            def _():
                l_xt[k] = l_xs[...]

            @pl.when(across)
            def _():
                left_across(b).start()

            @pl.when(jnp.logical_not(left_self(b) | across))
            def _():
                left_copy(b, k).start()

    def left_relay():
        @pl.when(x == y)
        def _():
            left_across(0).wait_recv()
            left_hand_on().start()

    def left_finish():
        for slot in range(2):

            @pl.when(jnp.logical_not((y == x) & (x == k) & (k == slot)))
            def _():
                left_copy(0, slot).wait_recv()

    def left_drain():
        for b in range(2):

            @pl.when(jnp.logical_not(left_self(b)))
            def _():
                left_copy(b, k).wait_send()

        @pl.when(x == y)
        def _():
            left_hand_on().wait_send()

    def left_block(index):
        rows = pl.ds(pl.multiple_of(index * l_nb, l_nb), l_nb)
        return dot_nt(l_xt[0], l_a[rows, :l_nb]) + dot_nt(l_xt[1], l_a[rows, l_nb:])

    def left_mate(a):
        return remote(l_mate_s.at[a], l_mate_r.at[a], lms_sem.at[a], lmr_sem.at[a], y, mate)

    def left_side():
        return remote(l_side_s, l_side_r, lss_sem, lsr_sem, y, 2 * (1 - x) + k)

    def left_multiply():
        l_mate_s[1 - x] = left_block(2 * (1 - x) + (1 - k))
        left_mate(1 - x).start()
        l_side_s[...] = left_block(2 * (1 - x) + k)
        l_mate_s[x] = left_block(2 * x + (1 - k))
        left_mate(x).start()
        left_mate(1 - x).wait_recv()
        l_side_s[...] = l_side_s[...] + l_mate_r[1 - x]
        left_side().start()
        l_y[...] = left_block(2 * x + k)

    def left_reduce_finish():
        left_mate(x).wait_recv()
        l_y[...] = l_y[...] + l_mate_r[x]
        left_side().wait_recv()
        l_y[...] = l_y[...] + l_side_r[...]
        left_side().wait_send()
        for a in range(2):
            left_mate(a).wait_send()

    def right_send(t):
        return remote(r_ps.at[t], r_pr.at[t], ps_sem.at[t], pr_sem.at[t], 1 - y, col)

    def right_part(b, h):
        total = None
        for s in range(4):
            part = dot(r_xt[s, h], r_a[b, s * r_nb + h * piece : s * r_nb + (h + 1) * piece, :])
            total = part if total is None else total + part
        return total

    def right_early(h):
        def one(t, carry):
            if h == 0:
                r_fetch(t).wait()
                r_ps[t] = right_part(t, h)
            else:
                r_ps[t] = r_ps[t] + right_part(t, h)
            return carry

        lax.fori_loop(0, TILES, one, 0)

    def right_others(last):
        def one(t, carry):
            r_ps[t] = r_ps[t] + right_part(t, CHUNKS - 1)
            if not last:
                right_send(t).start()
            r_fetch(t + RING).start()
            return carry

        lax.fori_loop(0, TILES, one, 0)

    def right_own(last, begin, end):
        def one(i, carry):
            t = i + TILES
            r_fetch(t).wait()
            b = t % RING
            total = None
            for h in range(CHUNKS):
                part = right_part(b, h)
                total = part if total is None else total + part
            r_y[:, pl.ds(pl.multiple_of(i * tile, tile), tile)] = total
            if not last:
                r_fetch(lax.rem(t + RING, 2 * TILES)).start()
            return carry

        lax.fori_loop(begin, end, one, 0)

    def left_gram():
        with jax.named_scope("l_red"):
            left_reduce_finish()
        half = l_y[...].astype(BF16)
        pack(0, dot_nt(half, half))

    def right_reduce_finish():
        gram = None
        for t in range(TILES):
            if t == TILES - 1:
                left_gram()
            right_send(t).wait_recv()
            res = r_y[:, t * tile : (t + 1) * tile] + r_pr[t]
            r_y[:, t * tile : (t + 1) * tile] = res
            half = res.astype(BF16)
            part = dot_nt(half, half)
            gram = part if gram is None else gram + part
        pack(1, gram)
        for t in range(TILES):
            right_send(t).wait_send()

    low_lane = lax.broadcasted_iota(jnp.int32, (32, S), 1)
    tall_row = lax.broadcasted_iota(jnp.int32, (S, S), 0)
    tall_lane = lax.broadcasted_iota(jnp.int32, (S, S), 1)
    count = jnp.where(k == 0, float(l_n), float(r_n))

    def pack(i, gram):
        g_loc[i, :64, :] = gram[:64]
        g_loc[i, 64:96, :] = jnp.where(low_lane < 64, pltpu.roll(gram[64:96], 64, axis=1), gram[96:])

    def sum_across(par, rows, after_sends=lambda: None):
        part = pl.ds(0, rows)
        one = remote(g_loc.at[1 - k, part], g_one.at[par, part], a1s_sem.at[par], a1r_sem.at[par], y, mate)
        one.start()
        with jax.named_scope("ar_one"):
            one.wait_recv()
        g_sum[part, :] = g_loc[k, part, :] + g_one[par, part, :]
        twos = []
        for q in (2, 1, 0):
            yd = y + ((q + 1) // 2) * (1 - 2 * y)
            xd = x + ((q + 1) % 2) * (1 - 2 * x)
            two = remote(
                g_sum.at[part], g_two.at[par, q, part], a2s_sem.at[par, q], a2r_sem.at[par, q], yd, 2 * xd + k
            )
            two.start()
            twos.append(two)
        after_sends()
        with jax.named_scope("ar_two"):
            for two in twos:
                two.wait_recv()
        total = (g_sum[part, :] + g_two[par, 0, part, :]) + (g_two[par, 1, part, :] + g_two[par, 2, part, :])
        one.wait_send()
        for two in twos:
            two.wait_send()
        return total / count

    def hand_over(par, left_work, right_work):
        mine, other = g_fac.at[k], g_fac.at[1 - k]
        copy = remote(mine, mine, a3s_sem.at[par], a3r_sem.at[par], y, mate)
        back = remote(other, other, a3s_sem.at[par], a3r_sem.at[par], y, mate)
        copy.start()

        @pl.when(k == 0)
        def _():
            left_work()
            back.wait_recv()
            right_work()

        @pl.when(k == 1)
        def _():
            right_work()
            back.wait_recv()
            left_work()

        copy.wait_send()

    def factor(par):
        gram = sum_across(par, 96)
        g_m[:64, :] = gram[:64]
        g_m[64:96, :] = pltpu.roll(gram[64:], 64, axis=1)
        g_m[96:, :] = gram[64:]
        with jax.named_scope("chol"):
            inverse_factor(g_m)
        g_fac[k] = jnp.where(tall_lane <= tall_row, g_m[...], 0.0)

    def apply_piece(o, lhs, start, width):
        high, mid, low = split(o.y[:, start : start + width])
        rhs = jnp.concatenate([high, high, mid, mid, low, high], axis=0)
        return dot(lhs, rhs)

    def apply_lhs(o):
        high, mid, low = split(g_fac[o.i])
        return jnp.concatenate([high, mid, high, mid, high, low], axis=1)

    def second_gram(o):
        lhs = apply_lhs(o)
        for start in range(0, o.nb, 256):
            res = apply_piece(o, lhs, start, 256)
            o.y[:, start : start + 256] = res
            parts = split(res)
            for q in range(3):
                o.sp[q * S : (q + 1) * S, start : start + 256] = parts[q]
        both = dot_nt(o.sp[: 2 * S, :], o.sp[: 2 * S, :])
        cross = dot_nt(o.sp[:S, :], o.sp[2 * S :, :])
        pack(o.i, both[:S, :S] + ((both[:S, S:] + both[S:, :S]) + (both[S:, S:] + (cross + cross.T))))

    def high_dot_nt(lhs, rhs):
        return lax.dot_general(lhs, rhs, NT, precision=lax.Precision.HIGHEST, preferred_element_type=F32)

    def new_left():
        lhs = apply_lhs(left)
        for start in range(0, l_nb, 256):
            res = apply_piece(left, lhs, start, 256)
            l_y[:, start : start + 256] = res
            l_xs[:, start : start + 256] = res.astype(BF16)

    def new_right():
        lhs = apply_lhs(right)
        for h in range(CHUNKS):
            for start in range(h * piece, (h + 1) * piece, 256):
                res = apply_piece(right, lhs, start, 256)
                r_y[:, start : start + 256] = res
                r_xs[h, :, start - h * piece : start - h * piece + 256] = res.astype(BF16)
            later.start(h)

    def multiply(last, after_relay=lambda: None, after_left=lambda: None):
        with jax.named_scope("r_mul0"):
            right_others(last)
        with jax.named_scope("l_relay"):
            left_relay()
            after_relay()
        with jax.named_scope("r_mul1"):
            right_own(last, 0, 2)
        with jax.named_scope("l_fin"):
            left_finish()
        with jax.named_scope("l_mul"):
            left_multiply()
            after_left()
        with jax.named_scope("r_mul2"):
            right_own(last, 2, TILES)

    first, later = Gather(True), Gather(False)
    for h in range(CHUNKS):
        for b in range(piece // S):
            r_xs[h, :, b * S : (b + 1) * S] = r_start[h * piece + b * S : h * piece + (b + 1) * S, :].T.astype(BF16)
        first.start(h)
    for b in range(l_nb // S):
        l_xs[:, b * S : (b + 1) * S] = l_start[b * S : (b + 1) * S, :].T.astype(BF16)
    left_start()
    with jax.named_scope("gather_first"):
        first.finish()
    first.drain()
    l_load.wait()

    def sweep(i, carry):
        multiply(False)
        with jax.named_scope("r_red"):
            right_reduce_finish()
        left_drain()
        pl.when(i > 0)(later.drain)
        with jax.named_scope("factor0"):
            factor(0)
        with jax.named_scope("gram2"):
            hand_over(0, lambda: second_gram(left), lambda: second_gram(right))
        with jax.named_scope("factor1"):
            factor(1)
        with jax.named_scope("new_basis"):
            hand_over(1, new_left, new_right)
            left_start()
        with jax.named_scope("gather"):
            later.finish()
        return carry

    lax.fori_loop(0, SWEEPS, sweep, 0)

    stays = (x == y) & (k == y)

    def swap(c):
        return remote(r_keep.at[0, c], r_keep.at[1, c], es_sem.at[c], er_sem.at[c], 1 - y, col)

    def home(q, c):
        place = 2 * k + (y if q == 0 else 1 - y)
        return remote(r_keep.at[q, c], r_pr.at[c], xs_sem.at[q, c], xr_sem.at[c], y, place)

    def pass_on(c):
        @pl.when(x == y)
        def _():
            home(1, c).start()

    def own_home(c):
        @pl.when((x == y) & (k != y))
        def _():
            home(0, c).start()

    def after_relay():
        own_home(0)
        own_home(1)

    def after_left():
        swap(0).wait_recv()
        pass_on(0)
        own_home(2)

    for c in range(TILES):
        r_keep[0, c] = r_y[:, c * tile : (c + 1) * tile]
        swap(c).start()
    l_out[...] = l_y[...]
    with jax.named_scope("last_mul"):
        multiply(True, after_relay, after_left)
    with jax.named_scope("ray"):
        total = high_dot_nt(r_keep[1, 0], r_ps[0])
        for c in range(TILES):
            total = total + high_dot_nt(r_keep[0, c], r_y[:, c * tile : (c + 1) * tile])
        for c in range(1, TILES):
            if c == TILES - 1:
                with jax.named_scope("l_red"):
                    left_reduce_finish()
                g_loc[0] = high_dot_nt(l_out[...], l_y[...])
            with jax.named_scope("swap"):
                swap(c).wait_recv()
            if c == 1:
                pass_on(c)
            total = total + high_dot_nt(r_keep[1, c], r_ps[c])
        g_loc[1] = total

    def rest_home():
        pass_on(2)
        own_home(3)
        pass_on(3)

    with jax.named_scope("last_sum"):
        g_fac[k] = sum_across(2, S, rest_home)
    left_drain()
    later.drain()
    with jax.named_scope("last_hand"):
        hand_over(2, lambda: None, lambda: None)
    ray_out[...] = g_fac[...]
    with jax.named_scope("home"):
        for c in range(TILES):
            swap(c).wait_send()

            @pl.when(x == y)
            def _():
                home(1, c).wait_send()

            @pl.when((x == y) & (k != y))
            def _():
                home(0, c).wait_send()

            @pl.when(stays)
            def _():
                r_out[:, c * tile : (c + 1) * tile] = r_keep[0, c]

            @pl.when(jnp.logical_not(stays))
            def _():
                home(0, c).wait_recv()
                r_out[:, c * tile : (c + 1) * tile] = r_pr[c]


def finish_kernel(l_in, r_in, ray_in, l_out, l_ray, r_out, r_ray):
    for src, dst in ((l_in, l_out), (r_in, r_out)):
        for b in range(dst.shape[0] // S):
            dst[b * S : (b + 1) * S, :] = src[:, b * S : (b + 1) * S].T
    l_ray[...] = ray_in[0]
    r_ray[...] = ray_in[1]


def solution(mesh):
    def local_program(left_op, left_start, right_op, right_start):
        l_nb, r_nb = left_op.shape[0] // 4, right_op.shape[0] // 4
        dma = pltpu.SemaphoreType.DMA
        vmem = pl.BlockSpec(memory_space=pltpu.VMEM)
        hbm = pl.BlockSpec(memory_space=pl.ANY)
        shape = jax.ShapeDtypeStruct
        left_t, right_t, rayleigh = pl.pallas_call(
            kernel,
            out_shape=(shape((S, l_nb), F32), shape((S, r_nb), F32), shape((2, S, S), F32)),
            in_specs=[hbm, vmem, hbm, vmem],
            out_specs=(vmem, vmem, vmem),
            scratch_shapes=[
                pltpu.VMEM(left_op.shape, BF16),
                pltpu.VMEM((RING, right_op.shape[0], r_nb // TILES), BF16),
                pltpu.VMEM((S, l_nb), BF16),
                pltpu.VMEM((2, S, l_nb), BF16),
                pltpu.VMEM((2, S, l_nb), F32),
                pltpu.VMEM((2, S, l_nb), F32),
                pltpu.VMEM((S, l_nb), F32),
                pltpu.VMEM((S, l_nb), F32),
                pltpu.VMEM((S, l_nb), BF16),
                pltpu.VMEM((S, l_nb), F32),
                pltpu.VMEM((3 * S, l_nb), BF16),
                pltpu.VMEM((CHUNKS, S, r_nb // CHUNKS), BF16),
                pltpu.VMEM((4, CHUNKS, S, r_nb // CHUNKS), BF16),
                pltpu.VMEM((TILES, S, r_nb // TILES), F32),
                pltpu.VMEM((TILES, S, r_nb // TILES), F32),
                pltpu.VMEM((S, r_nb), F32),
                pltpu.VMEM((3 * S, r_nb), BF16),
                pltpu.VMEM((2, TILES, S, r_nb // TILES), F32),
                pltpu.VMEM((2, S, S), F32),
                pltpu.VMEM((3, S, S), F32),
                pltpu.VMEM((S, S), F32),
                pltpu.VMEM((3, 3, S, S), F32),
                pltpu.VMEM((S, S), F32),
                pltpu.VMEM((2, S, S), F32),
                dma, dma((RING,)),
                dma((2, CHUNKS)), dma((2, CHUNKS)), dma((2, CHUNKS)), dma((2, CHUNKS)),
                dma((TILES,)), dma((TILES,)), dma((2, TILES)), dma((TILES,)), dma((TILES,)), dma((TILES,)),
                dma((2,)), dma((2,)), dma, dma, dma((2,)), dma((2,)), dma, dma,
                dma((3,)), dma((3,)), dma((3, 3)), dma((3, 3)), dma((3,)), dma((3,)),
            ],
            compiler_params=pltpu.CompilerParams(has_side_effects=True, vmem_limit_bytes=64 * 1024 * 1024 - 65536),
        )(left_op, left_start, right_op, right_start)
        left_basis, left_ray, right_basis, right_ray = pl.pallas_call(
            finish_kernel,
            out_shape=(shape((l_nb, S), F32), shape((S, S), F32), shape((r_nb, S), F32), shape((S, S), F32)),
            in_specs=[vmem] * 3,
            out_specs=(vmem,) * 4,
        )(left_t, right_t, rayleigh)
        return left_basis, left_ray, right_basis, right_ray

    op_spec = P(("batch", "row"), "col")
    vec_spec = P(("batch", "row", "col"), None)
    small_spec = P("batch", None)
    return jax.shard_map(
        local_program, mesh=mesh, in_specs=(op_spec, vec_spec, op_spec, vec_spec),
        out_specs=(vec_spec, small_spec, vec_spec, small_spec), check_vma=False,
    )
```

```python
import jax
import jax.numpy as jnp
from jax import lax
from jax.experimental import pallas as pl
from jax.experimental.pallas import tpu as pltpu
from jax.sharding import PartitionSpec as P


SWEEPS = 4
S = 128
RING = 4
TILES = 4
CHUNKS = 2
PANEL = 16
MESH = pl.DeviceIdType.MESH
F32, BF16 = jnp.float32, jnp.bfloat16
NT = (((1,), (1,)), ((), ()))
TN = (((0,), (0,)), ((), ()))


def dot(lhs, rhs):
    return jnp.dot(lhs, rhs, preferred_element_type=F32)


def dot_nt(lhs, rhs):
    return lax.dot_general(lhs, rhs, NT, preferred_element_type=F32)


def split(value):
    high = value.astype(BF16)
    rest = value - high.astype(F32)
    mid = rest.astype(BF16)
    low = (rest - mid.astype(F32)).astype(BF16)
    return high, mid, low


def remote(src, dst, send_sem, recv_sem, row, col):
    return pltpu.make_async_remote_copy(
        src_ref=src, dst_ref=dst, send_sem=send_sem, recv_sem=recv_sem,
        device_id={"row": row, "col": col}, device_id_type=MESH,
    )


def inverse_factor(ref):
    sub = lax.broadcasted_iota(jnp.int32, (PANEL, S), 0)
    lane = lax.broadcasted_iota(jnp.int32, (PANEL, S), 1)

    tall_row = lax.broadcasted_iota(jnp.int32, (S, S), 0)
    tall_lane = lax.broadcasted_iota(jnp.int32, (S, S), 1)

    def panel(p, carry):
        k0 = pl.multiple_of(p * PANEL, PANEL)
        inside = (tall_lane >= k0) & (tall_lane < k0 + PANEL) & (tall_row >= k0 + PANEL)
        at = lane - k0
        rows = ref[pl.ds(k0, PANEL), :]
        heads = jnp.stack(
            [
                jnp.broadcast_to(jnp.sum(jnp.where(at == j, rows, 0.0), axis=1, keepdims=True), (PANEL, S))
                for j in range(PANEL)
            ]
        )
        high, mid, low = split(jnp.where(at >= PANEL, rows, 0.0))
        cols = jnp.concatenate([high, mid, high, mid, high, low], axis=0)
        rows = jnp.where((at >= 0) & (at < PANEL), jnp.where(at == sub, 1.0, 0.0), rows)
        done = rows
        piv = heads[0, 0:1, :]
        for j in range(PANEL):
            here = sub == j
            root = lax.rsqrt(piv)
            inv = root * root
            done = jnp.where(here, rows * root, done)
            mult = jnp.where(here, 0.0, heads[0])
            if j < PANEL - 1:
                head_rows = heads[1:, j : j + 1, :] * inv
                piv = heads[1, j + 1 : j + 2, :] - heads[0, j + 1 : j + 2, :] * head_rows[0]
                heads = jnp.where(here[None], head_rows, heads[1:] - mult[None] * head_rows)
            scaled = rows[j : j + 1, :] * inv
            rows = jnp.where(here, scaled, rows - mult * scaled)
        high, mid, low = split(rows)
        rhs = jnp.concatenate([high, high, mid, mid, low, high], axis=0)
        change = lax.dot_general(cols, rhs, TN, preferred_element_type=F32)
        ref[...] = jnp.where(inside, 0.0, ref[...]) - change
        ref[pl.ds(k0, PANEL), :] = done
        return carry

    lax.fori_loop(0, S // PANEL, panel, 0)


class Op:
    def __init__(self, **refs):
        self.__dict__.update(refs)


def kernel(
    l_op, l_start, r_op, r_start,
    l_out, r_out, ray_out,
    l_a, r_a,
    l_xs, l_xt, l_mate_s, l_mate_r, l_side_s, l_side_r, l_hand, l_y, l_sp,
    r_xs, r_xt, r_ps, r_pr, r_y, r_sp, r_keep,
    g_loc, g_one, g_sum, g_two, g_m, g_fac,
    l_asem, r_asem,
    gs_sem, gr_sem, fs_sem, fr_sem, ps_sem, pr_sem, xs_sem, xr_sem, es_sem, er_sem,
    lgs_sem, lgr_sem, lhs_sem, lhr_sem, lms_sem, lmr_sem, lss_sem, lsr_sem,
    a1s_sem, a1r_sem, a2s_sem, a2r_sem, a3s_sem, a3r_sem,
):
    y = lax.axis_index("row")
    col = lax.axis_index("col")
    x = col // 2
    k = col % 2
    mate = x * 2 + (1 - k)
    l_n, r_n = l_op.shape[0] * 2, r_op.shape[0] * 2
    l_nb, r_nb = l_n // 8, r_n // 8
    tile = r_nb // TILES
    piece = r_nb // CHUNKS

    left = Op(i=0, n=l_n, nb=l_nb, y=l_y, sp=l_sp)
    right = Op(i=1, n=r_n, nb=r_nb, y=r_y, sp=r_sp)
    ops = [left, right]

    def r_fetch(t):
        half = jnp.where(t < TILES, 1 - y, y)
        start = pl.multiple_of(half * r_nb + (t % TILES) * tile, tile)
        return pltpu.make_async_copy(r_op.at[:, pl.ds(start, tile)], r_a.at[t % RING], r_asem.at[t % RING])

    for t in range(RING):
        r_fetch(t).start()
    l_load = pltpu.make_async_copy(l_op, l_a, l_asem)
    l_load.start()

    class Gather:
        def __init__(self, first):
            self.dest_row = y if first else x
            self.my_slot = 2 * x + k if first else 2 * k + y
            self.src = x if first else y
            self.slots = [2 * a + k if first else 2 * k + a for a in range(2)]
            self.other_slots = [2 * a + (1 - k) if first else 2 * (1 - k) + a for a in range(2)]
            self.sends_to_self = [(self.dest_row == y) & (x == a) for a in range(2)]
            self.gets_from_self = [(x == a) if first else ((x == y) & (y == a)) for a in range(2)]

        def copy(self, a, h, recv):
            return remote(
                r_xs.at[h], r_xt.at[self.my_slot, h], gs_sem.at[a, h], gr_sem.at[recv, h], self.dest_row, 2 * a + k
            )

        def forward(self, a, h, slots):
            ref = r_xt.at[slots[a], h]
            return remote(ref, ref, fs_sem.at[a, h], fr_sem.at[a, h], y, mate)

        def start(self, h):
            for a in range(2):

                @pl.when(self.sends_to_self[a])
                def _():
                    r_xt[self.my_slot, h] = r_xs[h]

                @pl.when(jnp.logical_not(self.sends_to_self[a]))
                def _():
                    self.copy(a, h, self.src).start()

        def finish(self):
            for h in range(CHUNKS):
                for a in range(2):

                    @pl.when(jnp.logical_not(self.gets_from_self[a]))
                    def _():
                        self.copy(0, h, a).wait_recv()

                    self.forward(a, h, self.slots).start()
                for a in range(2):
                    self.forward(a, h, self.other_slots).wait_recv()
                if h < CHUNKS - 1:
                    right_early(h)

        def drain(self):
            for h in range(CHUNKS):
                for a in range(2):
                    self.forward(a, h, self.slots).wait_send()

                    @pl.when(jnp.logical_not(self.sends_to_self[a]))
                    def _():
                        self.copy(a, h, self.src).wait_send()

    def left_copy(b, slot):
        return remote(l_xs, l_xt.at[slot], lgs_sem.at[b], lgr_sem.at[slot], b, 2 * y + x)

    def left_across(b):
        return remote(l_xs, l_hand, lgs_sem.at[b], lhr_sem, 1 - y, col)

    def left_hand_on():
        return remote(l_hand, l_xt.at[k], lhs_sem, lgr_sem.at[k], y, 2 * (1 - x) + x)

    def left_self(b):
        return (b == y) & (y == x) & (x == k)

    def left_start():
        for b in (1 - y, y):
            across = (b != y) & (x != y)

            @pl.when(left_self(b))
            def _():
                l_xt[k] = l_xs[...]

            @pl.when(across)
            def _():
                left_across(b).start()

            @pl.when(jnp.logical_not(left_self(b) | across))
            def _():
                left_copy(b, k).start()

    def left_relay():
        @pl.when(x == y)
        def _():
            left_across(0).wait_recv()
            left_hand_on().start()

    def left_finish():
        for slot in range(2):

            @pl.when(jnp.logical_not((y == x) & (x == k) & (k == slot)))
            def _():
                left_copy(0, slot).wait_recv()

    def left_drain():
        for b in range(2):

            @pl.when(jnp.logical_not(left_self(b)))
            def _():
                left_copy(b, k).wait_send()

        @pl.when(x == y)
        def _():
            left_hand_on().wait_send()

    def left_block(index):
        rows = pl.ds(pl.multiple_of(index * l_nb, l_nb), l_nb)
        return dot_nt(l_xt[0], l_a[rows, :l_nb]) + dot_nt(l_xt[1], l_a[rows, l_nb:])

    def left_mate(a):
        return remote(l_mate_s.at[a], l_mate_r.at[a], lms_sem.at[a], lmr_sem.at[a], y, mate)

    def left_side():
        return remote(l_side_s, l_side_r, lss_sem, lsr_sem, y, 2 * (1 - x) + k)

    def left_multiply():
        l_mate_s[1 - x] = left_block(2 * (1 - x) + (1 - k))
        left_mate(1 - x).start()
        l_side_s[...] = left_block(2 * (1 - x) + k)
        l_mate_s[x] = left_block(2 * x + (1 - k))
        left_mate(x).start()
        left_mate(1 - x).wait_recv()
        l_side_s[...] = l_side_s[...] + l_mate_r[1 - x]
        left_side().start()
        l_y[...] = left_block(2 * x + k)

    def left_reduce_finish():
        left_mate(x).wait_recv()
        l_y[...] = l_y[...] + l_mate_r[x]
        left_side().wait_recv()
        l_y[...] = l_y[...] + l_side_r[...]
        left_side().wait_send()
        for a in range(2):
            left_mate(a).wait_send()

    def right_send(t):
        return remote(r_ps.at[t], r_pr.at[t], ps_sem.at[t], pr_sem.at[t], 1 - y, col)

    def right_part(b, h):
        total = None
        for s in range(4):
            part = dot(r_xt[s, h], r_a[b, s * r_nb + h * piece : s * r_nb + (h + 1) * piece, :])
            total = part if total is None else total + part
        return total

    def right_early(h):
        def one(t, carry):
            if h == 0:
                r_fetch(t).wait()
                r_ps[t] = right_part(t, h)
            else:
                r_ps[t] = r_ps[t] + right_part(t, h)
            return carry

        lax.fori_loop(0, TILES, one, 0)

    def right_others(last):
        def one(t, carry):
            r_ps[t] = r_ps[t] + right_part(t, CHUNKS - 1)
            if not last:
                right_send(t).start()
            r_fetch(t + RING).start()
            return carry

        lax.fori_loop(0, TILES, one, 0)

    def right_own(last, begin, end):
        def one(i, carry):
            t = i + TILES
            r_fetch(t).wait()
            b = t % RING
            total = None
            for h in range(CHUNKS):
                part = right_part(b, h)
                total = part if total is None else total + part
            r_y[:, pl.ds(pl.multiple_of(i * tile, tile), tile)] = total
            if not last:
                r_fetch(lax.rem(t + RING, 2 * TILES)).start()
            return carry

        lax.fori_loop(begin, end, one, 0)

    def left_gram():
        with jax.named_scope("l_red"):
            left_reduce_finish()
        half = l_y[...].astype(BF16)
        pack(0, dot_nt(half, half))

    def right_reduce_finish():
        gram = None
        for t in range(TILES):
            if t == TILES - 1:
                left_gram()
            right_send(t).wait_recv()
            res = r_y[:, t * tile : (t + 1) * tile] + r_pr[t]
            r_y[:, t * tile : (t + 1) * tile] = res
            half = res.astype(BF16)
            part = dot_nt(half, half)
            gram = part if gram is None else gram + part
        pack(1, gram)
        for t in range(TILES):
            right_send(t).wait_send()

    low_lane = lax.broadcasted_iota(jnp.int32, (32, S), 1)
    tall_row = lax.broadcasted_iota(jnp.int32, (S, S), 0)
    tall_lane = lax.broadcasted_iota(jnp.int32, (S, S), 1)
    count = jnp.where(k == 0, float(l_n), float(r_n))

    def pack(i, gram):
        g_loc[i, :64, :] = gram[:64]
        g_loc[i, 64:96, :] = jnp.where(low_lane < 64, pltpu.roll(gram[64:96], 64, axis=1), gram[96:])

    def sum_across(par, rows, after_sends=lambda: None):
        part = pl.ds(0, rows)
        one = remote(g_loc.at[1 - k, part], g_one.at[par, part], a1s_sem.at[par], a1r_sem.at[par], y, mate)
        one.start()
        with jax.named_scope("ar_one"):
            one.wait_recv()
        g_sum[part, :] = g_loc[k, part, :] + g_one[par, part, :]
        twos = []
        for q in (2, 1, 0):
            yd = y + ((q + 1) // 2) * (1 - 2 * y)
            xd = x + ((q + 1) % 2) * (1 - 2 * x)
            two = remote(
                g_sum.at[part], g_two.at[par, q, part], a2s_sem.at[par, q], a2r_sem.at[par, q], yd, 2 * xd + k
            )
            two.start()
            twos.append(two)
        after_sends()
        with jax.named_scope("ar_two"):
            for two in twos:
                two.wait_recv()
        total = (g_sum[part, :] + g_two[par, 0, part, :]) + (g_two[par, 1, part, :] + g_two[par, 2, part, :])
        one.wait_send()
        for two in twos:
            two.wait_send()
        return total / count

    def hand_over(par, left_work, right_work):
        mine, other = g_fac.at[k], g_fac.at[1 - k]
        copy = remote(mine, mine, a3s_sem.at[par], a3r_sem.at[par], y, mate)
        back = remote(other, other, a3s_sem.at[par], a3r_sem.at[par], y, mate)
        copy.start()

        @pl.when(k == 0)
        def _():
            left_work()
            back.wait_recv()
            right_work()

        @pl.when(k == 1)
        def _():
            right_work()
            back.wait_recv()
            left_work()

        copy.wait_send()

    def factor(par):
        gram = sum_across(par, 96)
        g_m[:64, :] = gram[:64]
        g_m[64:96, :] = pltpu.roll(gram[64:], 64, axis=1)
        g_m[96:, :] = gram[64:]
        with jax.named_scope("chol"):
            inverse_factor(g_m)
        g_fac[k] = jnp.where(tall_lane <= tall_row, g_m[...], 0.0)

    def apply_piece(o, lhs, start, width):
        high, mid, low = split(o.y[:, start : start + width])
        rhs = jnp.concatenate([high, high, mid, mid, low, high], axis=0)
        return dot(lhs, rhs)

    def apply_lhs(o):
        high, mid, low = split(g_fac[o.i])
        return jnp.concatenate([high, mid, high, mid, high, low], axis=1)

    def second_gram(o):
        lhs = apply_lhs(o)
        for start in range(0, o.nb, 256):
            res = apply_piece(o, lhs, start, 256)
            o.y[:, start : start + 256] = res
            parts = split(res)
            for q in range(3):
                o.sp[q * S : (q + 1) * S, start : start + 256] = parts[q]
        both = dot_nt(o.sp[: 2 * S, :], o.sp[: 2 * S, :])
        cross = dot_nt(o.sp[:S, :], o.sp[2 * S :, :])
        pack(o.i, both[:S, :S] + ((both[:S, S:] + both[S:, :S]) + (both[S:, S:] + (cross + cross.T))))

    def high_dot_nt(lhs, rhs):
        return lax.dot_general(lhs, rhs, NT, precision=lax.Precision.HIGHEST, preferred_element_type=F32)

    def new_left():
        lhs = apply_lhs(left)
        for start in range(0, l_nb, 256):
            res = apply_piece(left, lhs, start, 256)
            l_y[:, start : start + 256] = res
            l_xs[:, start : start + 256] = res.astype(BF16)

    def new_right():
        lhs = apply_lhs(right)
        for h in range(CHUNKS):
            for start in range(h * piece, (h + 1) * piece, 256):
                res = apply_piece(right, lhs, start, 256)
                r_y[:, start : start + 256] = res
                r_xs[h, :, start - h * piece : start - h * piece + 256] = res.astype(BF16)
            later.start(h)

    def multiply(last, after_relay=lambda: None, after_left=lambda: None):
        with jax.named_scope("r_mul0"):
            right_others(last)
        with jax.named_scope("l_relay"):
            left_relay()
            after_relay()
        with jax.named_scope("r_mul1"):
            right_own(last, 0, 2)
        with jax.named_scope("l_fin"):
            left_finish()
        with jax.named_scope("l_mul"):
            left_multiply()
            after_left()
        with jax.named_scope("r_mul2"):
            right_own(last, 2, TILES)

    first, later = Gather(True), Gather(False)
    for h in range(CHUNKS):
        for b in range(piece // S):
            r_xs[h, :, b * S : (b + 1) * S] = r_start[h * piece + b * S : h * piece + (b + 1) * S, :].T.astype(BF16)
        first.start(h)
    for b in range(l_nb // S):
        l_xs[:, b * S : (b + 1) * S] = l_start[b * S : (b + 1) * S, :].T.astype(BF16)
    left_start()
    with jax.named_scope("gather_first"):
        first.finish()
    first.drain()
    l_load.wait()

    def sweep(i, carry):
        multiply(False)
        with jax.named_scope("r_red"):
            right_reduce_finish()
        left_drain()
        pl.when(i > 0)(later.drain)
        with jax.named_scope("factor0"):
            factor(0)
        with jax.named_scope("gram2"):
            hand_over(0, lambda: second_gram(left), lambda: second_gram(right))
        with jax.named_scope("factor1"):
            factor(1)
        with jax.named_scope("new_basis"):
            hand_over(1, new_left, new_right)
            left_start()
        with jax.named_scope("gather"):
            later.finish()
        return carry

    lax.fori_loop(0, SWEEPS, sweep, 0)

    stays = (x == y) & (k == y)

    def swap(c):
        return remote(r_keep.at[0, c], r_keep.at[1, c], es_sem.at[c], er_sem.at[c], 1 - y, col)

    def home(q, c):
        place = 2 * k + (y if q == 0 else 1 - y)
        return remote(r_keep.at[q, c], r_pr.at[c], xs_sem.at[q, c], xr_sem.at[c], y, place)

    direct = (x != y) & (k == y)
    passes_last = (x == y) & (k == y)
    straight = remote(
        r_keep.at[0, TILES - 1], r_pr.at[TILES - 1], xs_sem.at[0, TILES - 1], xr_sem.at[TILES - 1], x, 2 * k + y
    )

    def pass_on(c):
        @pl.when(x == y)
        def _():
            home(1, c).start()

    def own_home(c):
        @pl.when((x == y) & (k != y))
        def _():
            home(0, c).start()

    def after_relay():
        own_home(0)
        own_home(1)

    def after_left():
        swap(0).wait_recv()
        pass_on(0)
        own_home(2)

    for c in range(TILES):
        r_keep[0, c] = r_y[:, c * tile : (c + 1) * tile]
        swap(c).start()
    l_out[...] = l_y[...]
    with jax.named_scope("last_mul"):
        multiply(True, after_relay, after_left)
    with jax.named_scope("ray"):
        total = high_dot_nt(r_keep[1, 0], r_ps[0])
        for c in range(TILES):
            total = total + high_dot_nt(r_keep[0, c], r_y[:, c * tile : (c + 1) * tile])
        for c in range(1, TILES):
            if c == TILES - 1:
                with jax.named_scope("l_red"):
                    left_reduce_finish()
                g_loc[0] = high_dot_nt(l_out[...], l_y[...])
            with jax.named_scope("swap"):
                swap(c).wait_recv()
            if c == 1:
                pass_on(c)
            total = total + high_dot_nt(r_keep[1, c], r_ps[c])
        g_loc[1] = total

    def rest_home():
        own_home(TILES - 1)
        for c in range(2, TILES - 1):
            pass_on(c)

        @pl.when(passes_last)
        def _():
            home(1, TILES - 1).start()

        @pl.when(direct)
        def _():
            straight.start()


    with jax.named_scope("last_sum"):
        g_fac[k] = sum_across(2, S, rest_home)
    left_drain()
    later.drain()
    with jax.named_scope("last_hand"):
        hand_over(2, lambda: None, lambda: None)
    ray_out[...] = g_fac[...]
    with jax.named_scope("home"):
        for c in range(TILES):
            swap(c).wait_send()

            @pl.when(passes_last if c == TILES - 1 else x == y)
            def _():
                home(1, c).wait_send()

            if c == TILES - 1:

                @pl.when(direct)
                def _():
                    straight.wait_send()

            @pl.when((x == y) & (k != y))
            def _():
                home(0, c).wait_send()

            @pl.when(stays)
            def _():
                r_out[:, c * tile : (c + 1) * tile] = r_keep[0, c]

            @pl.when(jnp.logical_not(stays))
            def _():
                home(0, c).wait_recv()
                r_out[:, c * tile : (c + 1) * tile] = r_pr[c]


def finish_kernel(l_in, r_in, ray_in, l_out, l_ray, r_out, r_ray):
    for src, dst in ((l_in, l_out), (r_in, r_out)):
        for b in range(dst.shape[0] // S):
            dst[b * S : (b + 1) * S, :] = src[:, b * S : (b + 1) * S].T
    l_ray[...] = ray_in[0]
    r_ray[...] = ray_in[1]


def solution(mesh):
    def local_program(left_op, left_start, right_op, right_start):
        l_nb, r_nb = left_op.shape[0] // 4, right_op.shape[0] // 4
        dma = pltpu.SemaphoreType.DMA
        vmem = pl.BlockSpec(memory_space=pltpu.VMEM)
        hbm = pl.BlockSpec(memory_space=pl.ANY)
        shape = jax.ShapeDtypeStruct
        left_t, right_t, rayleigh = pl.pallas_call(
            kernel,
            out_shape=(shape((S, l_nb), F32), shape((S, r_nb), F32), shape((2, S, S), F32)),
            in_specs=[hbm, vmem, hbm, vmem],
            out_specs=(vmem, vmem, vmem),
            scratch_shapes=[
                pltpu.VMEM(left_op.shape, BF16),
                pltpu.VMEM((RING, right_op.shape[0], r_nb // TILES), BF16),
                pltpu.VMEM((S, l_nb), BF16),
                pltpu.VMEM((2, S, l_nb), BF16),
                pltpu.VMEM((2, S, l_nb), F32),
                pltpu.VMEM((2, S, l_nb), F32),
                pltpu.VMEM((S, l_nb), F32),
                pltpu.VMEM((S, l_nb), F32),
                pltpu.VMEM((S, l_nb), BF16),
                pltpu.VMEM((S, l_nb), F32),
                pltpu.VMEM((3 * S, l_nb), BF16),
                pltpu.VMEM((CHUNKS, S, r_nb // CHUNKS), BF16),
                pltpu.VMEM((4, CHUNKS, S, r_nb // CHUNKS), BF16),
                pltpu.VMEM((TILES, S, r_nb // TILES), F32),
                pltpu.VMEM((TILES, S, r_nb // TILES), F32),
                pltpu.VMEM((S, r_nb), F32),
                pltpu.VMEM((3 * S, r_nb), BF16),
                pltpu.VMEM((2, TILES, S, r_nb // TILES), F32),
                pltpu.VMEM((2, S, S), F32),
                pltpu.VMEM((3, S, S), F32),
                pltpu.VMEM((S, S), F32),
                pltpu.VMEM((3, 3, S, S), F32),
                pltpu.VMEM((S, S), F32),
                pltpu.VMEM((2, S, S), F32),
                dma, dma((RING,)),
                dma((2, CHUNKS)), dma((2, CHUNKS)), dma((2, CHUNKS)), dma((2, CHUNKS)),
                dma((TILES,)), dma((TILES,)), dma((2, TILES)), dma((TILES,)), dma((TILES,)), dma((TILES,)),
                dma((2,)), dma((2,)), dma, dma, dma((2,)), dma((2,)), dma, dma,
                dma((3,)), dma((3,)), dma((3, 3)), dma((3, 3)), dma((3,)), dma((3,)),
            ],
            compiler_params=pltpu.CompilerParams(has_side_effects=True, vmem_limit_bytes=64 * 1024 * 1024 - 65536),
        )(left_op, left_start, right_op, right_start)
        left_basis, left_ray, right_basis, right_ray = pl.pallas_call(
            finish_kernel,
            out_shape=(shape((l_nb, S), F32), shape((S, S), F32), shape((r_nb, S), F32), shape((S, S), F32)),
            in_specs=[vmem] * 3,
            out_specs=(vmem,) * 4,
        )(left_t, right_t, rayleigh)
        return left_basis, left_ray, right_basis, right_ray

    op_spec = P(("batch", "row"), "col")
    vec_spec = P(("batch", "row", "col"), None)
    small_spec = P("batch", None)
    return jax.shard_map(
        local_program, mesh=mesh, in_specs=(op_spec, vec_spec, op_spec, vec_spec),
        out_specs=(vec_spec, small_spec, vec_spec, small_spec), check_vma=False,
    )
```

```python
import jax
import jax.numpy as jnp
from jax import lax
from jax.experimental import pallas as pl
from jax.experimental.pallas import tpu as pltpu
from jax.sharding import PartitionSpec as P

SWEEPS = 4
S = 128
RING = 4
TILES = 4
CHUNKS = 2
STRAIGHT = 2
PANEL = 16
MESH = pl.DeviceIdType.MESH
F32, BF16 = jnp.float32, jnp.bfloat16
NT = (((1,), (1,)), ((), ()))
TN = (((0,), (0,)), ((), ()))


def dot(lhs, rhs):
    return jnp.dot(lhs, rhs, preferred_element_type=F32)


def dot_nt(lhs, rhs):
    return lax.dot_general(lhs, rhs, NT, preferred_element_type=F32)


def split(value):
    high = value.astype(BF16)
    rest = value - high.astype(F32)
    mid = rest.astype(BF16)
    low = (rest - mid.astype(F32)).astype(BF16)
    return high, mid, low


def remote(src, dst, send_sem, recv_sem, row, col):
    return pltpu.make_async_remote_copy(
        src_ref=src, dst_ref=dst, send_sem=send_sem, recv_sem=recv_sem,
        device_id={"row": row, "col": col}, device_id_type=MESH,
    )


def inverse_factor(ref):
    sub = lax.broadcasted_iota(jnp.int32, (PANEL, S), 0)
    lane = lax.broadcasted_iota(jnp.int32, (PANEL, S), 1)

    tall_row = lax.broadcasted_iota(jnp.int32, (S, S), 0)
    tall_lane = lax.broadcasted_iota(jnp.int32, (S, S), 1)

    def panel(p, carry):
        k0 = pl.multiple_of(p * PANEL, PANEL)
        inside = (tall_lane >= k0) & (tall_lane < k0 + PANEL) & (tall_row >= k0 + PANEL)
        at = lane - k0
        rows = ref[pl.ds(k0, PANEL), :]
        heads = jnp.stack(
            [
                jnp.broadcast_to(jnp.sum(jnp.where(at == j, rows, 0.0), axis=1, keepdims=True), (PANEL, S))
                for j in range(PANEL)
            ]
        )
        high, mid, low = split(jnp.where(at >= PANEL, rows, 0.0))
        cols = jnp.concatenate([high, mid, high, mid, high, low], axis=0)
        rows = jnp.where((at >= 0) & (at < PANEL), jnp.where(at == sub, 1.0, 0.0), rows)
        done = rows
        piv = heads[0, 0:1, :]
        for j in range(PANEL):
            here = sub == j
            root = lax.rsqrt(piv)
            inv = root * root
            done = jnp.where(here, rows * root, done)
            mult = jnp.where(here, 0.0, heads[0])
            if j < PANEL - 1:
                head_rows = heads[1:, j : j + 1, :] * inv
                piv = heads[1, j + 1 : j + 2, :] - heads[0, j + 1 : j + 2, :] * head_rows[0]
                heads = jnp.where(here[None], head_rows, heads[1:] - mult[None] * head_rows)
            scaled = rows[j : j + 1, :] * inv
            rows = jnp.where(here, scaled, rows - mult * scaled)
        high, mid, low = split(rows)
        rhs = jnp.concatenate([high, high, mid, mid, low, high], axis=0)
        change = lax.dot_general(cols, rhs, TN, preferred_element_type=F32)
        ref[...] = jnp.where(inside, 0.0, ref[...]) - change
        ref[pl.ds(k0, PANEL), :] = done
        return carry

    lax.fori_loop(0, S // PANEL, panel, 0)


class Op:
    def __init__(self, **refs):
        self.__dict__.update(refs)


def kernel(
    l_op, l_start, r_op, r_start,
    l_out, r_out, ray_out,
    l_a, r_a,
    l_xs, l_xt, l_mate_s, l_mate_r, l_side_s, l_side_r, l_hand, l_y, l_sp,
    r_xs, r_xt, r_ps, r_pr, r_y, r_sp, r_keep,
    g_loc, g_one, g_sum, g_two, g_m, g_fac,
    l_asem, r_asem,
    gs_sem, gr_sem, fs_sem, fr_sem, ps_sem, pr_sem, xs_sem, xr_sem, es_sem, er_sem,
    lgs_sem, lgr_sem, lhs_sem, lhr_sem, lms_sem, lmr_sem, lss_sem, lsr_sem,
    a1s_sem, a1r_sem, a2s_sem, a2r_sem, a3s_sem, a3r_sem,
):
    y = lax.axis_index("row")
    col = lax.axis_index("col")
    x = col // 2
    k = col % 2
    mate = x * 2 + (1 - k)
    l_n, r_n = l_op.shape[0] * 2, r_op.shape[0] * 2
    l_nb, r_nb = l_n // 8, r_n // 8
    tile = r_nb // TILES
    piece = r_nb // CHUNKS

    left = Op(i=0, n=l_n, nb=l_nb, y=l_y, sp=l_sp)
    right = Op(i=1, n=r_n, nb=r_nb, y=r_y, sp=r_sp)
    ops = [left, right]

    def r_fetch(t):
        half = jnp.where(t < TILES, 1 - y, y)
        start = pl.multiple_of(half * r_nb + (t % TILES) * tile, tile)
        return pltpu.make_async_copy(r_op.at[:, pl.ds(start, tile)], r_a.at[t % RING], r_asem.at[t % RING])

    for t in range(RING):
        r_fetch(t).start()
    l_load = pltpu.make_async_copy(l_op, l_a, l_asem)
    l_load.start()

    class Gather:
        def __init__(self, first):
            self.dest_row = y if first else x
            self.my_slot = 2 * x + k if first else 2 * k + y
            self.src = x if first else y
            self.slots = [2 * a + k if first else 2 * k + a for a in range(2)]
            self.other_slots = [2 * a + (1 - k) if first else 2 * (1 - k) + a for a in range(2)]
            self.sends_to_self = [(self.dest_row == y) & (x == a) for a in range(2)]
            self.gets_from_self = [(x == a) if first else ((x == y) & (y == a)) for a in range(2)]

        def copy(self, a, h, recv):
            return remote(
                r_xs.at[h], r_xt.at[self.my_slot, h], gs_sem.at[a, h], gr_sem.at[recv, h], self.dest_row, 2 * a + k
            )

        def forward(self, a, h, slots):
            ref = r_xt.at[slots[a], h]
            return remote(ref, ref, fs_sem.at[a, h], fr_sem.at[a, h], y, mate)

        def start(self, h):
            for a in range(2):

                @pl.when(self.sends_to_self[a])
                def _():
                    r_xt[self.my_slot, h] = r_xs[h]

                @pl.when(jnp.logical_not(self.sends_to_self[a]))
                def _():
                    self.copy(a, h, self.src).start()

        def finish(self):
            for h in range(CHUNKS):
                for a in range(2):

                    @pl.when(jnp.logical_not(self.gets_from_self[a]))
                    def _():
                        self.copy(0, h, a).wait_recv()

                    self.forward(a, h, self.slots).start()
                for a in range(2):
                    self.forward(a, h, self.other_slots).wait_recv()
                if h < CHUNKS - 1:
                    right_early(h)

        def drain(self):
            for h in range(CHUNKS):
                for a in range(2):
                    self.forward(a, h, self.slots).wait_send()

                    @pl.when(jnp.logical_not(self.sends_to_self[a]))
                    def _():
                        self.copy(a, h, self.src).wait_send()

    def left_copy(b, slot):
        return remote(l_xs, l_xt.at[slot], lgs_sem.at[b], lgr_sem.at[slot], b, 2 * y + x)

    def left_across(b):
        return remote(l_xs, l_hand, lgs_sem.at[b], lhr_sem, 1 - y, col)

    def left_hand_on():
        return remote(l_hand, l_xt.at[k], lhs_sem, lgr_sem.at[k], y, 2 * (1 - x) + x)

    def left_self(b):
        return (b == y) & (y == x) & (x == k)

    def left_start():
        for b in (1 - y, y):
            across = (b != y) & (x != y)

            @pl.when(left_self(b))
            def _():
                l_xt[k] = l_xs[...]

            @pl.when(across)
            def _():
                left_across(b).start()

            @pl.when(jnp.logical_not(left_self(b) | across))
            def _():
                left_copy(b, k).start()

    def left_relay():
        @pl.when(x == y)
        def _():
            left_across(0).wait_recv()
            left_hand_on().start()

    def left_finish():
        for slot in range(2):

            @pl.when(jnp.logical_not((y == x) & (x == k) & (k == slot)))
            def _():
                left_copy(0, slot).wait_recv()

    def left_drain():
        for b in range(2):

            @pl.when(jnp.logical_not(left_self(b)))
            def _():
                left_copy(b, k).wait_send()

        @pl.when(x == y)
        def _():
            left_hand_on().wait_send()

    def left_block(index):
        rows = pl.ds(pl.multiple_of(index * l_nb, l_nb), l_nb)
        return dot_nt(l_xt[0], l_a[rows, :l_nb]) + dot_nt(l_xt[1], l_a[rows, l_nb:])

    def left_mate(a):
        return remote(l_mate_s.at[a], l_mate_r.at[a], lms_sem.at[a], lmr_sem.at[a], y, mate)

    def left_side():
        return remote(l_side_s, l_side_r, lss_sem, lsr_sem, y, 2 * (1 - x) + k)

    def left_multiply():
        l_mate_s[1 - x] = left_block(2 * (1 - x) + (1 - k))
        left_mate(1 - x).start()
        l_side_s[...] = left_block(2 * (1 - x) + k)
        l_mate_s[x] = left_block(2 * x + (1 - k))
        left_mate(x).start()
        left_mate(1 - x).wait_recv()
        l_side_s[...] = l_side_s[...] + l_mate_r[1 - x]
        left_side().start()
        l_y[...] = left_block(2 * x + k)

    def left_reduce_finish():
        left_mate(x).wait_recv()
        l_y[...] = l_y[...] + l_mate_r[x]
        left_side().wait_recv()
        l_y[...] = l_y[...] + l_side_r[...]
        left_side().wait_send()
        for a in range(2):
            left_mate(a).wait_send()

    def right_send(t):
        return remote(r_ps.at[t], r_pr.at[t], ps_sem.at[t], pr_sem.at[t], 1 - y, col)

    def right_part(b, h):
        total = None
        for s in range(4):
            part = dot(r_xt[s, h], r_a[b, s * r_nb + h * piece : s * r_nb + (h + 1) * piece, :])
            total = part if total is None else total + part
        return total

    def right_early(h):
        def one(t, carry):
            if h == 0:
                r_fetch(t).wait()
                r_ps[t] = right_part(t, h)
            else:
                r_ps[t] = r_ps[t] + right_part(t, h)
            return carry

        lax.fori_loop(0, TILES, one, 0)

    def right_others(last):
        def one(t, carry):
            r_ps[t] = r_ps[t] + right_part(t, CHUNKS - 1)
            if not last:
                right_send(t).start()
            r_fetch(t + RING).start()
            return carry

        lax.fori_loop(0, TILES, one, 0)

    def right_own(last, begin, end):
        def one(i, carry):
            t = i + TILES
            r_fetch(t).wait()
            b = t % RING
            total = None
            for h in range(CHUNKS):
                part = right_part(b, h)
                total = part if total is None else total + part
            r_y[:, pl.ds(pl.multiple_of(i * tile, tile), tile)] = total
            if not last:
                r_fetch(lax.rem(t + RING, 2 * TILES)).start()
            return carry

        lax.fori_loop(begin, end, one, 0)

    def left_gram():
        with jax.named_scope("l_red"):
            left_reduce_finish()
        half = l_y[...].astype(BF16)
        pack(0, dot_nt(half, half))

    def right_reduce_finish():
        gram = None
        for t in range(TILES):
            if t == TILES - 1:
                left_gram()
            right_send(t).wait_recv()
            res = r_y[:, t * tile : (t + 1) * tile] + r_pr[t]
            r_y[:, t * tile : (t + 1) * tile] = res
            half = res.astype(BF16)
            part = dot_nt(half, half)
            gram = part if gram is None else gram + part
        pack(1, gram)
        for t in range(TILES):
            right_send(t).wait_send()

    low_lane = lax.broadcasted_iota(jnp.int32, (32, S), 1)
    tall_row = lax.broadcasted_iota(jnp.int32, (S, S), 0)
    tall_lane = lax.broadcasted_iota(jnp.int32, (S, S), 1)
    count = jnp.where(k == 0, float(l_n), float(r_n))

    def pack(i, gram):
        g_loc[i, :64, :] = gram[:64]
        g_loc[i, 64:96, :] = jnp.where(low_lane < 64, pltpu.roll(gram[64:96], 64, axis=1), gram[96:])

    def sum_across(par, rows, after_sends=lambda: None):
        part = pl.ds(0, rows)
        one = remote(g_loc.at[1 - k, part], g_one.at[par, part], a1s_sem.at[par], a1r_sem.at[par], y, mate)
        one.start()
        with jax.named_scope("ar_one"):
            one.wait_recv()
        g_sum[part, :] = g_loc[k, part, :] + g_one[par, part, :]
        twos = []
        for q in (2, 1, 0):
            yd = y + ((q + 1) // 2) * (1 - 2 * y)
            xd = x + ((q + 1) % 2) * (1 - 2 * x)
            two = remote(
                g_sum.at[part], g_two.at[par, q, part], a2s_sem.at[par, q], a2r_sem.at[par, q], yd, 2 * xd + k
            )
            two.start()
            twos.append(two)
        after_sends()
        with jax.named_scope("ar_two"):
            for two in twos:
                two.wait_recv()
        total = (g_sum[part, :] + g_two[par, 0, part, :]) + (g_two[par, 1, part, :] + g_two[par, 2, part, :])
        one.wait_send()
        for two in twos:
            two.wait_send()
        return total / count

    def hand_over(par, left_work, right_work):
        mine, other = g_fac.at[k], g_fac.at[1 - k]
        copy = remote(mine, mine, a3s_sem.at[par], a3r_sem.at[par], y, mate)
        back = remote(other, other, a3s_sem.at[par], a3r_sem.at[par], y, mate)
        copy.start()

        @pl.when(k == 0)
        def _():
            left_work()
            back.wait_recv()
            right_work()

        @pl.when(k == 1)
        def _():
            right_work()
            back.wait_recv()
            left_work()

        copy.wait_send()

    def factor(par):
        gram = sum_across(par, 96)
        g_m[:64, :] = gram[:64]
        g_m[64:96, :] = pltpu.roll(gram[64:], 64, axis=1)
        g_m[96:, :] = gram[64:]
        with jax.named_scope("chol"):
            inverse_factor(g_m)
        g_fac[k] = jnp.where(tall_lane <= tall_row, g_m[...], 0.0)

    def apply_piece(o, lhs, start, width):
        high, mid, low = split(o.y[:, start : start + width])
        rhs = jnp.concatenate([high, high, mid, mid, low, high], axis=0)
        return dot(lhs, rhs)

    def apply_lhs(o):
        high, mid, low = split(g_fac[o.i])
        return jnp.concatenate([high, mid, high, mid, high, low], axis=1)

    def second_gram(o):
        lhs = apply_lhs(o)
        for start in range(0, o.nb, 256):
            res = apply_piece(o, lhs, start, 256)
            o.y[:, start : start + 256] = res
            parts = split(res)
            for q in range(3):
                o.sp[q * S : (q + 1) * S, start : start + 256] = parts[q]
        both = dot_nt(o.sp[: 2 * S, :], o.sp[: 2 * S, :])
        cross = dot_nt(o.sp[:S, :], o.sp[2 * S :, :])
        pack(o.i, both[:S, :S] + ((both[:S, S:] + both[S:, :S]) + (both[S:, S:] + (cross + cross.T))))

    def high_dot_nt(lhs, rhs):
        return lax.dot_general(lhs, rhs, NT, precision=lax.Precision.HIGHEST, preferred_element_type=F32)

    def new_left():
        lhs = apply_lhs(left)
        for start in range(0, l_nb, 256):
            res = apply_piece(left, lhs, start, 256)
            l_y[:, start : start + 256] = res
            l_xs[:, start : start + 256] = res.astype(BF16)

    def new_right():
        lhs = apply_lhs(right)
        for h in range(CHUNKS):
            for start in range(h * piece, (h + 1) * piece, 256):
                res = apply_piece(right, lhs, start, 256)
                r_y[:, start : start + 256] = res
                r_xs[h, :, start - h * piece : start - h * piece + 256] = res.astype(BF16)
            later.start(h)

    def multiply(last, after_relay=lambda: None, after_left=lambda: None):
        with jax.named_scope("r_mul0"):
            right_others(last)
        with jax.named_scope("l_relay"):
            left_relay()
            after_relay()
        with jax.named_scope("r_mul1"):
            right_own(last, 0, 2)
        with jax.named_scope("l_fin"):
            left_finish()
        with jax.named_scope("l_mul"):
            left_multiply()
            after_left()
        with jax.named_scope("r_mul2"):
            right_own(last, 2, TILES)

    first, later = Gather(True), Gather(False)
    for h in range(CHUNKS):
        for b in range(piece // S):
            r_xs[h, :, b * S : (b + 1) * S] = r_start[h * piece + b * S : h * piece + (b + 1) * S, :].T.astype(BF16)
        first.start(h)
    for b in range(l_nb // S):
        l_xs[:, b * S : (b + 1) * S] = l_start[b * S : (b + 1) * S, :].T.astype(BF16)
    left_start()
    with jax.named_scope("gather_first"):
        first.finish()
    first.drain()
    l_load.wait()

    def sweep(i, carry):
        multiply(False)
        with jax.named_scope("r_red"):
            right_reduce_finish()
        left_drain()
        pl.when(i > 0)(later.drain)
        with jax.named_scope("factor0"):
            factor(0)
        with jax.named_scope("gram2"):
            hand_over(0, lambda: second_gram(left), lambda: second_gram(right))
        with jax.named_scope("factor1"):
            factor(1)
        with jax.named_scope("new_basis"):
            hand_over(1, new_left, new_right)
            left_start()
        with jax.named_scope("gather"):
            later.finish()
        return carry

    lax.fori_loop(0, SWEEPS, sweep, 0)

    stays = (x == y) & (k == y)

    def swap(c):
        return remote(r_keep.at[0, c], r_keep.at[1, c], es_sem.at[c], er_sem.at[c], 1 - y, col)

    def home(q, c):
        place = 2 * k + (y if q == 0 else 1 - y)
        return remote(r_keep.at[q, c], r_pr.at[c], xs_sem.at[q, c], xr_sem.at[c], y, place)

    direct = (x != y) & (k == y)
    passes_last = (x == y) & (k == y)

    def straight(c):
        return remote(r_keep.at[0, c], r_pr.at[c], xs_sem.at[0, c], xr_sem.at[c], x, 2 * k + y)

    def pass_on(c):
        @pl.when(x == y)
        def _():
            home(1, c).start()

    def own_home(c):
        @pl.when((x == y) & (k != y))
        def _():
            home(0, c).start()

    def after_relay():
        own_home(0)
        own_home(1)

    def after_left():
        swap(0).wait_recv()
        pass_on(0)
        own_home(2)

    for c in range(TILES):
        r_keep[0, c] = r_y[:, c * tile : (c + 1) * tile]
        swap(c).start()
    l_out[...] = l_y[...]
    with jax.named_scope("last_mul"):
        multiply(True, after_relay, after_left)
    with jax.named_scope("ray"):
        total = high_dot_nt(r_keep[1, 0], r_ps[0])
        for c in range(TILES):
            total = total + high_dot_nt(r_keep[0, c], r_y[:, c * tile : (c + 1) * tile])
        for c in range(1, TILES):
            if c == TILES - 1:
                with jax.named_scope("l_red"):
                    left_reduce_finish()
                g_loc[0] = high_dot_nt(l_out[...], l_y[...])
            with jax.named_scope("swap"):
                swap(c).wait_recv()
            if c == 1:
                pass_on(c)
            total = total + high_dot_nt(r_keep[1, c], r_ps[c])
        g_loc[1] = total

    def rest_home():
        own_home(TILES - 1)
        for c in range(STRAIGHT, TILES):

            @pl.when(passes_last)
            def _():
                home(1, c).start()

            @pl.when(direct)
            def _():
                straight(c).start()


    with jax.named_scope("last_sum"):
        g_fac[k] = sum_across(2, S, rest_home)
    left_drain()
    later.drain()
    with jax.named_scope("last_hand"):
        hand_over(2, lambda: None, lambda: None)
    ray_out[...] = g_fac[...]
    with jax.named_scope("home"):
        for c in range(TILES):
            swap(c).wait_send()

            @pl.when(passes_last if c >= STRAIGHT else x == y)
            def _():
                home(1, c).wait_send()

            if c >= STRAIGHT:

                @pl.when(direct)
                def _():
                    straight(c).wait_send()

            @pl.when((x == y) & (k != y))
            def _():
                home(0, c).wait_send()

            @pl.when(stays)
            def _():
                r_out[:, c * tile : (c + 1) * tile] = r_keep[0, c]

            @pl.when(jnp.logical_not(stays))
            def _():
                home(0, c).wait_recv()
                r_out[:, c * tile : (c + 1) * tile] = r_pr[c]


def finish_kernel(l_in, r_in, ray_in, l_out, l_ray, r_out, r_ray):
    for src, dst in ((l_in, l_out), (r_in, r_out)):
        for b in range(dst.shape[0] // S):
            dst[b * S : (b + 1) * S, :] = src[:, b * S : (b + 1) * S].T
    l_ray[...] = ray_in[0]
    r_ray[...] = ray_in[1]


def solution(mesh):
    def local_program(left_op, left_start, right_op, right_start):
        l_nb, r_nb = left_op.shape[0] // 4, right_op.shape[0] // 4
        dma = pltpu.SemaphoreType.DMA
        vmem = pl.BlockSpec(memory_space=pltpu.VMEM)
        hbm = pl.BlockSpec(memory_space=pl.ANY)
        shape = jax.ShapeDtypeStruct
        left_t, right_t, rayleigh = pl.pallas_call(
            kernel,
            out_shape=(shape((S, l_nb), F32), shape((S, r_nb), F32), shape((2, S, S), F32)),
            in_specs=[hbm, vmem, hbm, vmem],
            out_specs=(vmem, vmem, vmem),
            scratch_shapes=[
                pltpu.VMEM(left_op.shape, BF16),
                pltpu.VMEM((RING, right_op.shape[0], r_nb // TILES), BF16),
                pltpu.VMEM((S, l_nb), BF16),
                pltpu.VMEM((2, S, l_nb), BF16),
                pltpu.VMEM((2, S, l_nb), F32),
                pltpu.VMEM((2, S, l_nb), F32),
                pltpu.VMEM((S, l_nb), F32),
                pltpu.VMEM((S, l_nb), F32),
                pltpu.VMEM((S, l_nb), BF16),
                pltpu.VMEM((S, l_nb), F32),
                pltpu.VMEM((3 * S, l_nb), BF16),
                pltpu.VMEM((CHUNKS, S, r_nb // CHUNKS), BF16),
                pltpu.VMEM((4, CHUNKS, S, r_nb // CHUNKS), BF16),
                pltpu.VMEM((TILES, S, r_nb // TILES), F32),
                pltpu.VMEM((TILES, S, r_nb // TILES), F32),
                pltpu.VMEM((S, r_nb), F32),
                pltpu.VMEM((3 * S, r_nb), BF16),
                pltpu.VMEM((2, TILES, S, r_nb // TILES), F32),
                pltpu.VMEM((2, S, S), F32),
                pltpu.VMEM((3, S, S), F32),
                pltpu.VMEM((S, S), F32),
                pltpu.VMEM((3, 3, S, S), F32),
                pltpu.VMEM((S, S), F32),
                pltpu.VMEM((2, S, S), F32),
                dma, dma((RING,)),
                dma((2, CHUNKS)), dma((2, CHUNKS)), dma((2, CHUNKS)), dma((2, CHUNKS)),
                dma((TILES,)), dma((TILES,)), dma((2, TILES)), dma((TILES,)), dma((TILES,)), dma((TILES,)),
                dma((2,)), dma((2,)), dma, dma, dma((2,)), dma((2,)), dma, dma,
                dma((3,)), dma((3,)), dma((3, 3)), dma((3, 3)), dma((3,)), dma((3,)),
            ],
            compiler_params=pltpu.CompilerParams(has_side_effects=True, vmem_limit_bytes=64 * 1024 * 1024 - 65536),
        )(left_op, left_start, right_op, right_start)
        left_basis, left_ray, right_basis, right_ray = pl.pallas_call(
            finish_kernel,
            out_shape=(shape((l_nb, S), F32), shape((S, S), F32), shape((r_nb, S), F32), shape((S, S), F32)),
            in_specs=[vmem] * 3,
            out_specs=(vmem,) * 4,
        )(left_t, right_t, rayleigh)
        return left_basis, left_ray, right_basis, right_ray

    op_spec = P(("batch", "row"), "col")
    vec_spec = P(("batch", "row", "col"), None)
    small_spec = P("batch", None)
    return jax.shard_map(
        local_program, mesh=mesh, in_specs=(op_spec, vec_spec, op_spec, vec_spec),
        out_specs=(vec_spec, small_spec, vec_spec, small_spec), check_vma=False,
    )
```

```python
import jax
import jax.numpy as jnp
from jax import lax
from jax.experimental import pallas as pl
from jax.experimental.pallas import tpu as pltpu
from jax.sharding import PartitionSpec as P

SWEEPS = 4
S = 128
RING = 4
TILES = 4
CHUNKS = 2
STRAIGHT = 2
PANEL = 16
MESH = pl.DeviceIdType.MESH
F32, BF16 = jnp.float32, jnp.bfloat16
NT = (((1,), (1,)), ((), ()))
TN = (((0,), (0,)), ((), ()))


def dot(lhs, rhs):
    return jnp.dot(lhs, rhs, preferred_element_type=F32)


def dot_nt(lhs, rhs):
    return lax.dot_general(lhs, rhs, NT, preferred_element_type=F32)


def split(value):
    high = value.astype(BF16)
    rest = value - high.astype(F32)
    mid = rest.astype(BF16)
    low = (rest - mid.astype(F32)).astype(BF16)
    return high, mid, low


def remote(src, dst, send_sem, recv_sem, row, col):
    return pltpu.make_async_remote_copy(
        src_ref=src, dst_ref=dst, send_sem=send_sem, recv_sem=recv_sem,
        device_id={"row": row, "col": col}, device_id_type=MESH,
    )


def inverse_factor(ref):
    sub = lax.broadcasted_iota(jnp.int32, (PANEL, S), 0)
    lane = lax.broadcasted_iota(jnp.int32, (PANEL, S), 1)

    tall_row = lax.broadcasted_iota(jnp.int32, (S, S), 0)
    tall_lane = lax.broadcasted_iota(jnp.int32, (S, S), 1)

    def panel(p, carry):
        k0 = pl.multiple_of(p * PANEL, PANEL)
        inside = (tall_lane >= k0) & (tall_lane < k0 + PANEL) & (tall_row >= k0 + PANEL)
        at = lane - k0
        rows = ref[pl.ds(k0, PANEL), :]
        heads = jnp.stack(
            [
                jnp.broadcast_to(jnp.sum(jnp.where(at == j, rows, 0.0), axis=1, keepdims=True), (PANEL, S))
                for j in range(PANEL)
            ]
        )
        high, mid, low = split(jnp.where(at >= PANEL, rows, 0.0))
        cols = jnp.concatenate([high, mid, high, mid, high, low], axis=0)
        rows = jnp.where((at >= 0) & (at < PANEL), jnp.where(at == sub, 1.0, 0.0), rows)
        done = rows
        piv = heads[0, 0:1, :]
        for j in range(PANEL):
            here = sub == j
            root = lax.rsqrt(piv)
            inv = root * root
            done = jnp.where(here, rows * root, done)
            mult = jnp.where(here, 0.0, heads[0])
            if j < PANEL - 1:
                head_rows = heads[1:, j : j + 1, :] * inv
                piv = heads[1, j + 1 : j + 2, :] - heads[0, j + 1 : j + 2, :] * head_rows[0]
                heads = jnp.where(here[None], head_rows, heads[1:] - mult[None] * head_rows)
            scaled = rows[j : j + 1, :] * inv
            rows = jnp.where(here, scaled, rows - mult * scaled)
        high, mid, low = split(rows)
        rhs = jnp.concatenate([high, high, mid, mid, low, high], axis=0)
        change = lax.dot_general(cols, rhs, TN, preferred_element_type=F32)
        ref[...] = jnp.where(inside, 0.0, ref[...]) - change
        ref[pl.ds(k0, PANEL), :] = done
        return carry

    lax.fori_loop(0, S // PANEL, panel, 0)


class Op:
    def __init__(self, **refs):
        self.__dict__.update(refs)


def kernel(
    l_op, l_start, r_op, r_start,
    l_out, r_out, ray_out,
    l_a, r_a,
    l_xs, l_xt, l_mate_s, l_mate_r, l_side_s, l_side_r, l_hand, l_y, l_keep, l_sp,
    r_xs, r_xt, r_ps, r_pr, r_y, r_sp, r_keep,
    g_loc, g_one, g_sum, g_two, g_m, g_fac,
    l_asem, r_asem,
    gs_sem, gr_sem, fs_sem, fr_sem, ps_sem, pr_sem, xs_sem, xr_sem, es_sem, er_sem,
    lgs_sem, lgr_sem, lhs_sem, lhr_sem, lms_sem, lmr_sem, lss_sem, lsr_sem,
    a1s_sem, a1r_sem, a2s_sem, a2r_sem, a3s_sem, a3r_sem,
):
    y = lax.axis_index("row")
    col = lax.axis_index("col")
    x = col // 2
    k = col % 2
    mate = x * 2 + (1 - k)
    l_n, r_n = l_op.shape[0] * 2, r_op.shape[0] * 2
    l_nb, r_nb = l_n // 8, r_n // 8
    tile = r_nb // TILES
    piece = r_nb // CHUNKS

    left = Op(i=0, n=l_n, nb=l_nb, y=l_y, sp=l_sp)
    right = Op(i=1, n=r_n, nb=r_nb, y=r_y, sp=r_sp)
    ops = [left, right]

    def r_fetch(t):
        half = jnp.where(t < TILES, 1 - y, y)
        start = pl.multiple_of(half * r_nb + (t % TILES) * tile, tile)
        return pltpu.make_async_copy(r_op.at[:, pl.ds(start, tile)], r_a.at[t % RING], r_asem.at[t % RING])

    for t in range(RING):
        r_fetch(t).start()
    l_load = pltpu.make_async_copy(l_op, l_a, l_asem)
    l_load.start()

    class Gather:
        def __init__(self, first):
            self.dest_row = y if first else x
            self.my_slot = 2 * x + k if first else 2 * k + y
            self.src = x if first else y
            self.slots = [2 * a + k if first else 2 * k + a for a in range(2)]
            self.other_slots = [2 * a + (1 - k) if first else 2 * (1 - k) + a for a in range(2)]
            self.sends_to_self = [(self.dest_row == y) & (x == a) for a in range(2)]
            self.gets_from_self = [(x == a) if first else ((x == y) & (y == a)) for a in range(2)]

        def copy(self, a, h, recv):
            return remote(
                r_xs.at[h], r_xt.at[self.my_slot, h], gs_sem.at[a, h], gr_sem.at[recv, h], self.dest_row, 2 * a + k
            )

        def forward(self, a, h, slots):
            ref = r_xt.at[slots[a], h]
            return remote(ref, ref, fs_sem.at[a, h], fr_sem.at[a, h], y, mate)

        def start(self, h):
            for a in range(2):

                @pl.when(self.sends_to_self[a])
                def _():
                    r_xt[self.my_slot, h] = r_xs[h]

                @pl.when(jnp.logical_not(self.sends_to_self[a]))
                def _():
                    self.copy(a, h, self.src).start()

        def finish(self):
            for h in range(CHUNKS):
                for a in range(2):

                    @pl.when(jnp.logical_not(self.gets_from_self[a]))
                    def _():
                        self.copy(0, h, a).wait_recv()

                    self.forward(a, h, self.slots).start()
                for a in range(2):
                    self.forward(a, h, self.other_slots).wait_recv()
                if h < CHUNKS - 1:
                    right_early(h)

        def drain(self):
            for h in range(CHUNKS):
                for a in range(2):
                    self.forward(a, h, self.slots).wait_send()

                    @pl.when(jnp.logical_not(self.sends_to_self[a]))
                    def _():
                        self.copy(a, h, self.src).wait_send()

    def left_copy(b, slot):
        return remote(l_xs, l_xt.at[slot], lgs_sem.at[b], lgr_sem.at[slot], b, 2 * y + x)

    def left_across(b):
        return remote(l_xs, l_hand, lgs_sem.at[b], lhr_sem, 1 - y, col)

    def left_hand_on():
        return remote(l_hand, l_xt.at[k], lhs_sem, lgr_sem.at[k], y, 2 * (1 - x) + x)

    def left_self(b):
        return (b == y) & (y == x) & (x == k)

    def left_start():
        for b in (1 - y, y):
            across = (b != y) & (x != y)

            @pl.when(left_self(b))
            def _():
                l_xt[k] = l_xs[...]

            @pl.when(across)
            def _():
                left_across(b).start()

            @pl.when(jnp.logical_not(left_self(b) | across))
            def _():
                left_copy(b, k).start()

    def left_relay():
        @pl.when(x == y)
        def _():
            left_across(0).wait_recv()
            left_hand_on().start()

    def left_finish():
        for slot in range(2):

            @pl.when(jnp.logical_not((y == x) & (x == k) & (k == slot)))
            def _():
                left_copy(0, slot).wait_recv()

    def left_drain():
        for b in range(2):

            @pl.when(jnp.logical_not(left_self(b)))
            def _():
                left_copy(b, k).wait_send()

        @pl.when(x == y)
        def _():
            left_hand_on().wait_send()

    def left_block(index):
        rows = pl.ds(pl.multiple_of(index * l_nb, l_nb), l_nb)
        return dot_nt(l_xt[0], l_a[rows, :l_nb]) + dot_nt(l_xt[1], l_a[rows, l_nb:])

    def left_mate(a):
        return remote(l_mate_s.at[a], l_mate_r.at[a], lms_sem.at[a], lmr_sem.at[a], y, mate)

    def left_side():
        return remote(l_side_s, l_side_r, lss_sem, lsr_sem, y, 2 * (1 - x) + k)

    def left_multiply():
        l_mate_s[1 - x] = left_block(2 * (1 - x) + (1 - k))
        left_mate(1 - x).start()
        l_side_s[...] = left_block(2 * (1 - x) + k)
        l_mate_s[x] = left_block(2 * x + (1 - k))
        left_mate(x).start()
        left_mate(1 - x).wait_recv()
        l_side_s[...] = l_side_s[...] + l_mate_r[1 - x]
        left_side().start()
        l_y[...] = left_block(2 * x + k)

    def left_reduce_finish():
        left_mate(x).wait_recv()
        l_y[...] = l_y[...] + l_mate_r[x]
        left_side().wait_recv()
        l_y[...] = l_y[...] + l_side_r[...]
        left_side().wait_send()
        for a in range(2):
            left_mate(a).wait_send()

    def right_send(t):
        return remote(r_ps.at[t], r_pr.at[t], ps_sem.at[t], pr_sem.at[t], 1 - y, col)

    def right_part(b, h):
        total = None
        for s in range(4):
            part = dot(r_xt[s, h], r_a[b, s * r_nb + h * piece : s * r_nb + (h + 1) * piece, :])
            total = part if total is None else total + part
        return total

    def right_early(h):
        def one(t, carry):
            if h == 0:
                r_fetch(t).wait()
                r_ps[t] = right_part(t, h)
            else:
                r_ps[t] = r_ps[t] + right_part(t, h)
            return carry

        lax.fori_loop(0, TILES, one, 0)

    def right_others(last):
        def one(t, carry):
            r_ps[t] = r_ps[t] + right_part(t, CHUNKS - 1)
            if not last:
                right_send(t).start()
            r_fetch(t + RING).start()
            return carry

        lax.fori_loop(0, TILES, one, 0)

    def right_own(last, begin, end):
        def one(i, carry):
            t = i + TILES
            r_fetch(t).wait()
            b = t % RING
            total = None
            for h in range(CHUNKS):
                part = right_part(b, h)
                total = part if total is None else total + part
            r_y[:, pl.ds(pl.multiple_of(i * tile, tile), tile)] = total
            if not last:
                r_fetch(lax.rem(t + RING, 2 * TILES)).start()
            return carry

        lax.fori_loop(begin, end, one, 0)

    def left_gram():
        with jax.named_scope("l_red"):
            left_reduce_finish()
        half = l_y[...].astype(BF16)
        pack(0, dot_nt(half, half))

    def right_reduce_finish():
        gram = None
        for t in range(TILES):
            if t == TILES - 1:
                left_gram()
            right_send(t).wait_recv()
            res = r_y[:, t * tile : (t + 1) * tile] + r_pr[t]
            r_y[:, t * tile : (t + 1) * tile] = res
            half = res.astype(BF16)
            part = dot_nt(half, half)
            gram = part if gram is None else gram + part
        pack(1, gram)
        for t in range(TILES):
            right_send(t).wait_send()

    low_lane = lax.broadcasted_iota(jnp.int32, (32, S), 1)
    tall_row = lax.broadcasted_iota(jnp.int32, (S, S), 0)
    tall_lane = lax.broadcasted_iota(jnp.int32, (S, S), 1)
    count = jnp.where(k == 0, float(l_n), float(r_n))

    def pack(i, gram):
        g_loc[i, :64, :] = gram[:64]
        g_loc[i, 64:96, :] = jnp.where(low_lane < 64, pltpu.roll(gram[64:96], 64, axis=1), gram[96:])

    def sum_across(par, rows, after_sends=lambda: None):
        part = pl.ds(0, rows)
        one = remote(g_loc.at[1 - k, part], g_one.at[par, part], a1s_sem.at[par], a1r_sem.at[par], y, mate)
        one.start()
        with jax.named_scope("ar_one"):
            one.wait_recv()
        g_sum[part, :] = g_loc[k, part, :] + g_one[par, part, :]
        twos = []
        for q in (2, 1, 0):
            yd = y + ((q + 1) // 2) * (1 - 2 * y)
            xd = x + ((q + 1) % 2) * (1 - 2 * x)
            two = remote(
                g_sum.at[part], g_two.at[par, q, part], a2s_sem.at[par, q], a2r_sem.at[par, q], yd, 2 * xd + k
            )
            two.start()
            twos.append(two)
        after_sends()
        with jax.named_scope("ar_two"):
            for two in twos:
                two.wait_recv()
        total = (g_sum[part, :] + g_two[par, 0, part, :]) + (g_two[par, 1, part, :] + g_two[par, 2, part, :])
        one.wait_send()
        for two in twos:
            two.wait_send()
        return total / count

    def hand_over(par, left_work, right_work):
        mine, other = g_fac.at[k], g_fac.at[1 - k]
        copy = remote(mine, mine, a3s_sem.at[par], a3r_sem.at[par], y, mate)
        back = remote(other, other, a3s_sem.at[par], a3r_sem.at[par], y, mate)
        copy.start()

        @pl.when(k == 0)
        def _():
            left_work()
            back.wait_recv()
            right_work()

        @pl.when(k == 1)
        def _():
            right_work()
            back.wait_recv()
            left_work()

        copy.wait_send()

    def factor(par):
        gram = sum_across(par, 96)
        g_m[:64, :] = gram[:64]
        g_m[64:96, :] = pltpu.roll(gram[64:], 64, axis=1)
        g_m[96:, :] = gram[64:]
        with jax.named_scope("chol"):
            inverse_factor(g_m)
        g_fac[k] = jnp.where(tall_lane <= tall_row, g_m[...], 0.0)

    def apply_piece(o, lhs, start, width):
        high, mid, low = split(o.y[:, start : start + width])
        rhs = jnp.concatenate([high, high, mid, mid, low, high], axis=0)
        return dot(lhs, rhs)

    def apply_lhs(o):
        high, mid, low = split(g_fac[o.i])
        return jnp.concatenate([high, mid, high, mid, high, low], axis=1)

    def second_gram(o):
        lhs = apply_lhs(o)
        for start in range(0, o.nb, 256):
            res = apply_piece(o, lhs, start, 256)
            o.y[:, start : start + 256] = res
            parts = split(res)
            for q in range(3):
                o.sp[q * S : (q + 1) * S, start : start + 256] = parts[q]
        both = dot_nt(o.sp[: 2 * S, :], o.sp[: 2 * S, :])
        cross = dot_nt(o.sp[:S, :], o.sp[2 * S :, :])
        pack(o.i, both[:S, :S] + ((both[:S, S:] + both[S:, :S]) + (both[S:, S:] + (cross + cross.T))))

    def high_dot_nt(lhs, rhs):
        return lax.dot_general(lhs, rhs, NT, precision=lax.Precision.HIGHEST, preferred_element_type=F32)

    def new_left():
        lhs = apply_lhs(left)
        for start in range(0, l_nb, 256):
            res = apply_piece(left, lhs, start, 256)
            l_y[:, start : start + 256] = res
            l_xs[:, start : start + 256] = res.astype(BF16)

    def new_right():
        lhs = apply_lhs(right)
        for h in range(CHUNKS):
            for start in range(h * piece, (h + 1) * piece, 256):
                res = apply_piece(right, lhs, start, 256)
                r_y[:, start : start + 256] = res
                r_xs[h, :, start - h * piece : start - h * piece + 256] = res.astype(BF16)
            later.start(h)

    def multiply(last, after_relay=lambda: None, after_left=lambda: None):
        with jax.named_scope("r_mul0"):
            right_others(last)
        with jax.named_scope("l_relay"):
            left_relay()
            after_relay()
        with jax.named_scope("r_mul1"):
            right_own(last, 0, 2)
        with jax.named_scope("l_fin"):
            left_finish()
        with jax.named_scope("l_mul"):
            left_multiply()
            after_left()
        with jax.named_scope("r_mul2"):
            right_own(last, 2, TILES)

    first, later = Gather(True), Gather(False)
    for h in range(CHUNKS):
        for b in range(piece // S):
            r_xs[h, :, b * S : (b + 1) * S] = r_start[h * piece + b * S : h * piece + (b + 1) * S, :].T.astype(BF16)
        first.start(h)
    for b in range(l_nb // S):
        l_xs[:, b * S : (b + 1) * S] = l_start[b * S : (b + 1) * S, :].T.astype(BF16)
    left_start()
    with jax.named_scope("gather_first"):
        first.finish()
    first.drain()
    l_load.wait()

    def sweep(i, carry):
        multiply(False)
        with jax.named_scope("r_red"):
            right_reduce_finish()
        left_drain()
        pl.when(i > 0)(later.drain)
        with jax.named_scope("factor0"):
            factor(0)
        with jax.named_scope("gram2"):
            hand_over(0, lambda: second_gram(left), lambda: second_gram(right))
        with jax.named_scope("factor1"):
            factor(1)
        with jax.named_scope("new_basis"):
            hand_over(1, new_left, new_right)
            left_start()
        with jax.named_scope("gather"):
            later.finish()
        return carry

    lax.fori_loop(0, SWEEPS, sweep, 0)

    stays = (x == y) & (k == y)

    def swap(c):
        return remote(r_keep.at[0, c], r_keep.at[1, c], es_sem.at[c], er_sem.at[c], 1 - y, col)

    def home(q, c):
        place = 2 * k + (y if q == 0 else 1 - y)
        return remote(r_keep.at[q, c], r_pr.at[c], xs_sem.at[q, c], xr_sem.at[c], y, place)

    direct = (x != y) & (k == y)
    passes_last = (x == y) & (k == y)

    def straight(c):
        return remote(r_keep.at[0, c], r_pr.at[c], xs_sem.at[0, c], xr_sem.at[c], x, 2 * k + y)

    def pass_on(c):
        @pl.when(x == y)
        def _():
            home(1, c).start()

    def own_home(c):
        @pl.when((x == y) & (k != y))
        def _():
            home(0, c).start()

    def after_relay():
        own_home(0)
        own_home(1)

    def after_left():
        swap(0).wait_recv()
        pass_on(0)
        own_home(2)

    for c in range(TILES):
        r_keep[0, c] = r_y[:, c * tile : (c + 1) * tile]
        swap(c).start()
    l_keep[...] = l_y[...]
    with jax.named_scope("last_mul"):
        multiply(True, after_relay, after_left)
    with jax.named_scope("ray"):
        total = high_dot_nt(r_keep[1, 0], r_ps[0])
        for c in range(TILES):
            total = total + high_dot_nt(r_keep[0, c], r_y[:, c * tile : (c + 1) * tile])
        for c in range(1, TILES):
            if c == TILES - 1:
                with jax.named_scope("l_red"):
                    left_reduce_finish()
                g_loc[0] = high_dot_nt(l_keep[...], l_y[...])
            with jax.named_scope("swap"):
                swap(c).wait_recv()
            if c == 1:
                pass_on(c)
            total = total + high_dot_nt(r_keep[1, c], r_ps[c])
        g_loc[1] = total

    def rest_home():
        own_home(TILES - 1)
        for c in range(STRAIGHT, TILES):

            @pl.when(passes_last)
            def _():
                home(1, c).start()

            @pl.when(direct)
            def _():
                straight(c).start()

        for b in range(0, l_nb, S):
            l_out[b : b + S, :] = l_keep[:, b : b + S].T


    with jax.named_scope("last_sum"):
        g_fac[k] = sum_across(2, S, rest_home)
    left_drain()
    later.drain()
    with jax.named_scope("last_hand"):
        hand_over(2, lambda: None, lambda: None)
    ray_out[...] = g_fac[...]

    def write(c, src):
        for b in range(0, tile, S):
            r_out[c * tile + b : c * tile + b + S, :] = src[:, b : b + S].T

    with jax.named_scope("home"):
        for c in range(TILES):
            swap(c).wait_send()

            @pl.when(passes_last if c >= STRAIGHT else x == y)
            def _():
                home(1, c).wait_send()

            if c >= STRAIGHT:

                @pl.when(direct)
                def _():
                    straight(c).wait_send()

            @pl.when((x == y) & (k != y))
            def _():
                home(0, c).wait_send()

            @pl.when(stays)
            def _():
                write(c, r_keep.at[0, c])

            @pl.when(jnp.logical_not(stays))
            def _():
                home(0, c).wait_recv()
                write(c, r_pr.at[c])


def finish_kernel(l_in, r_in, ray_in, l_out, l_ray, r_out, r_ray):
    l_out[...] = l_in[...]
    r_out[...] = r_in[...]
    l_ray[...] = ray_in[0]
    r_ray[...] = ray_in[1]


def solution(mesh):
    def local_program(left_op, left_start, right_op, right_start):
        l_nb, r_nb = left_op.shape[0] // 4, right_op.shape[0] // 4
        dma = pltpu.SemaphoreType.DMA
        vmem = pl.BlockSpec(memory_space=pltpu.VMEM)
        hbm = pl.BlockSpec(memory_space=pl.ANY)
        shape = jax.ShapeDtypeStruct
        left_own, right_own, rayleigh = pl.pallas_call(
            kernel,
            out_shape=(shape((l_nb, S), F32), shape((r_nb, S), F32), shape((2, S, S), F32)),
            in_specs=[hbm, vmem, hbm, vmem],
            out_specs=(vmem, vmem, vmem),
            scratch_shapes=[
                pltpu.VMEM(left_op.shape, BF16),
                pltpu.VMEM((RING, right_op.shape[0], r_nb // TILES), BF16),
                pltpu.VMEM((S, l_nb), BF16),
                pltpu.VMEM((2, S, l_nb), BF16),
                pltpu.VMEM((2, S, l_nb), F32),
                pltpu.VMEM((2, S, l_nb), F32),
                pltpu.VMEM((S, l_nb), F32),
                pltpu.VMEM((S, l_nb), F32),
                pltpu.VMEM((S, l_nb), BF16),
                pltpu.VMEM((S, l_nb), F32),
                pltpu.VMEM((S, l_nb), F32),
                pltpu.VMEM((3 * S, l_nb), BF16),
                pltpu.VMEM((CHUNKS, S, r_nb // CHUNKS), BF16),
                pltpu.VMEM((4, CHUNKS, S, r_nb // CHUNKS), BF16),
                pltpu.VMEM((TILES, S, r_nb // TILES), F32),
                pltpu.VMEM((TILES, S, r_nb // TILES), F32),
                pltpu.VMEM((S, r_nb), F32),
                pltpu.VMEM((3 * S, r_nb), BF16),
                pltpu.VMEM((2, TILES, S, r_nb // TILES), F32),
                pltpu.VMEM((2, S, S), F32),
                pltpu.VMEM((3, S, S), F32),
                pltpu.VMEM((S, S), F32),
                pltpu.VMEM((3, 3, S, S), F32),
                pltpu.VMEM((S, S), F32),
                pltpu.VMEM((2, S, S), F32),
                dma, dma((RING,)),
                dma((2, CHUNKS)), dma((2, CHUNKS)), dma((2, CHUNKS)), dma((2, CHUNKS)),
                dma((TILES,)), dma((TILES,)), dma((2, TILES)), dma((TILES,)), dma((TILES,)), dma((TILES,)),
                dma((2,)), dma((2,)), dma, dma, dma((2,)), dma((2,)), dma, dma,
                dma((3,)), dma((3,)), dma((3, 3)), dma((3, 3)), dma((3,)), dma((3,)),
            ],
            compiler_params=pltpu.CompilerParams(has_side_effects=True, vmem_limit_bytes=64 * 1024 * 1024 - 65536),
        )(left_op, left_start, right_op, right_start)
        left_basis, left_ray, right_basis, right_ray = pl.pallas_call(
            finish_kernel,
            out_shape=(shape((l_nb, S), F32), shape((S, S), F32), shape((r_nb, S), F32), shape((S, S), F32)),
            in_specs=[vmem] * 3,
            out_specs=(vmem,) * 4,
        )(left_own, right_own, rayleigh)
        return left_basis, left_ray, right_basis, right_ray

    op_spec = P(("batch", "row"), "col")
    vec_spec = P(("batch", "row", "col"), None)
    small_spec = P("batch", None)
    return jax.shard_map(
        local_program, mesh=mesh, in_specs=(op_spec, vec_spec, op_spec, vec_spec),
        out_specs=(vec_spec, small_spec, vec_spec, small_spec), check_vma=False,
    )
```
